32 devices in a mesh: col: 8 (over z, y), row: 4 (over x, core).
Axes of the slice: x: 2, y: 2, z: 4, core: 2. Of those that a mesh axis runs over, the one named last changes fastest.
Arguments:
- vel_u: float32 [75, 192, 2048], P(None, 'row', 'col')
- vel_v: float32 [75, 192, 2048], P(None, 'row', 'col')
- temperature: float32 [75, 192, 2048], P(None, 'row', 'col')
- salinity: float32 [75, 192, 2048], P(None, 'row', 'col')
- sea_level: float32 [192, 2048], P('row', 'col')
- trans_u: float32 [192, 2048], P('row', 'col')
- trans_v: float32 [192, 2048], P('row', 'col')
- bathymetry: float32 [192, 2048], P('row', 'col')
- kmt_levels: int32 [192, 2048], P('row', 'col')
- tide_force: float32 [30, 2], replicated
Outputs:
- output 1: float32 [192, 2048], P('row', 'col')
- output 2: float32 [192, 2048], P('row', 'col')
- output 3: float32 [192, 2048], P('row', 'col')
- output 4: float32 [75, 192, 2048], P(None, 'row', 'col')
- output 5: float32 [75, 192, 2048], P(None, 'row', 'col')
- output 6: float32 [75, 192, 2048], P(None, 'row', 'col')
- output 7: float32 [75, 192, 2048], P(None, 'row', 'col')
All inputs are finite; a program needn't handle non-finite values.
Results may differ from the reference program's by a relative error of at most 0.001.
Values sent between devices are 32-bit elements.
A program may use at most 1 GiB of HBM per device.

```python
import jax
import jax.numpy as jnp
from jax import lax

LEVELS = 75
SUBCYCLES = 30
GRID_NY = 192
GRID_NX = 2048

GRAVITY = 1.0
GRID_DX = 1.0
TIME_STEP = 4.0
ALPHA_T = 0.02
BETA_S = 0.015
T_REF = 1.0
S_REF = 1.0
VISC_KV = 0.001
DIFF_KT = 0.0005


def pad_halo(field):
    wrapped = jnp.concatenate([field[..., -1:], field, field[..., :1]], axis=-1)
    walls = jnp.zeros_like(wrapped[..., :1, :])
    return jnp.concatenate([walls, wrapped, walls], axis=-2)


def level_mask(count, n_levels):
    levels = jnp.arange(n_levels, dtype=jnp.int32)[:, None, None]
    return (levels < count[None]).astype(jnp.float32)


def interface_coef(count, thick, kappa, n_levels):
    levels = jnp.arange(n_levels - 1, dtype=jnp.int32)[:, None, None]
    active = (levels + 1 < count[None]).astype(jnp.float32)
    safe = jnp.where(count > 0, thick, 1.0)
    return active * (TIME_STEP * kappa / (safe * safe))[None]


def column_solve(source, couple):
    edge = jnp.zeros_like(source[:1])
    upper = jnp.concatenate([couple, edge], axis=0)
    lower = jnp.concatenate([edge, couple], axis=0)
    diag = 1.0 + upper + lower

    def forward(carry, slab):
        gain_prev, part_prev = carry
        lower_k, diag_k, upper_k, source_k = slab
        pivot = diag_k - lower_k * gain_prev
        gain = upper_k / pivot
        part = (source_k + lower_k * part_prev) / pivot
        return (gain, part), (gain, part)

    start = (jnp.zeros_like(source[0]), jnp.zeros_like(source[0]))
    _, (gains, parts) = lax.scan(forward, start, (lower, diag, upper, source))

    def backward(below, slab):
        gain, part = slab
        here = part + gain * below
        return here, here

    _, profile = lax.scan(backward, jnp.zeros_like(source[0]), (gains, parts), reverse=True)
    return profile


def geometry(kmt_ext, depth_ext):
    kmt_cell = kmt_ext[1:-1, 1:-1]
    thick_ext = depth_ext / jnp.maximum(kmt_ext, 1).astype(jnp.float32)
    thick_cell = thick_ext[1:-1, 1:-1]
    return {"k_cell": kmt_cell, "k_u": jnp.minimum(kmt_cell, kmt_ext[1:-1, 2:]), "k_v": jnp.minimum(kmt_cell, kmt_ext[2:, 1:-1]), "dz_cell": thick_cell, "dz_u": 0.5 * (thick_cell + thick_ext[1:-1, 2:]), "dz_v": 0.5 * (thick_cell + thick_ext[2:, 1:-1])}


def surface_fields(layout):
    k_faces = jnp.stack([layout["k_u"], layout["k_v"]])
    face_depth = k_faces.astype(jnp.float32) * jnp.stack([layout["dz_u"], layout["dz_v"]])
    face_wet = (k_faces > 0).astype(jnp.float32)
    wet_cell = (layout["k_cell"] > 0).astype(jnp.float32)
    return face_depth, face_wet, wet_cell


def momentum_tend(u_ext, v_ext, p_ext):
    cen_u = 0.5 * (u_ext[:, 1:-1, :-1] + u_ext[:, 1:-1, 1:])
    corner_v = 0.5 * (v_ext[:, :-1, 1:-1] + v_ext[:, :-1, 2:])
    corner_u = 0.5 * (u_ext[:, :-1, 1:-1] + u_ext[:, 1:, 1:-1])
    flux_uu = cen_u * cen_u
    flux_vu = corner_v * corner_u
    tend_u = -(flux_uu[:, :, 1:] - flux_uu[:, :, :-1] + flux_vu[:, 1:, :] - flux_vu[:, :-1, :] + p_ext[:, 1:-1, 2:] - p_ext[:, 1:-1, 1:-1]) / GRID_DX
    cen_v = 0.5 * (v_ext[:, :-1, 1:-1] + v_ext[:, 1:, 1:-1])
    side_u = 0.5 * (u_ext[:, 1:-1, :-1] + u_ext[:, 2:, :-1])
    side_v = 0.5 * (v_ext[:, 1:-1, :-1] + v_ext[:, 1:-1, 1:])
    flux_vv = cen_v * cen_v
    flux_uv = side_u * side_v
    tend_v = -(flux_vv[:, 1:, :] - flux_vv[:, :-1, :] + flux_uv[:, :, 1:] - flux_uv[:, :, :-1] + p_ext[:, 2:, 1:-1] - p_ext[:, 1:-1, 1:-1]) / GRID_DX
    return tend_u, tend_v


def baroclinic_predict(vel_u, vel_v, temperature, salinity, layout, halo_fn):
    n_levels = vel_u.shape[0]
    mask_c = level_mask(layout["k_cell"], n_levels)
    mask_u = level_mask(layout["k_u"], n_levels)
    mask_v = level_mask(layout["k_v"], n_levels)
    vel_um = vel_u * mask_u
    vel_vm = vel_v * mask_v
    density = mask_c * (BETA_S * (salinity - S_REF) - ALPHA_T * (temperature - T_REF))
    pressure = GRAVITY * layout["dz_cell"] * (jnp.cumsum(density, axis=0) - 0.5 * density)
    cell_coef = interface_coef(layout["k_cell"], layout["dz_cell"], DIFF_KT, n_levels)
    temp_mix = column_solve(temperature * mask_c, cell_coef)
    salt_mix = column_solve(salinity * mask_c, cell_coef)
    edges = halo_fn(jnp.stack([vel_um, vel_vm, pressure, temp_mix, salt_mix]))
    tend_u, tend_v = momentum_tend(edges[0], edges[1], edges[2])
    u_star = column_solve(mask_u * (vel_um + TIME_STEP * tend_u), interface_coef(layout["k_u"], layout["dz_u"], VISC_KV, n_levels))
    v_star = column_solve(mask_v * (vel_vm + TIME_STEP * tend_v), interface_coef(layout["k_v"], layout["dz_v"], VISC_KV, n_levels))
    forcing = jnp.stack([jnp.sum(layout["dz_u"] * (u_star - vel_um), axis=0), jnp.sum(layout["dz_v"] * (v_star - vel_vm), axis=0)]) / TIME_STEP
    return u_star, v_star, forcing, edges[3:], (mask_c, mask_u, mask_v)


def barotropic(eta_start, trans_start, face_depth, face_wet, wet_cell, forcing, tide_force, halo_fn):
    n_sub = tide_force.shape[0]
    dt_sub = TIME_STEP / n_sub
    weight_norm = 6.0 / (n_sub * (n_sub + 1) * (n_sub + 2))

    def substep(step, carry):
        eta_now, trans_now, trans_avg = carry
        trans_ext = halo_fn(trans_now)
        divergence = (trans_now[0] - trans_ext[0, 1:-1, :-2] + trans_now[1] - trans_ext[1, :-2, 1:-1]) / GRID_DX
        eta_next = wet_cell * (eta_now - dt_sub * divergence)
        eta_ext = halo_fn(eta_next)
        slope = jnp.stack([eta_ext[1:-1, 2:] - eta_next, eta_ext[2:, 1:-1] - eta_next]) / GRID_DX
        tide_now = lax.dynamic_index_in_dim(tide_force, step, 0, keepdims=False)
        trans_next = face_wet * (trans_now + dt_sub * (face_depth * (tide_now[:, None, None] - GRAVITY * slope) + forcing))
        weight = weight_norm * ((step + 1) * (n_sub - step)).astype(jnp.float32)
        return eta_next, trans_next, trans_avg + weight * trans_next

    return lax.fori_loop(0, n_sub, substep, (eta_start, trans_start, jnp.zeros_like(trans_start)))


def correct_velocity(star, dz_face, depth_face, mean_trans, mask):
    safe = jnp.where(depth_face > 0, depth_face, 1.0)
    return mask * (star + ((mean_trans - jnp.sum(dz_face * star, axis=0)) / safe)[None])


def advect_tracers(tracer_ext, flow_ext, mask_c):
    flux_x = flow_ext[0, :, 1:-1, :-1] * (0.5 * (tracer_ext[..., 1:-1, :-1] + tracer_ext[..., 1:-1, 1:]))
    flux_y = flow_ext[1, :, :-1, 1:-1] * (0.5 * (tracer_ext[..., :-1, 1:-1] + tracer_ext[..., 1:, 1:-1]))
    divergence = (flux_x[..., 1:] - flux_x[..., :-1] + flux_y[..., 1:, :] - flux_y[..., :-1, :]) / GRID_DX
    return mask_c * (tracer_ext[..., 1:-1, 1:-1] - TIME_STEP * divergence)


def baroclinic_finish(u_star, v_star, trans_avg, face_depth, layout, tracer_ext, masks, halo_fn):
    mask_c, mask_u, mask_v = masks
    vel_uc = correct_velocity(u_star, layout["dz_u"], face_depth[0], trans_avg[0], mask_u)
    vel_vc = correct_velocity(v_star, layout["dz_v"], face_depth[1], trans_avg[1], mask_v)
    flows = halo_fn(jnp.stack([vel_uc, vel_vc]))
    tracers = advect_tracers(tracer_ext, flows, mask_c)
    return vel_uc, vel_vc, tracers[0], tracers[1]


def ocean_step(vel_u, vel_v, temperature, salinity, sea_level, trans_u, trans_v, bathymetry, kmt_levels, tide_force, halo_fn):
    layout = geometry(halo_fn(kmt_levels), halo_fn(bathymetry))
    u_star, v_star, forcing, tracer_ext, masks = baroclinic_predict(vel_u, vel_v, temperature, salinity, layout, halo_fn)
    face_depth, face_wet, wet_cell = surface_fields(layout)
    eta_new, trans_new, trans_avg = barotropic(wet_cell * sea_level, face_wet * jnp.stack([trans_u, trans_v]), face_depth, face_wet, wet_cell, forcing, tide_force, halo_fn)
    vel_uc, vel_vc, temp_new, salt_new = baroclinic_finish(u_star, v_star, trans_avg, face_depth, layout, tracer_ext, masks, halo_fn)
    return eta_new, trans_new[0], trans_new[1], vel_uc, vel_vc, temp_new, salt_new


def draw_levels(key):
    key_count, key_land = jax.random.split(key)
    counts = jax.random.randint(key_count, (GRID_NY, GRID_NX), (LEVELS + 2) // 3, LEVELS + 1)
    land = jax.random.randint(key_land, (GRID_NY, GRID_NX), 0, 12) == 0
    levels = jnp.where(land, 0, counts).astype(jnp.int32)
    return levels.at[0, 0].set(0).at[GRID_NY - 1, GRID_NX - 1].set(LEVELS)


def setup_inputs(seed: int = 0) -> dict:
    keys = jax.random.split(jax.random.key(seed), 10)
    shape_cube = (LEVELS, GRID_NY, GRID_NX)
    shape_plane = (GRID_NY, GRID_NX)
    depth_frac = jnp.arange(LEVELS, dtype=jnp.float32)[:, None, None] / LEVELS
    return {
        "vel_u": 0.1 * jax.random.normal(keys[0], shape_cube, jnp.float32),
        "vel_v": 0.1 * jax.random.normal(keys[1], shape_cube, jnp.float32),
        "temperature": 2.0 * (1.0 - depth_frac) + 0.5 * jax.random.normal(keys[2], shape_cube, jnp.float32),
        "salinity": 1.0 + depth_frac + 0.3 * jax.random.normal(keys[3], shape_cube, jnp.float32),
        "sea_level": 0.05 * jax.random.normal(keys[4], shape_plane, jnp.float32),
        "trans_u": 0.05 * jax.random.normal(keys[5], shape_plane, jnp.float32),
        "trans_v": 0.05 * jax.random.normal(keys[6], shape_plane, jnp.float32),
        "bathymetry": 0.6 + 0.8 * jax.random.uniform(keys[7], shape_plane, jnp.float32),
        "kmt_levels": draw_levels(keys[8]),
        "tide_force": 0.01 + 0.01 * jax.random.normal(keys[9], (SUBCYCLES, 2), jnp.float32),
    }


def reference(vel_u, vel_v, temperature, salinity, sea_level, trans_u, trans_v, bathymetry, kmt_levels, tide_force):
    return ocean_step(vel_u, vel_v, temperature, salinity, sea_level, trans_u, trans_v, bathymetry, kmt_levels, tide_force, pad_halo)
```

```python
import functools

import jax
import jax.numpy as jnp
from jax import lax
from jax.experimental import pallas as pl
from jax.experimental.pallas import tpu as pltpu
from jax.sharding import PartitionSpec as P

TIME_STEP = 4.0
ALPHA_T = 0.02
BETA_S = 0.015
VISC_KV = 0.001
DIFF_KT = 0.0005
MESH = pl.DeviceIdType.MESH
H = 32
CH = 15
UN = 5
UM = 3
KB = 5
SUB, LANES = 8, 128
LAST = LANES - 1
F32 = jnp.float32
KMT, DEPTH, ETA, TU, TV, FX, FY = range(7)
KU, KV, DZU, DZV, GU, GV, BU, BV, WD = range(9)
FIRST, SECOND = slice(0, 1), slice(1, 2)


def iota(shape, axis):
    return lax.broadcasted_iota(jnp.int32, shape, axis)


def reduced(x):
    return pl.reciprocal(x, approx=False)


def lane_of(x):
    return iota(x.shape, 1)


def slot_of(k, bank):
    b = (k >= bank).astype(jnp.int32)
    return b, 2 * (k - b * bank)


def turn(x, n):
    return pltpu.roll(x, n % LANES if isinstance(n, int) else n, 1)


def shift_east(x, halo):
    left, right = turn(x[:, :LANES], -1), turn(x[:, LANES:], -1)
    edge = lane_of(left) == LAST
    return jnp.concatenate([jnp.where(edge, right, left), jnp.where(edge, halo, right)], axis=1)


def shift_west(x, halo):
    left, right = turn(x[:, :LANES], 1), turn(x[:, LANES:], 1)
    edge = lane_of(left) == 0
    return jnp.concatenate([jnp.where(edge, halo, left), jnp.where(edge, left, right)], axis=1)


def tiles_of(x):
    return [x[SUB * t:SUB * t + SUB] for t in range(x.shape[0] // SUB)]


def shift_north(x, halo):
    rolled = [pltpu.roll(t, SUB - 1, 0) for t in tiles_of(x)]
    edge = iota(rolled[0].shape, 0) == SUB - 1
    rolled.append(jnp.broadcast_to(halo, rolled[0].shape))
    return jnp.concatenate([jnp.where(edge, b, a) for a, b in zip(rolled[:-1], rolled[1:])], axis=0)


def shift_south(x, halo):
    rolled = [pltpu.roll(t, 1, 0) for t in tiles_of(x)]
    edge = iota(rolled[0].shape, 0) == 0
    rolled.insert(0, jnp.broadcast_to(halo, rolled[0].shape))
    return jnp.concatenate([jnp.where(edge, a, b) for a, b in zip(rolled[:-1], rolled[1:])], axis=0)


def merged(west, east):
    even = lane_of(west) % 2 == 0
    back = turn(east, -1)
    return jnp.where(even, west, back), turn(jnp.where(even, back, west), -1)


def main_kernel(n_rows, n_cols,
                kmt_in, bat_in, eta_in, tu_in, tv_in, u_in, v_in, t_in, s_in, tide,
                us_out, vs_out, tm_out, sm_out, bar_out, corr_out, face_out, vcs_out,
                halo_out, trow_n_out, trow_s_out,
                kmt_v, ext, xp, acc, pk_w, pk_e, r_e, r_w, r_ne, r_nw, r_se, r_sw,
                ub, vb, tb, sb, pu, pv, gc, gu, gv, pp, wet_v, dz_v, cc_v, cum_v, faces, coefs, push_v, sum_v,
                bank_uv, bank_ts, sc_w, sc_e, rc_e, rc_w, rc_nw, rc_se, hc, corner_p,
                sr_n, sr_s, sp_s, rr_n, rr_s, rp_n,
                tc_w, tc_e, tr_n, tr_s, qc_e, qc_w, qr_n, qr_s, su_e, sv_n, ru_w, rv_s,
                plane_sem, in_sem, out_sem, send_sem, recv_sem):
    n_sub = tide.shape[0]
    n_lev = u_in.shape[0]
    n_chunk = n_lev // CH
    bank = (n_lev + 1) // 2
    ny, nx = kmt_in.shape
    dt_sub = TIME_STEP / n_sub
    col, row = lax.axis_index("col"), lax.axis_index("row")
    east, west = lax.rem(col + 1, n_cols), lax.rem(col + n_cols - 1, n_cols)
    north, south = lax.rem(row + 1, n_rows), lax.rem(row + n_rows - 1, n_rows)
    where_to = {"n": (col, north), "s": (col, south), "e": (east, row), "w": (west, row),
                "ne": (east, north), "nw": (west, north), "se": (east, south), "sw": (west, south)}
    own = (pl.ds(H, ny), pl.ds(0, nx))
    mid, cols = slice(H, H + ny), slice(0, nx)
    at_n, at_s = slice(H + ny, H + ny + 1), slice(H - 1, H)
    whole, wide = ny + 2 * H, nx + LANES
    at_w, at_e = slice(wide - 1, wide), slice(nx, nx + 1)
    first_row, last_row = FIRST, slice(ny - 1, ny)

    planes = [pltpu.make_async_copy(kmt_in, kmt_v, plane_sem.at[KMT])]
    for i, ref in ((DEPTH, bat_in), (ETA, eta_in), (TU, tu_in), (TV, tv_in)):
        planes.append(pltpu.make_async_copy(ref, ext.at[(i, *own)], plane_sem.at[i]))
    for c in planes:
        c.start()

    def load(a, c):
        src, dst, off = ((t_in, tb, 1), (s_in, sb, 1), (u_in, ub, 0), (v_in, vb, 0))[a]
        return pltpu.make_async_copy(src.at[pl.ds(c * CH, CH)], dst.at[pl.ds(c * CH + off, CH)], in_sem.at[a, c])

    for c in range(n_chunk):
        for a in range(4):
            load(a, c).start()

    barrier = pltpu.get_barrier_semaphore()
    for c_id, r_id in where_to.values():
        pl.semaphore_signal(barrier, inc=1, device_id={"col": c_id, "row": r_id}, device_id_type=MESH)

    used = []

    def remote(src, dst, to):
        c_id, r_id = where_to[to]
        i = len(used)
        used.append(i)
        return pltpu.make_async_remote_copy(src_ref=src, dst_ref=dst, send_sem=send_sem.at[i], recv_sem=recv_sem.at[i],
                                            device_id={"col": c_id, "row": r_id}, device_id_type=MESH)

    def started(copies):
        for c in copies:
            c.start()
        return copies

    def wide_copies(p0, n):
        ps = pl.ds(p0, n)
        low, mids, high = pl.ds(0, 2 * SUB), pl.ds(0, SUB), pl.ds(2 * SUB, SUB)
        return started([
            remote(ext.at[ps, pl.ds(H, H), pl.ds(0, nx)], ext.at[ps, pl.ds(H + ny, H), pl.ds(0, nx)], "s"),
            remote(ext.at[ps, pl.ds(ny, H), pl.ds(0, nx)], ext.at[ps, pl.ds(0, H), pl.ds(0, nx)], "n"),
            remote(pk_w.at[ps, low], r_e.at[ps], "w"),
            remote(pk_e.at[ps, low], r_w.at[ps], "e"),
            remote(pk_w.at[ps, mids], r_ne.at[ps], "sw"),
            remote(pk_e.at[ps, mids], r_nw.at[ps], "se"),
            remote(pk_w.at[ps, high], r_se.at[ps], "nw"),
            remote(pk_e.at[ps, high], r_sw.at[ps], "ne"),
        ])

    group = iota((SUB, LANES), 1) // H
    n_groups = LANES // H

    def pack(p):
        x = ext[(p, *own)]
        for ref, tile, g0 in ((pk_w, x[:, :LANES], 0), (pk_e, x[:, nx - LANES:], n_groups - 1)):
            for at, first, count in ((0, 0, 4), (1, 4, 2), (2, 2, 4)):
                total = jnp.zeros((SUB, LANES), F32)
                for q in range(count):
                    rows = tile[SUB * (first + q):SUB * (first + q) + SUB]
                    rows = turn(rows, H * (q - g0)) if q != g0 else rows
                    total = jnp.where(group == q, rows, total)
                ref[p, SUB * at:SUB * at + SUB, :] = total

    def unpack(p):
        edge = H // SUB
        for t in range(whole // SUB):
            if t < edge:
                e_tile, w_tile, q = r_se[p], r_sw[p], t
            elif t < (H + ny) // SUB:
                rows = slice(SUB * ((t - edge) // n_groups), SUB * ((t - edge) // n_groups) + SUB)
                e_tile, w_tile, q = r_e[p, rows], r_w[p, rows], (t - edge) % n_groups
            else:
                e_tile, w_tile, q = r_ne[p], r_nw[p], t - (H + ny) // SUB
            e_tile = turn(e_tile, -H * q) if q else e_tile
            w_tile = turn(w_tile, H * (n_groups - 1 - q)) if q != n_groups - 1 else w_tile
            side = jnp.where(group == 0, e_tile, jnp.where(group == n_groups - 1, w_tile, 0.0))
            ext[p, SUB * t:SUB * t + SUB, nx:] = side

    for c in planes:
        c.wait()
    kmt = kmt_v[...].astype(F32)
    ext[(KMT, *own)] = kmt
    for p in range(FX):
        pack(p)
    pl.semaphore_wait(barrier, len(where_to))
    first = wide_copies(KMT, FX)

    dz = ext[(DEPTH, *own)] / jnp.maximum(kmt, 1.0)
    safe = jnp.where(kmt > 0, dz, 1.0)
    zero = jnp.zeros((ny, nx), F32)
    wet_v[...] = kmt
    dz_v[...] = dz
    cc_v[...] = (TIME_STEP * DIFF_KT) / (safe * safe)
    cum_v[...] = zero
    for ref in (tb, sb, pu, pv):
        ref[0] = zero
        ref[n_lev + 1] = zero
    for ref in (gc, gu, gv):
        ref[0] = zero + 1.0
    for ref in (bank_uv, bank_ts, sc_w, su_e):
        ref[...] = jnp.zeros(ref.shape, F32)
    lane = iota((ny, LANES), 1)
    even = lane % 2 == 0

    def both_edges(x):
        return jnp.where(lane < LANES // 2, x[:, :LANES], x[:, nx - LANES:])

    def down_levels(k0):
        g, t_up, s_up, cum = gc[k0], tb[k0], sb[k0], cum_v[...]
        wet = k0.astype(F32) < wet_v[...]
        for d in range(UN):
            k = k0 + d
            below = (k + 1).astype(F32) < wet_v[...]
            t, s = tb[k + 1], sb[k + 1]
            dens = jnp.where(wet, BETA_S * (s - 1.0) - ALPHA_T * (t - 1.0), 0.0)
            cum = cum + dens
            pres = dz_v[...] * (cum - 0.5 * dens)
            pp[k] = pres
            coef = cc_v[...]
            up = jnp.where(below, coef, 0.0)
            inv = reduced(1.0 + up + coef * (1.0 - g))
            g = up * inv
            t_up = jnp.where(wet, (t + coef * t_up) * inv, 0.0)
            s_up = jnp.where(wet, (s + coef * s_up) * inv, 0.0)
            gc[k + 1] = g
            tb[k + 1] = t_up
            sb[k + 1] = s_up
            wet = below
            u, v = ub[k], vb[k]
            b, m = slot_of(k, bank)
            here = ((lane + 1 - m) & LAST) < 2
            pltpu.store(bank_uv.at[0, b], turn(both_edges(u), m), mask=here)
            pltpu.store(bank_uv.at[1, b], turn(both_edges(v), m), mask=here)
            pltpu.store(sc_w.at[2], turn(pres[:, :LANES], m + b), mask=lane == m + b)
            sr_s[k, FIRST] = u[first_row]
            sr_s[k, SECOND] = v[first_row]
            sp_s[k] = pres[first_row]
            sr_n[k, FIRST] = u[last_row]
            sr_n[k, SECOND] = v[last_row]
        cum_v[...] = cum

    def down_chunk(c, carry):
        for a in range(4):
            load(a, c).wait()

        def levels(i, carry):
            down_levels(c * CH + i * UN)
            return carry

        return lax.fori_loop(0, CH // UN, levels, carry)

    lax.fori_loop(0, n_chunk, down_chunk, 0)

    def split_banks(banks):
        a, b = banks[0], turn(banks[1], 1)
        return jnp.where(even, a, b), turn(jnp.where(even, b, a), 1)

    for i in range(2):
        sc_w[i], sc_e[i] = split_banks(bank_uv.at[i])
    second = started([
        remote(sc_w, rc_e, "w"),
        remote(sc_e, rc_w, "e"),
        remote(sr_n, rr_s, "n"),
        remote(sr_s, rr_n, "s"),
        remote(sp_s, rp_n, "s"),
        remote(sc_e.at[0, pl.ds(0, SUB)], rc_nw, "se"),
        remote(sc_w.at[1, pl.ds(ny - SUB, SUB)], rc_se, "nw"),
    ])

    def store_out(a, c):
        src, dst = ((tb, tm_out), (sb, sm_out), (pu, us_out), (pv, vs_out))[a]
        return pltpu.make_async_copy(src.at[pl.ds(c * CH + 1, CH)], dst.at[pl.ds(c * CH, CH)], out_sem.at[a, c])

    def upward(a, level):
        def chunk(j, carry):
            c = n_chunk - 1 - j

            def levels(i, carry):
                level(c * CH + CH - 1 - i * UN)
                return carry

            lax.fori_loop(0, CH // UN, levels, 0)
            store_out(a, c).start()
            store_out(a + 1, c).start()
            return carry

        lax.fori_loop(0, n_chunk, chunk, 0)

    def mix_levels(k0):
        t, s = tb[k0 + 2], sb[k0 + 2]
        for d in range(UN):
            k = k0 - d
            g = gc[k + 1]
            t = tb[k + 1] + g * t
            s = sb[k + 1] + g * s
            tb[k + 1] = t
            sb[k + 1] = s
            b, m = slot_of(k, bank)
            here = ((lane + 1 - m) & LAST) < 2
            pltpu.store(bank_ts.at[0, b], turn(both_edges(t), m), mask=here)
            pltpu.store(bank_ts.at[1, b], turn(both_edges(s), m), mask=here)
            tr_s[k, FIRST] = t[first_row]
            tr_s[k, SECOND] = s[first_row]
            tr_n[k, FIRST] = t[last_row]
            tr_n[k, SECOND] = s[last_row]

    upward(0, mix_levels)
    for i in range(2):
        tc_w[i], tc_e[i] = split_banks(bank_ts.at[i])

    for c in first:
        c.wait()
    for p in range(FX):
        unpack(p)
    line = iota((whole, wide), 0)
    seen = ((line >= H) | (row > 0)) & ((line < H + ny) | (row < n_rows - 1))
    kx = jnp.where(seen, ext[KMT], 0.0)
    ext[KMT] = kx
    dzx = ext[DEPTH] / jnp.maximum(kx, 1.0)
    ku = jnp.minimum(kx, pltpu.roll(kx, wide - 1, 1))
    kv = jnp.minimum(kx, pltpu.roll(kx, whole - 1, 0))
    dzu = 0.5 * (dzx + pltpu.roll(dzx, wide - 1, 1))
    dzv = 0.5 * (dzx + pltpu.roll(dzx, whole - 1, 0))
    xp[KU] = ku
    xp[KV] = kv
    xp[DZU] = dzu
    xp[DZV] = dzv
    xp[GU] = jnp.where(ku > 0, dt_sub * (ku * dzu), 0.0)
    xp[GV] = jnp.where(kv > 0, dt_sub * (kv * dzv), 0.0)
    xp[WD] = jnp.where(kx > 0, dt_sub, 0.0)
    ext[ETA] = jnp.where(kx > 0, ext[ETA], 0.0)
    ext[TU] = jnp.where(ku > 0, ext[TU], 0.0)
    ext[TV] = jnp.where(kv > 0, ext[TV], 0.0)
    face_out[2] = wet_v[...]
    for i in range(2):
        count = xp[(KU + i, *own)]
        safe = jnp.where(count > 0, xp[(DZU + i, *own)], 1.0)
        faces[i] = count
        face_out[i] = count
        coefs[i] = (TIME_STEP * VISC_KV) / (safe * safe)
        push_v[i] = zero
        sum_v[i] = zero

    for c in second:
        c.wait_recv()
    pair = lane // 2
    lev = jnp.where(pair < bank, pair + bank * (lane % 2), n_lev).astype(F32)

    def column(ref, count):
        return jnp.where(lev < count, ref, 0.0)

    u_w = column(rc_w[0], xp[KU, mid, at_w])
    v_w = column(rc_w[1], xp[KV, mid, at_w])
    u_e = column(rc_e[0], xp[KU, mid, at_e])
    v_e = column(rc_e[1], xp[KV, mid, at_e])
    u_last = column(sc_e[0], xp[KU, mid, nx - 1:nx])
    v_zero = column(sc_w[1], xp[KV, mid, FIRST])
    corner_u = jnp.where(lev[FIRST] < xp[KU, at_n, at_w], rc_nw[FIRST, :], 0.0)
    q_e = 0.25 * (u_last + u_e) * (u_last + u_e) + rc_e[2]
    c_w = (u_w + shift_north(u_w, corner_u)) * (v_w + v_zero)
    hc[0, 0], hc[0, 1] = merged(u_w, q_e)
    hc[1, 0], hc[1, 1] = merged(c_w, v_e)
    corner_p[...] = jnp.where(lev[:SUB] < xp[KV, H - SUB:H, at_e], rc_se[...], 0.0)

    def momentum_levels(i, carry):
        k0 = i * UM
        parts = [pu[k0], pv[k0]]
        gains = [gu[k0], gv[k0]]
        wets = [k0.astype(F32) < faces[f] for f in range(2)]
        for d in range(UM):
            k = k0 + d
            kf = k.astype(F32)
            u = jnp.where(wets[0], ub[k], 0.0)
            v = jnp.where(wets[1], vb[k], 0.0)
            p = pp[k]
            b, m = slot_of(k, bank)
            edge_uq = turn(hc[0, b], LANES - m)
            edge_cv = turn(hc[1, b], LANES - m)
            rows_n, rows_s = rr_n[k], rr_s[k]
            u_n = jnp.where(kf < xp[KU, at_n, cols], rows_n[FIRST], 0.0)
            v_n = jnp.where(kf < xp[KV, at_n, cols], rows_n[SECOND], 0.0)
            u_s = jnp.where(kf < xp[KU, at_s, cols], rows_s[FIRST], 0.0)
            v_s = jnp.where(kf < xp[KV, at_s, cols], rows_s[SECOND], 0.0)
            corner_v = turn(corner_p[...], LAST - m - b)[SUB - 1:]
            v_s8 = jnp.broadcast_to(v_s, (SUB, nx))
            v_s_e = shift_east(v_s8, jnp.broadcast_to(corner_v, (SUB, LANES)))[FIRST]

            cen_u = shift_west(u, edge_uq) + u
            head_u = 0.25 * (cen_u * cen_u) + p
            corner = (u + shift_north(u, u_n)) * (v + shift_east(v, edge_cv))
            corner_s = (u_s + u[first_row]) * (v_s + v_s_e)
            grad_u = (shift_east(head_u, edge_uq) - head_u) + 0.25 * (corner - shift_south(corner, corner_s))
            cen_v = shift_south(v, v_s) + v
            head_v = 0.25 * (cen_v * cen_v) + p
            edge_v = v[last_row] + v_n
            edge_v = 0.25 * (edge_v * edge_v) + rp_n[k]
            grad_v = (shift_north(head_v, edge_v) - head_v) + 0.25 * (corner - shift_west(corner, edge_cv))
            for f, grad, now, part, gain in ((0, grad_u, u, pu, gu), (1, grad_v, v, pv, gv)):
                below = kf + 1.0 < faces[f]
                push = jnp.where(wets[f], -TIME_STEP * grad, 0.0)
                source = now + push
                push_v[f] += push
                sum_v[f] += source
                coef = coefs[f]
                up = jnp.where(below, coef, 0.0)
                inv = reduced(1.0 + up + coef * (1.0 - gains[f]))
                gains[f] = up * inv
                parts[f] = jnp.where(wets[f], (source + coef * parts[f]) * inv, 0.0)
                gain[k + 1] = gains[f]
                part[k + 1] = parts[f]
                wets[f] = below
        return carry

    lax.fori_loop(0, n_lev // UM, momentum_levels, 0)

    for f in range(2):
        ext[(FX + f, *own)] = xp[(DZU + f, *own)] * push_v[f] * (1.0 / TIME_STEP)
        pack(FX + f)
    third = wide_copies(FX, 2)
    tracer = started([
        remote(tc_w, qc_e, "w"),
        remote(tc_e, qc_w, "e"),
        remote(tr_n, qr_s, "n"),
        remote(tr_s, qr_n, "s"),
    ])

    def rise_levels(k0):
        u, v = pu[k0 + 2], pv[k0 + 2]
        for d in range(UN):
            k = k0 - d
            u = pu[k + 1] + gu[k + 1] * u
            v = pv[k + 1] + gv[k + 1] * v
            pu[k + 1] = u
            pv[k + 1] = v
            b, m = slot_of(k, bank)
            pltpu.store(su_e, turn(u[:, nx - LANES:], m + b + 1), mask=lane == m + b)
            sv_n[k] = v[last_row]

    upward(2, rise_levels)
    fourth = started([remote(su_e, ru_w, "e"), remote(sv_n, rv_s, "n")])

    for c in third:
        c.wait_recv()
    for f in range(2):
        unpack(FX + f)
        xp[BU + f] = jnp.where(xp[KU + f] > 0, dt_sub * ext[FX + f], 0.0)
    acc[...] = jnp.zeros(acc.shape, F32)
    norm = 6.0 / (n_sub * (n_sub + 1) * (n_sub + 2))
    tiles = whole // SUB
    line8 = iota((SUB, wide), 0)
    t0 = H // SUB - 1

    def substep(n, carry):
        tide_u, tide_v = tide[n, 0], tide[n, 1]
        weight = norm * ((n + 1) * (n_sub - n)).astype(F32)

        def finish(t, eta, rolled, rolled_next, u, v):
            rows = slice(SUB * t, SUB * t + SUB)
            eta_n = jnp.where(line8 == SUB - 1, rolled_next, rolled)
            eta_e = pltpu.roll(eta, wide - 1, 1)
            u_new = u + (xp[GU, rows] * (tide_u + (eta - eta_e)) + xp[BU, rows])
            v_new = v + (xp[GV, rows] * (tide_v + (eta - eta_n)) + xp[BV, rows])
            ext[TU, rows] = u_new
            ext[TV, rows] = v_new
            if t0 <= t < (H + ny) // SUB:
                at = slice(SUB * (t - t0), SUB * (t - t0) + SUB)
                acc[0, at] += weight * u_new
                acc[1, at, :nx] += weight * v_new[:, :nx]

        last = None
        v_below = jnp.zeros((SUB, wide), F32)
        for t in range(tiles):
            rows = slice(SUB * t, SUB * t + SUB)
            u, v = ext[TU, rows], ext[TV, rows]
            v_roll = pltpu.roll(v, 1, 0)
            v_s = jnp.where(line8 == 0, v_below, v_roll)
            v_below = v_roll
            eta = ext[ETA, rows] - xp[WD, rows] * ((u - pltpu.roll(u, 1, 1)) + (v - v_s))
            ext[ETA, rows] = eta
            rolled = pltpu.roll(eta, SUB - 1, 0)
            if last is not None:
                eta_b, rolled_b, u_b, v_b = last
                finish(t - 1, eta_b, rolled_b, rolled, u_b, v_b)
            last = (eta, rolled, u, v)
        finish(tiles - 1, eta, rolled, rolled, u, v)
        return carry

    lax.fori_loop(0, n_sub, substep, 0)
    for i in range(3):
        bar_out[i] = ext[(ETA + i, *own)]

    def safe_depth(f, rows, lanes):
        depth = xp[KU + f, rows, lanes] * xp[DZU + f, rows, lanes]
        return jnp.where(depth > 0, depth, 1.0)

    inner = slice(SUB, SUB + ny)
    for f in range(2):
        corr_out[f] = (acc[f, inner, cols] - xp[DZU + f, mid, cols] * sum_v[f]) / safe_depth(f, mid, cols)
    for c in fourth:
        c.wait_recv()
    star = ru_w[...]
    fix = (acc[0, inner, at_w] - xp[DZU, mid, at_w] * jnp.sum(star, axis=1, keepdims=True)) / safe_depth(0, mid, at_w)
    u_c = column(star + fix, xp[KU, mid, at_w])
    star = rv_s[...]
    fix = (acc[1, SUB - 1:SUB, cols] - xp[DZV, at_s, cols] * jnp.sum(star, axis=0)) / safe_depth(1, at_s, cols)
    levels = iota(star.shape, 0).astype(F32)
    vcs_out[...] = jnp.where(levels < xp[KV, at_s, cols][None], star + fix[None], 0.0)
    for c in tracer:
        c.wait_recv()
    for i in range(2):
        halo_out[i, 0], halo_out[i, 1] = merged(u_c * (qc_w[i] + tc_w[i]), qc_e[i])
    trow_n_out[...] = qr_n[...]
    trow_s_out[...] = qr_s[...]
    for c in second + third + tracer + fourth:
        c.wait_send()
    for c in range(n_chunk):
        for a in range(4):
            store_out(a, c).wait()


def last_kernel(us, vs, tm, sm, bar, corr, faces, vcs, halo, trow_n, trow_s,
                eta_out, tu_out, tv_out, u_out, v_out, t_out, s_out, *, bank):
    step = pl.program_id(0)

    @pl.when(step == 0)
    def _():
        for i, ref in enumerate((eta_out, tu_out, tv_out)):
            ref[...] = bar[i]

    for i in range(KB):
        k = step * KB + i
        kf = k.astype(F32)
        u = jnp.where(kf < faces[0], us[i] + corr[0], 0.0)
        v = jnp.where(kf < faces[1], vs[i] + corr[1], 0.0)
        u_out[i] = u
        v_out[i] = v
        wet = kf < faces[2]
        v_s = vcs[k]
        rows_n, rows_s = trow_n[k], trow_s[k]
        b, m = slot_of(k, bank)
        for a, src, dst in ((0, tm, t_out), (1, sm, s_out)):
            x = src[i]
            edge = turn(halo[a, b], LANES - m)
            flux_x = u * (x + shift_east(x, edge))
            flux_y = v * (x + shift_north(x, rows_n[a:a + 1]))
            edge_y = v_s * (rows_s[a:a + 1] + x[FIRST])
            div = flux_x - shift_west(flux_x, edge) + flux_y - shift_south(flux_y, edge_y)
            dst[i] = jnp.where(wet, x - (0.5 * TIME_STEP) * div, 0.0)


def solution(mesh):
    n_cols, n_rows = mesh.shape["col"], mesh.shape["row"]

    def local_step(vel_u, vel_v, value_a11, salinity, sea_level, trans_u, trans_v, bathymetry, kmt_levels, tide_force):
        n_lev, ny, nx = vel_u.shape
        whole, wide = ny + 2 * H, nx + LANES
        n_chunk, bank = n_lev // CH, (n_lev + 1) // 2
        any_spec = pl.BlockSpec(memory_space=pl.ANY)
        vmem_spec = pl.BlockSpec(memory_space=pltpu.VMEM)
        cube = (n_lev, ny, nx)
        deep = (n_lev + 2, ny, nx)
        column, pair_c, rows1, rows2 = (ny, LANES), (2, ny, LANES), (n_lev, 1, nx), (n_lev, 2, nx)
        banks, two, small = (2, 2, ny, LANES), (2, ny, nx), (SUB, LANES)

        def sds(*shape):
            return jax.ShapeDtypeStruct(shape, F32)

        def bufs(*shapes):
            return [pltpu.VMEM(shape, F32) for shape in shapes]

        def sems(*shape):
            return pltpu.SemaphoreType.DMA(shape)

        passed = [(3, ny, nx), two, (3, ny, nx), rows1, banks, rows2, rows2]
        *cubes, bar, corr, face, vcs, halo, trow_n, trow_s = pl.pallas_call(
            functools.partial(main_kernel, n_rows, n_cols),
            out_shape=[sds(*s) for s in [cube] * 4 + passed],
            in_specs=[any_spec] * 9 + [pl.BlockSpec(memory_space=pltpu.SMEM)],
            out_specs=[any_spec] * 4 + [vmem_spec] * len(passed),
            scratch_shapes=[
                pltpu.VMEM((ny, nx), jnp.int32),
                *bufs((7, whole, wide), (9, whole, wide), (2, ny + SUB, wide)),
                *bufs(*[(7, 3 * SUB, LANES)] * 2, *[(7, 2 * SUB, LANES)] * 2, *[(7, SUB, LANES)] * 4),
                *bufs(cube, cube, *[deep] * 7, cube, *[(ny, nx)] * 4, two, two, two, two),
                *bufs(banks, banks, (3, ny, LANES), pair_c, (3, ny, LANES), pair_c, small, small, banks, small),
                *bufs(rows2, rows2, rows1, rows2, rows2, rows1),
                *bufs(pair_c, pair_c, rows2, rows2, pair_c, pair_c, rows2, rows2, column, rows1, column, rows1),
                sems(5), sems(4, n_chunk), sems(4, n_chunk), sems(29), sems(29),
            ],
            compiler_params=pltpu.CompilerParams(collective_id=0, has_side_effects=True, vmem_limit_bytes=56 * 2**20),
        )(kmt_levels, bathymetry, sea_level, trans_u, trans_v, vel_u, vel_v, value_a11, salinity, tide_force)

        block = pl.BlockSpec((KB, ny, nx), lambda i: (i, 0, 0))

        def full(*shape):
            return pl.BlockSpec(shape, lambda i: (0,) * len(shape))

        return pl.pallas_call(
            functools.partial(last_kernel, bank=bank),
            grid=(n_lev // KB,),
            out_shape=[sds(ny, nx)] * 3 + [sds(*cube)] * 4,
            in_specs=[block] * 4 + [full(*s) for s in passed],
            out_specs=[full(ny, nx)] * 3 + [block] * 4,
        )(*cubes, bar, corr, face, vcs, halo, trow_n, trow_s)

    spec_cube = P(None, "row", "col")
    spec_plane = P("row", "col")
    return jax.shard_map(local_step, mesh=mesh, in_specs=(spec_cube,) * 4 + (spec_plane,) * 5 + (P(None, None),),
                         out_specs=(spec_plane,) * 3 + (spec_cube,) * 4, check_vma=False)
```

```python
import functools

import jax
import jax.numpy as jnp
from jax import lax
from jax.experimental import pallas as pl
from jax.experimental.pallas import tpu as pltpu
from jax.sharding import PartitionSpec as P

TIME_STEP = 4.0
ALPHA_T = 0.02
BETA_S = 0.015
VISC_KV = 0.001
DIFF_KT = 0.0005
MESH = pl.DeviceIdType.MESH
H = 32
CH = 15
UN = 5
UE = 15
KB = 5
SUB, LANES = 8, 128
LAST = LANES - 1
F32 = jnp.float32
HEAD = 0.25 * TIME_STEP
KMT, DEPTH, ETA, TU, TV, FX, FY = range(7)
KU, KV, DZU, DZV, GU, GV, BU, BV, WD, GW, BW, UW = range(12)
FIRST, SECOND = slice(0, 1), slice(1, 2)


def iota(shape, axis):
    return lax.broadcasted_iota(jnp.int32, shape, axis)


def reduced(x):
    return pl.reciprocal(x, approx=False)


def scaled(x):
    return x if HEAD == 1.0 else HEAD * x


def lane_of(x):
    return iota(x.shape, 1)


def slot_of(k, bank):
    b = (k >= bank).astype(jnp.int32)
    return b, 2 * (k - b * bank)


def turn(x, n):
    return pltpu.roll(x, n % LANES if isinstance(n, int) else n, 1)


def shift_east(x, halo):
    left, right = turn(x[:, :LANES], -1), turn(x[:, LANES:], -1)
    edge = lane_of(left) == LAST
    return jnp.concatenate([jnp.where(edge, right, left), jnp.where(edge, halo, right)], axis=1)


def shift_west(x, halo):
    left, right = turn(x[:, :LANES], 1), turn(x[:, LANES:], 1)
    edge = lane_of(left) == 0
    return jnp.concatenate([jnp.where(edge, halo, left), jnp.where(edge, left, right)], axis=1)


def tiles_of(x):
    return [x[SUB * t:SUB * t + SUB] for t in range(x.shape[0] // SUB)]


def shift_north(x, halo):
    rolled = [pltpu.roll(t, SUB - 1, 0) for t in tiles_of(x)]
    edge = iota(rolled[0].shape, 0) == SUB - 1
    rolled.append(jnp.broadcast_to(halo, rolled[0].shape))
    return jnp.concatenate([jnp.where(edge, b, a) for a, b in zip(rolled[:-1], rolled[1:])], axis=0)


def shift_south(x, halo):
    rolled = [pltpu.roll(t, 1, 0) for t in tiles_of(x)]
    edge = iota(rolled[0].shape, 0) == 0
    rolled.insert(0, jnp.broadcast_to(halo, rolled[0].shape))
    return jnp.concatenate([jnp.where(edge, a, b) for a, b in zip(rolled[:-1], rolled[1:])], axis=0)


def merged(west, east):
    even = lane_of(west) % 2 == 0
    back = turn(east, -1)
    return jnp.where(even, west, back), turn(jnp.where(even, back, west), -1)


def main_kernel(n_rows, n_cols,
                kmt_in, bat_in, eta_in, tu_in, tv_in, u_in, v_in, t_in, s_in, tide,
                pu, pv, tb, sb, bar_out, corr_out, face_out, vcs_out,
                halo_out, trow_n_out, trow_s_out,
                kmt_v, ext, xp, acc, pk_w, pk_e, r_e, r_w, r_ne, r_nw, r_se, r_sw,
                ub, vb, gc, gu, gv, pp, wet_v, dz_v, cc_v, cum_v, faces, coefs, push_v, sum_v, s_now, s_head, s_corner, s_side, s_edge,
                bank_uv, bank_ts, sc_w, sc_e, sp_w, rc_e, rc_w, rp_e, rc_nw, rc_se, hc, corner_p,
                sr_n, sr_s, sp_s, rr_n, rr_s, rp_n,
                tc_w, tc_e, tr_n, tr_s, qc_e, qc_w, qr_n, qr_s, su_e, sv_n, ru_w, rv_s,
                plane_sem, in_sem, send_sem, recv_sem):
    n_sub = tide.shape[1]
    n_lev = u_in.shape[0]
    n_chunk = n_lev // CH
    bank = (n_lev + 1) // 2
    ny, nx = kmt_in.shape
    dt_sub = TIME_STEP / n_sub
    col, row = lax.axis_index("col"), lax.axis_index("row")
    east, west = lax.rem(col + 1, n_cols), lax.rem(col + n_cols - 1, n_cols)
    north, south = lax.rem(row + 1, n_rows), lax.rem(row + n_rows - 1, n_rows)
    where_to = {"n": (col, north), "s": (col, south), "e": (east, row), "w": (west, row),
                "ne": (east, north), "nw": (west, north), "se": (east, south), "sw": (west, south)}
    own = (pl.ds(H, ny), pl.ds(0, nx))
    mid, cols = slice(H, H + ny), slice(0, nx)
    at_n, at_s = slice(H + ny, H + ny + 1), slice(H - 1, H)
    whole, wide = ny + 2 * H, nx + LANES
    at_w, at_e = slice(wide - 1, wide), slice(nx, nx + 1)
    first_row, last_row = FIRST, slice(ny - 1, ny)

    planes = [pltpu.make_async_copy(kmt_in, kmt_v, plane_sem.at[KMT])]
    for i, ref in ((DEPTH, bat_in), (ETA, eta_in), (TU, tu_in), (TV, tv_in)):
        planes.append(pltpu.make_async_copy(ref, ext.at[(i, *own)], plane_sem.at[i]))
    for c in planes:
        c.start()

    def load(a, c):
        src, dst, off = ((u_in, ub, 0), (v_in, vb, 0), (t_in, tb, 1), (s_in, sb, 1))[a]
        return pltpu.make_async_copy(src.at[pl.ds(c * CH, CH)], dst.at[pl.ds(c * CH + off, CH)], in_sem.at[a, c])

    for a in (0, 2):
        for c in range(n_chunk):
            load(a, c).start()
            load(a + 1, c).start()

    barrier = pltpu.get_barrier_semaphore()
    for c_id, r_id in where_to.values():
        pl.semaphore_signal(barrier, inc=1, device_id={"col": c_id, "row": r_id}, device_id_type=MESH)

    used = []

    def remote(src, dst, to):
        c_id, r_id = where_to[to]
        i = len(used)
        used.append(i)
        return pltpu.make_async_remote_copy(src_ref=src, dst_ref=dst, send_sem=send_sem.at[i], recv_sem=recv_sem.at[i],
                                            device_id={"col": c_id, "row": r_id}, device_id_type=MESH)

    def started(copies):
        for c in copies:
            c.start()
        return copies

    def wide_copies(p0, n):
        ps = pl.ds(p0, n)
        low, mids, high = pl.ds(0, 2 * SUB), pl.ds(0, SUB), pl.ds(2 * SUB, SUB)
        return started([
            remote(ext.at[ps, pl.ds(H, H), pl.ds(0, nx)], ext.at[ps, pl.ds(H + ny, H), pl.ds(0, nx)], "s"),
            remote(ext.at[ps, pl.ds(ny, H), pl.ds(0, nx)], ext.at[ps, pl.ds(0, H), pl.ds(0, nx)], "n"),
            remote(pk_w.at[ps, low], r_e.at[ps], "w"),
            remote(pk_e.at[ps, low], r_w.at[ps], "e"),
            remote(pk_w.at[ps, mids], r_ne.at[ps], "sw"),
            remote(pk_e.at[ps, mids], r_nw.at[ps], "se"),
            remote(pk_w.at[ps, high], r_se.at[ps], "nw"),
            remote(pk_e.at[ps, high], r_sw.at[ps], "ne"),
        ])

    group = iota((SUB, LANES), 1) // H
    n_groups = LANES // H

    def pack(p):
        x = ext[(p, *own)]
        for ref, tile, g0 in ((pk_w, x[:, :LANES], 0), (pk_e, x[:, nx - LANES:], n_groups - 1)):
            for at, first, count in ((0, 0, 4), (1, 4, 2), (2, 2, 4)):
                total = jnp.zeros((SUB, LANES), F32)
                for q in range(count):
                    rows = tile[SUB * (first + q):SUB * (first + q) + SUB]
                    rows = turn(rows, H * (q - g0)) if q != g0 else rows
                    total = jnp.where(group == q, rows, total)
                ref[p, SUB * at:SUB * at + SUB, :] = total

    def unpack(p):
        edge = H // SUB
        for t in range(whole // SUB):
            if t < edge:
                e_tile, w_tile, q = r_se[p], r_sw[p], t
            elif t < (H + ny) // SUB:
                rows = slice(SUB * ((t - edge) // n_groups), SUB * ((t - edge) // n_groups) + SUB)
                e_tile, w_tile, q = r_e[p, rows], r_w[p, rows], (t - edge) % n_groups
            else:
                e_tile, w_tile, q = r_ne[p], r_nw[p], t - (H + ny) // SUB
            e_tile = turn(e_tile, -H * q) if q else e_tile
            w_tile = turn(w_tile, H * (n_groups - 1 - q)) if q != n_groups - 1 else w_tile
            side = jnp.where(group == 0, e_tile, jnp.where(group == n_groups - 1, w_tile, 0.0))
            ext[p, SUB * t:SUB * t + SUB, nx:] = side

    for c in planes:
        c.wait()
    kmt = kmt_v[...].astype(F32)
    ext[(KMT, *own)] = kmt
    for p in range(FX):
        pack(p)
    pl.semaphore_wait(barrier, len(where_to))
    first = wide_copies(KMT, FX)

    zero = jnp.zeros((ny, nx), F32)
    for ref in (bank_uv, bank_ts, sp_w, su_e):
        ref[...] = jnp.zeros(ref.shape, F32)
    lane = iota((ny, LANES), 1)
    even = lane % 2 == 0

    def both_edges(x):
        return jnp.where(lane < LANES // 2, x[:, :LANES], x[:, nx - LANES:])

    def gather(x, y, k, banks, rows_s, rows_n):
        b, m = slot_of(k, bank)
        here = ((lane + 1 - m) & LAST) < 2
        pltpu.store(banks.at[0, b], turn(both_edges(x), m), mask=here)
        pltpu.store(banks.at[1, b], turn(both_edges(y), m), mask=here)
        rows_s[k, FIRST] = x[first_row]
        rows_s[k, SECOND] = y[first_row]
        rows_n[k, FIRST] = x[last_row]
        rows_n[k, SECOND] = y[last_row]

    def in_chunks(arrays, levels, step):
        def chunk(c, carry):
            for a in arrays:
                load(a, c).wait()

            def group_of(i, carry):
                levels(c * CH + i * step)
                return carry

            return lax.fori_loop(0, CH // step, group_of, carry)

        lax.fori_loop(0, n_chunk, chunk, 0)

    def edge_levels(k0):
        for d in range(UE):
            gather(ub[k0 + d], vb[k0 + d], k0 + d, bank_uv, sr_s, sr_n)

    in_chunks((0, 1), edge_levels, UE)

    def split_banks(banks):
        a, b = banks[0], turn(banks[1], 1)
        return jnp.where(even, a, b), turn(jnp.where(even, b, a), 1)

    for i in range(2):
        sc_w[i], sc_e[i] = split_banks(bank_uv.at[i])
    second = started([
        remote(sc_w, rc_e, "w"),
        remote(sc_e, rc_w, "e"),
        remote(sr_n, rr_s, "n"),
        remote(sr_s, rr_n, "s"),
        remote(sc_e.at[0, pl.ds(0, SUB)], rc_nw, "se"),
        remote(sc_w.at[1, pl.ds(ny - SUB, SUB)], rc_se, "nw"),
    ])

    dz = ext[(DEPTH, *own)] / jnp.maximum(kmt, 1.0)
    safe = jnp.where(kmt > 0, dz, 1.0)
    wet_v[...] = kmt
    dz_v[...] = TIME_STEP * dz
    cc_v[...] = (TIME_STEP * DIFF_KT) / (safe * safe)
    cum_v[...] = zero
    for ref in (tb, sb, pu, pv):
        ref[0] = zero
        ref[n_lev + 1] = zero
    for ref in (gc, gu, gv):
        ref[0] = zero + 1.0

    def pressure_levels(k0):
        cum = cum_v[...]
        for d in range(UE):
            k = k0 + d
            dens = BETA_S * (sb[k + 1] - 1.0) - ALPHA_T * (tb[k + 1] - 1.0)
            dens = jnp.where(k.astype(F32) < wet_v[...], dens, 0.0)
            cum = cum + dens
            pres = dz_v[...] * (cum - 0.5 * dens)
            pp[k] = pres
            b, m = slot_of(k, bank)
            pltpu.store(sp_w, turn(pres[:, :LANES], m + b), mask=lane == m + b)
            sp_s[k] = pres[first_row]
        cum_v[...] = cum

    in_chunks((2, 3), pressure_levels, UE)
    second += started([remote(sp_w, rp_e, "w"), remote(sp_s, rp_n, "s")])

    def down_levels(i, carry):
        k0 = i * UN
        g, t_up, s_up = gc[k0], tb[k0], sb[k0]
        wet = k0.astype(F32) < wet_v[...]
        for d in range(UN):
            k = k0 + d
            below = (k + 1).astype(F32) < wet_v[...]
            coef = cc_v[...]
            up = jnp.where(below, coef, 0.0)
            inv = reduced(1.0 + up + coef * (1.0 - g))
            g = up * inv
            t_up = jnp.where(wet, (tb[k + 1] + coef * t_up) * inv, 0.0)
            s_up = jnp.where(wet, (sb[k + 1] + coef * s_up) * inv, 0.0)
            gc[k + 1] = g
            tb[k + 1] = t_up
            sb[k + 1] = s_up
            wet = below
        return carry

    lax.fori_loop(0, n_lev // UN, down_levels, 0)

    for c in first:
        c.wait()
    for p in range(FX):
        unpack(p)
    line = iota((whole, wide), 0)
    seen = ((line >= H) | (row > 0)) & ((line < H + ny) | (row < n_rows - 1))
    kx = jnp.where(seen, ext[KMT], 0.0)
    ext[KMT] = kx
    dzx = ext[DEPTH] / jnp.maximum(kx, 1.0)
    ku = jnp.minimum(kx, pltpu.roll(kx, wide - 1, 1))
    kv = jnp.minimum(kx, pltpu.roll(kx, whole - 1, 0))
    dzu = 0.5 * (dzx + pltpu.roll(dzx, wide - 1, 1))
    dzv = 0.5 * (dzx + pltpu.roll(dzx, whole - 1, 0))
    xp[KU] = ku
    xp[KV] = kv
    xp[DZU] = dzu
    xp[DZV] = dzv
    xp[GU] = jnp.where(ku > 0, dt_sub * (ku * dzu), 0.0)
    xp[GV] = jnp.where(kv > 0, dt_sub * (kv * dzv), 0.0)
    xp[WD] = jnp.where(kx > 0, dt_sub, 0.0)
    xp[GW] = pltpu.roll(xp[GU], 1, 1)
    ext[ETA] = jnp.where(kx > 0, ext[ETA], 0.0)
    ext[TU] = jnp.where(ku > 0, ext[TU], 0.0)
    ext[TV] = jnp.where(kv > 0, ext[TV], 0.0)
    xp[UW] = pltpu.roll(ext[TU], 1, 1)
    face_out[2] = wet_v[...]
    for i in range(2):
        count = xp[(KU + i, *own)]
        safe = jnp.where(count > 0, xp[(DZU + i, *own)], 1.0)
        faces[i] = count
        face_out[i] = count
        coefs[i] = (TIME_STEP * VISC_KV) / (safe * safe)
        push_v[i] = zero
        sum_v[i] = zero

    for c in second:
        c.wait_recv()
    pair = lane // 2
    lev = jnp.where(pair < bank, pair + bank * (lane % 2), n_lev).astype(F32)

    def column(ref, count):
        return jnp.where(lev < count, ref, 0.0)

    u_w = column(rc_w[0], xp[KU, mid, at_w])
    v_w = column(rc_w[1], xp[KV, mid, at_w])
    u_e = column(rc_e[0], xp[KU, mid, at_e])
    v_e = column(rc_e[1], xp[KV, mid, at_e])
    u_last = column(sc_e[0], xp[KU, mid, nx - 1:nx])
    v_zero = column(sc_w[1], xp[KV, mid, FIRST])
    corner_u = jnp.where(lev[FIRST] < xp[KU, at_n, at_w], rc_nw[FIRST, :], 0.0)
    q_e = scaled((u_last + u_e) * (u_last + u_e)) + rp_e[...]
    c_w = scaled((u_w + shift_north(u_w, corner_u)) * (v_w + v_zero))
    hc[0, 0], hc[0, 1] = merged(u_w, q_e)
    hc[1, 0], hc[1, 1] = merged(c_w, v_e)
    corner_p[...] = jnp.where(lev[:SUB] < xp[KV, H - SUB:H, at_e], rc_se[...], 0.0)

    def forces(k, slot):
        kf = k.astype(F32)
        u = jnp.where(kf < faces[0], ub[k], 0.0)
        v = jnp.where(kf < faces[1], vb[k], 0.0)
        p = pp[k]
        b, m = slot_of(k, bank)
        rows_n, rows_s = rr_n[k], rr_s[k]
        u_n = jnp.where(kf < xp[KU, at_n, cols], rows_n[FIRST], 0.0)
        v_n = jnp.where(kf < xp[KV, at_n, cols], rows_n[SECOND], 0.0)
        u_s = jnp.where(kf < xp[KU, at_s, cols], rows_s[FIRST], 0.0)
        v_s = jnp.where(kf < xp[KV, at_s, cols], rows_s[SECOND], 0.0)
        corner_v = turn(corner_p[...], LAST - m - b)[SUB - 1:]
        v_s8 = jnp.broadcast_to(v_s, (SUB, nx))
        v_s_e = shift_east(v_s8, jnp.broadcast_to(corner_v, (SUB, LANES)))[FIRST]
        for i in range(2):
            s_edge[slot, i] = turn(hc[i, b], LANES - m)
        cen_u = shift_west(u, s_edge[slot, 0]) + u
        s_head[slot] = scaled(cen_u * cen_u) + p
        corner = scaled((u + shift_north(u, u_n)) * (v + shift_east(v, s_edge[slot, 1])))
        s_corner[slot] = corner
        corner_s = scaled((u_s + u[first_row]) * (v_s + v_s_e))
        s_side[slot, 0] = corner - shift_south(corner, corner_s)
        cen_v = shift_south(v, v_s) + v
        head_v = scaled(cen_v * cen_v) + p
        edge_v = v[last_row] + v_n
        edge_v = scaled(edge_v * edge_v) + rp_n[k]
        s_side[slot, 1] = (shift_north(head_v, edge_v) - head_v) + corner
        s_now[slot, 0] = u
        s_now[slot, 1] = v

    def solve_down(k, slot):
        kf = k.astype(F32)
        head, corner = s_head[slot], s_corner[slot]
        grad_u = (shift_east(head, s_edge[slot, 0]) - head) + s_side[slot, 0]
        grad_v = s_side[slot, 1] - shift_west(corner, s_edge[slot, 1])
        for f, grad, part, gain in ((0, grad_u, pu, gu), (1, grad_v, pv, gv)):
            count, coef = faces[f], coefs[f]
            wet = kf < count
            up = jnp.where(kf + 1.0 < count, coef, 0.0)
            inv = reduced(1.0 + up + coef * (1.0 - gain[k]))
            gain[k + 1] = up * inv
            pull = jnp.where(wet, grad, 0.0)
            push_v[f] += pull
            low = jnp.where(wet, coef, 0.0)
            part[k + 1] = ((s_now[slot, f] - pull) + low * part[k]) * inv

    def momentum_levels(i, carry):
        k = UN * i
        for d in range(UN):
            forces(jnp.minimum(k + d + 1, n_lev - 1), (d + 1) % UN)
            solve_down(k + d, d)
        return carry

    forces(jnp.int32(0), 0)
    lax.fori_loop(0, n_lev // UN, momentum_levels, 0)

    for f in range(2):
        ext[(FX + f, *own)] = xp[(DZU + f, *own)] * push_v[f] * (-1.0 / TIME_STEP)
        pack(FX + f)
    third = wide_copies(FX, 2)

    def upward(levels):
        def group_of(i, carry):
            levels(n_lev - 1 - i * UE)
            return carry

        lax.fori_loop(0, n_lev // UE, group_of, 0)

    def mix_levels(k0):
        t, s = tb[k0 + 2], sb[k0 + 2]
        for d in range(UE):
            k = k0 - d
            g = gc[k + 1]
            t = tb[k + 1] + g * t
            s = sb[k + 1] + g * s
            tb[k + 1] = t
            sb[k + 1] = s
            gather(t, s, k, bank_ts, tr_s, tr_n)

    upward(mix_levels)
    for i in range(2):
        tc_w[i], tc_e[i] = split_banks(bank_ts.at[i])
    tracer = started([
        remote(tc_w, qc_e, "w"),
        remote(tc_e, qc_w, "e"),
        remote(tr_n, qr_s, "n"),
        remote(tr_s, qr_n, "s"),
    ])

    def rise_levels(k0):
        u, v = pu[k0 + 2], pv[k0 + 2]
        sum_u, sum_w = sum_v[0], sum_v[1]
        for d in range(UE):
            k = k0 - d
            u = pu[k + 1] + gu[k + 1] * u
            v = pv[k + 1] + gv[k + 1] * v
            pu[k + 1] = u
            pv[k + 1] = v
            sum_u += u
            sum_w += v
            b, m = slot_of(k, bank)
            pltpu.store(su_e, turn(u[:, nx - LANES:], m + b + 1), mask=lane == m + b)
            sv_n[k] = v[last_row]
        sum_v[0], sum_v[1] = sum_u, sum_w

    upward(rise_levels)
    fourth = started([remote(su_e, ru_w, "e"), remote(sv_n, rv_s, "n")])

    for c in third:
        c.wait_recv()
    for f in range(2):
        unpack(FX + f)
        xp[BU + f] = jnp.where(xp[KU + f] > 0, dt_sub * ext[FX + f], 0.0)
    xp[BW] = pltpu.roll(xp[BU], 1, 1)
    acc[...] = jnp.zeros(acc.shape, F32)
    norm = 6.0 / (n_sub * (n_sub + 1) * (n_sub + 2))
    line8 = iota((SUB, wide), 0)
    t0 = H // SUB - 1

    def substep(n, lo, hi):
        tide_u, tide_v = tide[0, n], tide[1, n]
        weight = norm * ((n + 1) * (n_sub - n)).astype(F32)

        def finish(t, eta, rolled, rolled_next, u, u_w, v):
            rows = slice(SUB * t, SUB * t + SUB)
            eta_n = jnp.where(line8 == SUB - 1, rolled_next, rolled)
            eta_e = pltpu.roll(eta, wide - 1, 1)
            eta_w = pltpu.roll(eta, 1, 1)
            xp[UW, rows] = u_w + (xp[GW, rows] * (tide_u + (eta_w - eta)) + xp[BW, rows])
            u_new = u + (xp[GU, rows] * (tide_u + (eta - eta_e)) + xp[BU, rows])
            v_new = v + (xp[GV, rows] * (tide_v + (eta - eta_n)) + xp[BV, rows])
            ext[TU, rows] = u_new
            ext[TV, rows] = v_new
            if t0 <= t < (H + ny) // SUB:
                at = slice(SUB * (t - t0), SUB * (t - t0) + SUB)
                acc[0, at] += weight * u_new
                acc[1, at, :nx] += weight * v_new[:, :nx]

        last = None
        v_below = jnp.zeros((SUB, wide), F32)
        for t in range(lo, hi):
            rows = slice(SUB * t, SUB * t + SUB)
            u, u_w, v = ext[TU, rows], xp[UW, rows], ext[TV, rows]
            v_roll = pltpu.roll(v, 1, 0)
            v_s = jnp.where(line8 == 0, v_below, v_roll)
            v_below = v_roll
            eta = ext[ETA, rows] - xp[WD, rows] * ((u - u_w) + (v - v_s))
            ext[ETA, rows] = eta
            rolled = pltpu.roll(eta, SUB - 1, 0)
            if last is not None:
                eta_b, rolled_b, *face_b = last
                finish(t - 1, eta_b, rolled_b, rolled, *face_b)
            last = (eta, rolled, u, u_w, v)
        finish(hi - 1, eta, rolled, rolled, u, u_w, v)

    edge_tiles = H // SUB
    for e in range(edge_tiles, 0, -1):
        begin = max(0, n_sub + 1 - SUB * e) if e < edge_tiles else 0
        end = n_sub + 1 - SUB * (e - 1) if e > 1 else n_sub
        span = (edge_tiles - e, whole // SUB - edge_tiles + e)

        def two(i, carry, begin=begin, span=span):
            substep(begin + 2 * i, *span)
            substep(begin + 2 * i + 1, *span)
            return carry

        lax.fori_loop(0, (end - begin) // 2, two, 0)
        if (end - begin) % 2:
            substep(jnp.int32(end - 1), *span)

    for i in range(3):
        bar_out[i] = ext[(ETA + i, *own)]

    def safe_depth(f, rows, lanes):
        depth = xp[KU + f, rows, lanes] * xp[DZU + f, rows, lanes]
        return jnp.where(depth > 0, depth, 1.0)

    inner = slice(SUB, SUB + ny)
    for f in range(2):
        corr_out[f] = (acc[f, inner, cols] - xp[DZU + f, mid, cols] * sum_v[f]) / safe_depth(f, mid, cols)
    for c in fourth:
        c.wait_recv()
    star = ru_w[...]
    fix = (acc[0, inner, at_w] - xp[DZU, mid, at_w] * jnp.sum(star, axis=1, keepdims=True)) / safe_depth(0, mid, at_w)
    u_c = column(star + fix, xp[KU, mid, at_w])
    star = rv_s[...]
    fix = (acc[1, SUB - 1:SUB, cols] - xp[DZV, at_s, cols] * jnp.sum(star, axis=0)) / safe_depth(1, at_s, cols)
    levels = iota(star.shape, 0).astype(F32)
    vcs_out[...] = jnp.where(levels < xp[KV, at_s, cols][None], star + fix[None], 0.0)
    for c in tracer:
        c.wait_recv()
    for i in range(2):
        halo_out[i, 0], halo_out[i, 1] = merged((0.5 * TIME_STEP) * u_c * (qc_w[i] + tc_w[i]), qc_e[i])
    trow_n_out[...] = qr_n[...]
    trow_s_out[...] = qr_s[...]
    for c in second + third + tracer + fourth:
        c.wait_send()


def last_kernel(us, vs, tm, sm, bar, corr, faces, vcs, halo, trow_n, trow_s,
                eta_out, tu_out, tv_out, u_out, v_out, t_out, s_out,
                new_u, new_v, new_t, new_s, flux, rest, turned, bar_sem, out_sem, *, bank):
    n_lev = u_out.shape[0]
    planes = [pltpu.make_async_copy(bar.at[i], ref, bar_sem.at[i]) for i, ref in enumerate((eta_out, tu_out, tv_out))]
    for c in planes:
        c.start()

    def fluxes(k, slot):
        kf = k.astype(F32)
        u = jnp.where(kf < faces[0], us[k + 1] + corr[0], 0.0)
        v = jnp.where(kf < faces[1], vs[k + 1] + corr[1], 0.0)
        new_u[k] = u
        new_v[k] = v
        u = (0.5 * TIME_STEP) * u
        v = (0.5 * TIME_STEP) * v
        v_s = (0.5 * TIME_STEP) * vcs[k]
        rows_n, rows_s = trow_n[k], trow_s[k]
        b, m = slot_of(k, bank)
        for a, src in ((0, tm), (1, sm)):
            x = src[k + 1]
            turned[slot, a] = turn(halo[a, b], LANES - m)
            flux_x = u * (x + shift_east(x, turned[slot, a]))
            flux_y = v * (x + shift_north(x, rows_n[a:a + 1]))
            edge_y = v_s * (rows_s[a:a + 1] + x[FIRST])
            flux[slot, a] = flux_x
            rest[slot, a] = (x - flux_x) - (flux_y - shift_south(flux_y, edge_y))

    def finish(k, slot):
        wet = k.astype(F32) < faces[2]
        for a, dst in ((0, new_t), (1, new_s)):
            moved = shift_west(flux[slot, a], turned[slot, a])
            dst[k] = jnp.where(wet, rest[slot, a] + moved, 0.0)

    def copies(c):
        return [pltpu.make_async_copy(src.at[pl.ds(c * KB, KB)], dst.at[pl.ds(c * KB, KB)], out_sem.at[i, c])
                for i, (src, dst) in enumerate(((new_u, u_out), (new_v, v_out), (new_t, t_out), (new_s, s_out)))]

    def chunk(c, carry):
        for d in range(KB):
            fluxes(jnp.minimum(c * KB + d + 1, n_lev - 1), (d + 1) % KB)
            finish(c * KB + d, d)
        for copy in copies(c):
            copy.start()
        return carry

    n_copy = n_lev // KB
    fluxes(jnp.int32(0), 0)
    lax.fori_loop(0, n_copy, chunk, 0)
    for c in range(n_copy):
        for copy in copies(c):
            copy.wait()
    for c in planes:
        c.wait()


def solution(mesh):
    n_cols, n_rows = mesh.shape["col"], mesh.shape["row"]

    def local_step(vel_u, vel_v, value_a11, salinity, sea_level, trans_u, trans_v, bathymetry, kmt_levels, tide_force):
        n_lev, ny, nx = vel_u.shape
        whole, wide = ny + 2 * H, nx + LANES
        n_chunk, bank = n_lev // CH, (n_lev + 1) // 2
        hbm_spec = pl.BlockSpec(memory_space=pltpu.HBM)
        vmem_spec = pl.BlockSpec(memory_space=pltpu.VMEM)
        cube = (n_lev, ny, nx)
        deep = (n_lev + 2, ny, nx)
        column, pair_c, rows1, rows2 = (ny, LANES), (2, ny, LANES), (n_lev, 1, nx), (n_lev, 2, nx)
        banks, two, small, both = (2, 2, ny, LANES), (2, ny, nx), (SUB, LANES), (UN, 2, ny, nx)

        edges = (UN, 2, ny, LANES)

        def sds(*shape):
            return jax.ShapeDtypeStruct(shape, F32)

        def bufs(*shapes):
            return [pltpu.VMEM(shape, F32) for shape in shapes]

        def sems(*shape):
            return pltpu.SemaphoreType.DMA(shape)

        passed = [(3, ny, nx), two, (3, ny, nx), rows1, banks, rows2, rows2]
        *cubes, bar, corr, face, vcs, halo, trow_n, trow_s = pl.pallas_call(
            functools.partial(main_kernel, n_rows, n_cols),
            out_shape=bufs(*[deep] * 4, *passed),
            in_specs=[hbm_spec] * 9 + [pl.BlockSpec(memory_space=pltpu.SMEM)],
            out_specs=[vmem_spec] * (4 + len(passed)),
            scratch_shapes=[
                pltpu.VMEM((ny, nx), jnp.int32),
                *bufs((7, whole, wide), (12, whole, wide), (2, ny + SUB, wide)),
                *bufs(*[(7, 3 * SUB, LANES)] * 2, *[(7, 2 * SUB, LANES)] * 2, *[(7, SUB, LANES)] * 4),
                *bufs(cube, cube, *[deep] * 3, cube, *[(ny, nx)] * 4, two, two, two, two, both, (UN, ny, nx), (UN, ny, nx), both, edges),
                *bufs(banks, banks, pair_c, pair_c, column, pair_c, pair_c, column, small, small, banks, small),
                *bufs(rows2, rows2, rows1, rows2, rows2, rows1),
                *bufs(pair_c, pair_c, rows2, rows2, pair_c, pair_c, rows2, rows2, column, rows1, column, rows1),
                sems(5), sems(4, n_chunk), sems(30), sems(30),
            ],
            compiler_params=pltpu.CompilerParams(collective_id=0, has_side_effects=True, vmem_limit_bytes=44 * 2**20),
        )(kmt_levels, bathymetry, sea_level, trans_u, trans_v, vel_u, vel_v, value_a11, salinity, tide_force.T)

        return pl.pallas_call(
            functools.partial(last_kernel, bank=bank),
            out_shape=[sds(ny, nx)] * 3 + [sds(*cube)] * 4,
            in_specs=[vmem_spec] * (4 + len(passed)),
            out_specs=[hbm_spec] * 7,
            scratch_shapes=[*bufs(*[cube] * 4, both, both, edges), sems(3), sems(4, n_lev // KB)],
            compiler_params=pltpu.CompilerParams(vmem_limit_bytes=18 * 2**20),
        )(*cubes, bar, corr, face, vcs, halo, trow_n, trow_s)

    spec_cube = P(None, "row", "col")
    spec_plane = P("row", "col")
    return jax.shard_map(local_step, mesh=mesh, in_specs=(spec_cube,) * 4 + (spec_plane,) * 5 + (P(None, None),),
                         out_specs=(spec_plane,) * 3 + (spec_cube,) * 4, check_vma=False)
```

```python
import functools

import jax
import jax.numpy as jnp
from jax import lax
from jax.experimental import pallas as pl
from jax.experimental.pallas import tpu as pltpu
from jax.sharding import PartitionSpec as P

TIME_STEP = 4.0
ALPHA_T = 0.02
BETA_S = 0.015
VISC_KV = 0.001
DIFF_KT = 0.0005
MESH = pl.DeviceIdType.MESH
H = 32
CH = 15
UN = 5
UE = 15
KB = 5
SUB, LANES = 8, 128
LAST = LANES - 1
F32 = jnp.float32
HEAD = 0.25 * TIME_STEP
KMT, DEPTH, ETA, TU, TV, FX, FY = range(7)
KU, KV, DZU, DZV, GU, GV, BU, BV, WD, GW, BW, UW = range(12)
FIRST = slice(0, 1)


def iota(shape, axis):
    return lax.broadcasted_iota(jnp.int32, shape, axis)


def reduced(x):
    return pl.reciprocal(x, approx=False)


def scaled(x):
    return x if HEAD == 1.0 else HEAD * x


def lane_of(x):
    return iota(x.shape, 1)


def slot_of(k, bank):
    b = int(k >= bank) if isinstance(k, int) else (k >= bank).astype(jnp.int32)
    return b, 2 * (k - b * bank)


def real(k):
    return float(k) if isinstance(k, int) else k.astype(F32)


def turn(x, n):
    return pltpu.roll(x, n % LANES if isinstance(n, int) else n, 1)


def shift_east(x, halo):
    left, right = turn(x[:, :LANES], -1), turn(x[:, LANES:], -1)
    edge = lane_of(left) == LAST
    return jnp.concatenate([jnp.where(edge, right, left), jnp.where(edge, halo, right)], axis=1)


def shift_west(x, halo):
    left, right = turn(x[:, :LANES], 1), turn(x[:, LANES:], 1)
    edge = lane_of(left) == 0
    return jnp.concatenate([jnp.where(edge, halo, left), jnp.where(edge, left, right)], axis=1)


def tiles_of(x):
    return [x[SUB * t:SUB * t + SUB] for t in range(x.shape[0] // SUB)]


def shift_north(x, halo):
    rolled = [pltpu.roll(t, SUB - 1, 0) for t in tiles_of(x)]
    edge = iota(rolled[0].shape, 0) == SUB - 1
    rolled.append(jnp.broadcast_to(halo, rolled[0].shape))
    return jnp.concatenate([jnp.where(edge, b, a) for a, b in zip(rolled[:-1], rolled[1:])], axis=0)


def shift_south(x, halo):
    rolled = [pltpu.roll(t, 1, 0) for t in tiles_of(x)]
    edge = iota(rolled[0].shape, 0) == 0
    rolled.insert(0, jnp.broadcast_to(halo, rolled[0].shape))
    return jnp.concatenate([jnp.where(edge, a, b) for a, b in zip(rolled[:-1], rolled[1:])], axis=0)


def merged(west, east):
    even = lane_of(west) % 2 == 0
    back = turn(east, -1)
    return jnp.where(even, west, back), turn(jnp.where(even, back, west), -1)


def main_kernel(n_rows, n_cols,
                kmt_in, bat_in, eta_in, tu_in, tv_in, u_in, v_in, t_in, s_in, tide,
                pu, pv, tb, sb, bar_out, corr_out, face_out, vcs_out,
                halo_out, trow_n_out, trow_s_out,
                kmt_v, ext, xp, acc, pk_w, pk_e, r_e, r_w, r_ne, r_nw, r_se, r_sw,
                ub, vb, gc, gu, gv, pp, wet_v, dz_v, cc_v, cum_v, faces, coefs, push_v, sum_v, s_now, s_low, s_head, s_corner, s_side, s_edge, row_h, corner_r,
                bank_uv, bank_ts, sc_w, sc_e, sp_w, rc_e, rc_w, rp_e, rc_nw, rc_se, hc, corner_p,
                sr_n, sr_s, sp_s, rr_n, rr_s, rp_n,
                tc_w, tc_e, tr_n, tr_s, qc_e, qc_w, qr_n, qr_s, su_e, sv_n, ru_w, rv_s,
                plane_sem, in_sem, send_sem, recv_sem):
    n_sub = tide.shape[1]
    n_lev = u_in.shape[0]
    n_chunk = n_lev // CH
    bank, n_row = (n_lev + 1) // 2, sp_s.shape[0]
    ny, nx = kmt_in.shape
    dt_sub = TIME_STEP / n_sub
    col, row = lax.axis_index("col"), lax.axis_index("row")
    east, west = lax.rem(col + 1, n_cols), lax.rem(col + n_cols - 1, n_cols)
    north, south = lax.rem(row + 1, n_rows), lax.rem(row + n_rows - 1, n_rows)
    where_to = {"n": (col, north), "s": (col, south), "e": (east, row), "w": (west, row),
                "ne": (east, north), "nw": (west, north), "se": (east, south), "sw": (west, south)}
    own = (pl.ds(H, ny), pl.ds(0, nx))
    mid, cols = slice(H, H + ny), slice(0, nx)
    at_n, at_s = slice(H + ny, H + ny + 1), slice(H - 1, H)
    whole, wide = ny + 2 * H, nx + LANES
    at_w, at_e = slice(wide - 1, wide), slice(nx, nx + 1)
    first_row, last_row = FIRST, slice(ny - 1, ny)

    planes = [pltpu.make_async_copy(kmt_in, kmt_v, plane_sem.at[KMT])]
    for i, ref in ((DEPTH, bat_in), (ETA, eta_in), (TU, tu_in), (TV, tv_in)):
        planes.append(pltpu.make_async_copy(ref, ext.at[(i, *own)], plane_sem.at[i]))
    for c in planes:
        c.start()

    def load(a, c):
        src, dst, off = ((u_in, ub, 0), (v_in, vb, 0), (t_in, tb, 1), (s_in, sb, 1))[a]
        return pltpu.make_async_copy(src.at[pl.ds(c * CH, CH)], dst.at[pl.ds(c * CH + off, CH)], in_sem.at[a, c])

    barrier = pltpu.get_barrier_semaphore()
    for c_id, r_id in where_to.values():
        pl.semaphore_signal(barrier, inc=1, device_id={"col": c_id, "row": r_id}, device_id_type=MESH)

    used = []

    def remote(src, dst, to):
        c_id, r_id = where_to[to]
        i = len(used)
        used.append(i)
        copy = pltpu.make_async_remote_copy(src_ref=src, dst_ref=dst, send_sem=send_sem.at[i], recv_sem=recv_sem.at[i],
                                            device_id={"col": c_id, "row": r_id}, device_id_type=MESH)
        return copy, to[0]

    below_wall, above_wall = row < n_rows - 1, row > 0

    def sends(copies, act):
        for copy, to in copies:
            if to in "ns":
                pl.when(below_wall if to == "n" else above_wall)(functools.partial(act, copy))
            else:
                act(copy)

    def started(copies):
        sends(copies, lambda c: c.start())
        return copies

    def sent(copies):
        sends(copies, lambda c: c.wait_send())

    def received(copies):
        for copy, to in copies:
            if to in "ns":
                pl.when(above_wall if to == "n" else below_wall)(copy.wait_recv)
            else:
                copy.wait_recv()

    def wide_copies(p0, n):
        ps = pl.ds(p0, n)
        low, mids, high = pl.ds(0, 2 * SUB), pl.ds(0, SUB), pl.ds(2 * SUB, SUB)
        return started([
            remote(ext.at[ps, pl.ds(H, H), pl.ds(0, nx)], ext.at[ps, pl.ds(H + ny, H), pl.ds(0, nx)], "s"),
            remote(ext.at[ps, pl.ds(ny, H), pl.ds(0, nx)], ext.at[ps, pl.ds(0, H), pl.ds(0, nx)], "n"),
            remote(pk_w.at[ps, low], r_e.at[ps], "w"),
            remote(pk_e.at[ps, low], r_w.at[ps], "e"),
            remote(pk_w.at[ps, mids], r_ne.at[ps], "sw"),
            remote(pk_e.at[ps, mids], r_nw.at[ps], "se"),
            remote(pk_w.at[ps, high], r_se.at[ps], "nw"),
            remote(pk_e.at[ps, high], r_sw.at[ps], "ne"),
        ])

    group = iota((SUB, LANES), 1) // H
    n_groups = LANES // H

    def pack(p):
        x = ext[(p, *own)]
        for ref, tile, g0 in ((pk_w, x[:, :LANES], 0), (pk_e, x[:, nx - LANES:], n_groups - 1)):
            for at, first, count in ((0, 0, 4), (1, 4, 2), (2, 2, 4)):
                total = jnp.zeros((SUB, LANES), F32)
                for q in range(count):
                    rows = tile[SUB * (first + q):SUB * (first + q) + SUB]
                    rows = turn(rows, H * (q - g0)) if q != g0 else rows
                    total = jnp.where(group == q, rows, total)
                ref[p, SUB * at:SUB * at + SUB, :] = total

    def unpack(p):
        edge = H // SUB
        for t in range(whole // SUB):
            if t < edge:
                e_tile, w_tile, q = r_se[p], r_sw[p], t
            elif t < (H + ny) // SUB:
                rows = slice(SUB * ((t - edge) // n_groups), SUB * ((t - edge) // n_groups) + SUB)
                e_tile, w_tile, q = r_e[p, rows], r_w[p, rows], (t - edge) % n_groups
            else:
                e_tile, w_tile, q = r_ne[p], r_nw[p], t - (H + ny) // SUB
            e_tile = turn(e_tile, -H * q) if q else e_tile
            w_tile = turn(w_tile, H * (n_groups - 1 - q)) if q != n_groups - 1 else w_tile
            side = jnp.where(group == 0, e_tile, jnp.where(group == n_groups - 1, w_tile, 0.0))
            ext[p, SUB * t:SUB * t + SUB, nx:] = side

    for c in planes:
        c.wait()
    for a in (0, 2):
        for c in range(n_chunk):
            load(a, c).start()
            load(a + 1, c).start()
    kmt = kmt_v[...].astype(F32)
    ext[(KMT, *own)] = kmt
    for p in range(FX):
        pack(p)
    pl.semaphore_wait(barrier, len(where_to))
    first = wide_copies(KMT, 2)

    zero = jnp.zeros((ny, nx), F32)
    for ref in (bank_uv, bank_ts, sp_w, su_e):
        ref[...] = jnp.zeros(ref.shape, F32)
    lane = iota((ny, LANES), 1)
    even = lane % 2 == 0

    def both_edges(x):
        return jnp.where(lane < LANES // 2, x[:, :LANES], x[:, nx - LANES:])

    def gather(x, y, k, banks, rows_s, rows_n):
        b, m = slot_of(k, bank)
        here = ((lane + 1 - m) & LAST) < 2
        pltpu.store(banks.at[0, b], turn(both_edges(x), m), mask=here)
        pltpu.store(banks.at[1, b], turn(both_edges(y), m), mask=here)
        here = pl.ds(k, 1)
        rows_s[0, here] = x[first_row]
        rows_s[1, here] = y[first_row]
        rows_n[0, here] = x[last_row]
        rows_n[1, here] = y[last_row]

    def in_chunks(arrays, levels, step):
        def chunk(c, carry):
            for a in arrays:
                load(a, c).wait()

            def group_of(i, carry):
                levels(c * CH + i * step)
                return carry

            return lax.fori_loop(0, CH // step, group_of, carry)

        lax.fori_loop(0, n_chunk, chunk, 0)

    def edge_levels(k0):
        for d in range(UE):
            gather(ub[k0 + d], vb[k0 + d], k0 + d, bank_uv, sr_s, sr_n)

    in_chunks((0, 1), edge_levels, UE)

    def split_banks(banks):
        a, b = banks[0], turn(banks[1], 1)
        return jnp.where(even, a, b), turn(jnp.where(even, b, a), 1)

    for i in range(2):
        sc_w[i], sc_e[i] = split_banks(bank_uv.at[i])
    second = started([
        remote(sc_w, rc_e, "w"),
        remote(sc_e, rc_w, "e"),
        remote(sr_n, rr_s, "n"),
        remote(sr_s, rr_n, "s"),
        remote(sc_e.at[0, pl.ds(0, SUB)], rc_nw, "se"),
        remote(sc_w.at[1, pl.ds(ny - SUB, SUB)], rc_se, "nw"),
    ])

    dz = ext[(DEPTH, *own)] / jnp.maximum(kmt, 1.0)
    safe = jnp.where(kmt > 0, dz, 1.0)
    wet_v[...] = kmt
    dz_v[...] = TIME_STEP * dz
    cc_v[...] = (TIME_STEP * DIFF_KT) / (safe * safe)
    cum_v[...] = zero
    for ref in (tb, sb, pu, pv):
        ref[0] = zero
        ref[n_lev + 1] = zero
    for ref in (gc, gu, gv):
        ref[0] = zero + 1.0

    def pressure_levels(k0):
        cum = cum_v[...]
        for d in range(UE):
            k = k0 + d
            dens = BETA_S * (sb[k + 1] - 1.0) - ALPHA_T * (tb[k + 1] - 1.0)
            dens = jnp.where(k.astype(F32) < wet_v[...], dens, 0.0)
            cum = cum + dens
            pres = dz_v[...] * (cum - 0.5 * dens)
            pp[k] = pres
            b, m = slot_of(k, bank)
            pltpu.store(sp_w, turn(pres[:, :LANES], m + b), mask=lane == m + b)
            sp_s[pl.ds(k, 1)] = pres[first_row]
        cum_v[...] = cum

    in_chunks((2, 3), pressure_levels, UE)
    last_edges = started([remote(sp_w, rp_e, "w"), remote(sp_s, rp_n, "s")])

    def down_levels(i, carry):
        k0 = i * UN
        g, t_up, s_up = gc[k0], tb[k0], sb[k0]
        wet = k0.astype(F32) < wet_v[...]
        for d in range(UN):
            k = k0 + d
            below = (k + 1).astype(F32) < wet_v[...]
            coef = cc_v[...]
            up = jnp.where(below, coef, 0.0)
            inv = reduced(1.0 + up + coef * (1.0 - g))
            g = up * inv
            t_up = jnp.where(wet, (tb[k + 1] + coef * t_up) * inv, 0.0)
            s_up = jnp.where(wet, (sb[k + 1] + coef * s_up) * inv, 0.0)
            gc[k + 1] = g
            tb[k + 1] = t_up
            sb[k + 1] = s_up
            wet = below
        return carry

    lax.fori_loop(0, n_lev // UN, down_levels, 0)

    sent(first)
    received(first)
    for p in (KMT, DEPTH):
        unpack(p)
    line = iota((whole, wide), 0)
    seen = ((line >= H) | (row > 0)) & ((line < H + ny) | (row < n_rows - 1))
    kx = jnp.where(seen, ext[KMT], 0.0)
    ext[KMT] = kx
    dzx = jnp.where(seen, ext[DEPTH], 0.0) / jnp.maximum(kx, 1.0)
    ku = jnp.minimum(kx, pltpu.roll(kx, wide - 1, 1))
    kv = jnp.minimum(kx, pltpu.roll(kx, whole - 1, 0))
    dzu = 0.5 * (dzx + pltpu.roll(dzx, wide - 1, 1))
    dzv = 0.5 * (dzx + pltpu.roll(dzx, whole - 1, 0))
    xp[KU] = ku
    xp[KV] = kv
    xp[DZU] = dzu
    xp[DZV] = dzv
    xp[GU] = jnp.where(ku > 0, dt_sub * (ku * dzu), 0.0)
    xp[GV] = jnp.where(kv > 0, dt_sub * (kv * dzv), 0.0)
    xp[WD] = jnp.where(kx > 0, dt_sub, 0.0)
    xp[GW] = pltpu.roll(xp[GU], 1, 1)
    face_out[2] = wet_v[...]
    for i in range(2):
        count = xp[(KU + i, *own)]
        safe = jnp.where(count > 0, xp[(DZU + i, *own)], 1.0)
        faces[i] = count
        face_out[i] = count
        coefs[i] = (TIME_STEP * VISC_KV) / (safe * safe)
        push_v[i] = zero
        sum_v[i] = zero

    received(second)
    pair = lane // 2
    lev = jnp.where(pair < bank, pair + bank * (lane % 2), n_lev).astype(F32)

    def column(ref, count):
        return jnp.where(lev < count, ref, 0.0)

    u_w = column(rc_w[0], xp[KU, mid, at_w])
    v_w = column(rc_w[1], xp[KV, mid, at_w])
    u_e = column(rc_e[0], xp[KU, mid, at_e])
    v_e = column(rc_e[1], xp[KV, mid, at_e])
    u_last = column(sc_e[0], xp[KU, mid, nx - 1:nx])
    v_zero = column(sc_w[1], xp[KV, mid, FIRST])
    corner_u = jnp.where(lev[FIRST] < xp[KU, at_n, at_w], rc_nw[FIRST, :], 0.0)
    q_e = scaled((u_last + u_e) * (u_last + u_e))
    c_w = scaled((u_w + shift_north(u_w, corner_u)) * (v_w + v_zero))
    hc[1, 0], hc[1, 1] = merged(c_w, v_e)
    corner_p[...] = jnp.where(lev[:SUB] < xp[KV, H - SUB:H, at_e], rc_se[...], 0.0)

    def corner_levels(i, carry):
        for d in range(UE):
            b, m = slot_of(i * UE + d, bank)
            corner_r[pl.ds(i * UE + d, 1)] = turn(corner_p[...], LAST - m - b)[SUB - 1:]
        return carry

    lax.fori_loop(0, n_lev // UE, corner_levels, 0)
    row_lev = iota((n_row, nx), 0).astype(F32)

    def row_of(x, f, at):
        return jnp.where(row_lev < xp[KU + f, at, cols], x, 0.0)

    v_s = row_of(rr_s[1], 1, at_s)
    v_last = row_of(sr_n[1], 1, slice(H + ny - 1, H + ny))
    v_n = row_of(rr_n[1], 1, at_n)
    row_h[0] = row_of(rr_n[0], 0, at_n)
    row_h[1] = scaled((row_of(rr_s[0], 0, at_s) + row_of(sr_s[0], 0, slice(H, H + 1))) * (v_s + shift_east(v_s, corner_r[...])))
    row_h[2] = v_s
    row_h[3] = scaled((v_last + v_n) * (v_last + v_n))
    received(last_edges)
    state = wide_copies(ETA, 3)
    hc[0, 0], hc[0, 1] = merged(u_w, q_e + rp_e[...])
    row_h[3] += jnp.where(below_wall, rp_n[...], 0.0)

    def forces(k, slot):
        kf = real(k)
        k = k if isinstance(k, int) else jnp.minimum(k, n_lev - 1)
        masked = []
        for f, ref in ((0, ub), (1, vb)):
            wet = kf < faces[f]
            masked.append(jnp.where(wet, ref[k], 0.0))
            s_now[slot, f] = masked[f]
            s_low[slot, f] = jnp.where(wet, coefs[f], 0.0)
        u, v = masked
        p = pp[k]
        b, m = slot_of(k, bank)
        u_n, corner_s, v_s, edge_v = [row_h[i, pl.ds(k, 1)] for i in range(4)]
        for i in range(2):
            s_edge[slot, i] = turn(hc[i, b], LANES - m)
        cen_u = shift_west(u, s_edge[slot, 0]) + u
        s_head[slot] = scaled(cen_u * cen_u) + p
        corner = scaled((u + shift_north(u, u_n)) * (v + shift_east(v, s_edge[slot, 1])))
        s_corner[slot] = corner
        s_side[slot, 0] = corner - shift_south(corner, corner_s)
        cen_v = shift_south(v, v_s) + v
        head_v = scaled(cen_v * cen_v) + p
        s_side[slot, 1] = (shift_north(head_v, edge_v) - head_v) + corner

    def solve_down(k, slot, below):
        kf = k.astype(F32)
        head, corner = s_head[slot], s_corner[slot]
        grad_u = (shift_east(head, s_edge[slot, 0]) - head) + s_side[slot, 0]
        grad_v = s_side[slot, 1] - shift_west(corner, s_edge[slot, 1])
        for f, grad, part, gain in ((0, grad_u, pu, gu), (1, grad_v, pv, gv)):
            low, up = s_low[slot, f], s_low[below, f]
            inv = reduced(1.0 + up + low * (1.0 - gain[k]))
            gain[k + 1] = up * inv
            pull = jnp.where(kf < faces[f], grad, 0.0)
            push_v[f] += pull
            part[k + 1] = ((s_now[slot, f] - pull) + low * part[k]) * inv

    def momentum_levels(i, carry):
        k = UN * i
        for d in range(UN):
            forces(k + d + 1, (d + 1) % UN)
            solve_down(k + d, d, (d + 1) % UN)
        return carry

    forces(0, 0)
    lax.fori_loop(0, n_lev // UN, momentum_levels, 0)

    for f in range(2):
        ext[(FX + f, *own)] = xp[(DZU + f, *own)] * push_v[f] * (-1.0 / TIME_STEP)
        pack(FX + f)
    third = wide_copies(FX, 2)

    def upward(levels):
        def group_of(i, carry):
            levels(n_lev - 1 - i * UE)
            return carry

        lax.fori_loop(0, n_lev // UE, group_of, 0)

    def mix_levels(k0):
        t, s = tb[k0 + 2], sb[k0 + 2]
        for d in range(UE):
            k = k0 - d
            g = gc[k + 1]
            t = tb[k + 1] + g * t
            s = sb[k + 1] + g * s
            tb[k + 1] = t
            sb[k + 1] = s
            gather(t, s, k, bank_ts, tr_s, tr_n)

    upward(mix_levels)
    for i in range(2):
        tc_w[i], tc_e[i] = split_banks(bank_ts.at[i])
    tracer = started([
        remote(tc_w, qc_e, "w"),
        remote(tc_e, qc_w, "e"),
        remote(tr_n, qr_s, "n"),
        remote(tr_s, qr_n, "s"),
    ])

    def rise_levels(k0):
        u, v = pu[k0 + 2], pv[k0 + 2]
        sum_u, sum_w = sum_v[0], sum_v[1]
        for d in range(UE):
            k = k0 - d
            u = pu[k + 1] + gu[k + 1] * u
            v = pv[k + 1] + gv[k + 1] * v
            pu[k + 1] = u
            pv[k + 1] = v
            sum_u += u
            sum_w += v
            b, m = slot_of(k, bank)
            pltpu.store(su_e, turn(u[:, nx - LANES:], m + b + 1), mask=lane == m + b)
            sv_n[pl.ds(k, 1)] = v[last_row]
        sum_v[0], sum_v[1] = sum_u, sum_w

    upward(rise_levels)
    fourth = started([remote(su_e, ru_w, "e"), remote(sv_n, rv_s, "n")])

    sent(state)
    received(state)
    for p in (ETA, TU, TV):
        unpack(p)
        ext[p] = jnp.where((xp[WD] if p == ETA else xp[KU + p - TU]) > 0, ext[p], 0.0)
    xp[UW] = pltpu.roll(ext[TU], 1, 1)
    received(third)
    for f in range(2):
        unpack(FX + f)
        xp[BU + f] = jnp.where(xp[KU + f] > 0, dt_sub * ext[FX + f], 0.0)
    xp[BW] = pltpu.roll(xp[BU], 1, 1)
    acc[...] = jnp.zeros(acc.shape, F32)
    norm = 6.0 / (n_sub * (n_sub + 1) * (n_sub + 2))
    line8 = iota((SUB, wide), 0)
    t0 = H // SUB - 1

    def substep(n, lo, hi):
        tide_u, tide_v = tide[0, n], tide[1, n]
        weight = norm * ((n + 1) * (n_sub - n)).astype(F32)

        def finish(t, eta, rolled, rolled_next, u, u_w, v):
            rows = slice(SUB * t, SUB * t + SUB)
            eta_n = jnp.where(line8 == SUB - 1, rolled_next, rolled)
            eta_e = pltpu.roll(eta, wide - 1, 1)
            eta_w = pltpu.roll(eta, 1, 1)
            xp[UW, rows] = u_w + (xp[GW, rows] * (tide_u + (eta_w - eta)) + xp[BW, rows])
            u_new = u + (xp[GU, rows] * (tide_u + (eta - eta_e)) + xp[BU, rows])
            v_new = v + (xp[GV, rows] * (tide_v + (eta - eta_n)) + xp[BV, rows])
            ext[TU, rows] = u_new
            ext[TV, rows] = v_new
            if t0 <= t < (H + ny) // SUB:
                at = slice(SUB * (t - t0), SUB * (t - t0) + SUB)
                acc[0, at] += weight * u_new
                acc[1, at, :nx] += weight * v_new[:, :nx]

        last = None
        v_below = jnp.zeros((SUB, wide), F32)
        for t in range(lo, hi):
            rows = slice(SUB * t, SUB * t + SUB)
            u, u_w, v = ext[TU, rows], xp[UW, rows], ext[TV, rows]
            v_roll = pltpu.roll(v, 1, 0)
            v_s = jnp.where(line8 == 0, v_below, v_roll)
            v_below = v_roll
            eta = ext[ETA, rows] - xp[WD, rows] * ((u - u_w) + (v - v_s))
            ext[ETA, rows] = eta
            rolled = pltpu.roll(eta, SUB - 1, 0)
            if last is not None:
                eta_b, rolled_b, *face_b = last
                finish(t - 1, eta_b, rolled_b, rolled, *face_b)
            last = (eta, rolled, u, u_w, v)
        finish(hi - 1, eta, rolled, rolled, u, u_w, v)

    edge_tiles = H // SUB
    for e in range(edge_tiles, 0, -1):
        begin = max(0, n_sub + 1 - SUB * e) if e < edge_tiles else 0
        end = n_sub + 1 - SUB * (e - 1) if e > 1 else n_sub
        span = (edge_tiles - e, whole // SUB - edge_tiles + e)

        def two(i, carry, begin=begin, span=span):
            substep(begin + 2 * i, *span)
            substep(begin + 2 * i + 1, *span)
            return carry

        lax.fori_loop(0, (end - begin) // 2, two, 0)
        if (end - begin) % 2:
            substep(jnp.int32(end - 1), *span)

    for i in range(3):
        bar_out[i] = ext[(ETA + i, *own)]

    def safe_depth(f, rows, lanes):
        depth = xp[KU + f, rows, lanes] * xp[DZU + f, rows, lanes]
        return jnp.where(depth > 0, depth, 1.0)

    inner = slice(SUB, SUB + ny)
    for f in range(2):
        corr_out[f] = (acc[f, inner, cols] - xp[DZU + f, mid, cols] * sum_v[f]) / safe_depth(f, mid, cols)
    received(fourth)
    star = ru_w[...]
    fix = (acc[0, inner, at_w] - xp[DZU, mid, at_w] * jnp.sum(star, axis=1, keepdims=True)) / safe_depth(0, mid, at_w)
    u_c = column(star + fix, xp[KU, mid, at_w])
    star = row_of(rv_s[...], 1, at_s)
    total = jnp.sum(star, axis=0, keepdims=True)
    fix = (acc[1, SUB - 1:SUB, cols] - xp[DZV, at_s, cols] * total) / safe_depth(1, at_s, cols)
    vcs_out[...] = row_of(star + fix, 1, at_s)
    received(tracer)
    for i in range(2):
        halo_out[i, 0], halo_out[i, 1] = merged((0.5 * TIME_STEP) * u_c * (qc_w[i] + tc_w[i]), qc_e[i])
    trow_n_out[...] = jnp.where(below_wall, qr_n[...], 0.0)
    trow_s_out[...] = jnp.where(above_wall, qr_s[...], 0.0)
    sent(second + last_edges + third + tracer + fourth)


def last_kernel(us, vs, tm, sm, bar, corr, faces, vcs, halo, trow_n, trow_s,
                eta_out, tu_out, tv_out, u_out, v_out, t_out, s_out,
                new_u, new_v, new_t, new_s, flux, rest, turned, bar_sem, out_sem, *, bank):
    n_lev = u_out.shape[0]
    planes = [pltpu.make_async_copy(bar.at[i], ref, bar_sem.at[i]) for i, ref in enumerate((eta_out, tu_out, tv_out))]
    for c in planes:
        c.start()

    def fluxes(k, slot):
        kf = real(k)
        u = jnp.where(kf < faces[0], us[k + 1] + corr[0], 0.0)
        v = jnp.where(kf < faces[1], vs[k + 1] + corr[1], 0.0)
        new_u[k] = u
        new_v[k] = v
        u = (0.5 * TIME_STEP) * u
        v = (0.5 * TIME_STEP) * v
        here = pl.ds(k, 1)
        v_s = (0.5 * TIME_STEP) * vcs[here]
        b, m = slot_of(k, bank)
        for a, src in ((0, tm), (1, sm)):
            x = src[k + 1]
            turned[slot, a] = turn(halo[a, b], LANES - m)
            flux_x = u * (x + shift_east(x, turned[slot, a]))
            flux_y = v * (x + shift_north(x, trow_n[a, here]))
            edge_y = v_s * (trow_s[a, here] + x[FIRST])
            flux[slot, a] = flux_x
            rest[slot, a] = (x - flux_x) - (flux_y - shift_south(flux_y, edge_y))

    def finish(k, slot):
        wet = k.astype(F32) < faces[2]
        for a, dst in ((0, new_t), (1, new_s)):
            moved = shift_west(flux[slot, a], turned[slot, a])
            dst[k] = jnp.where(wet, rest[slot, a] + moved, 0.0)

    def copies(c):
        return [pltpu.make_async_copy(src.at[pl.ds(c * KB, KB)], dst.at[pl.ds(c * KB, KB)], out_sem.at[i, c])
                for i, (src, dst) in enumerate(((new_u, u_out), (new_v, v_out), (new_t, t_out), (new_s, s_out)))]

    def chunk(c, carry):
        for d in range(KB):
            fluxes(jnp.minimum(c * KB + d + 1, n_lev - 1), (d + 1) % KB)
            finish(c * KB + d, d)
        for copy in copies(c):
            copy.start()
        return carry

    n_copy = n_lev // KB
    fluxes(0, 0)
    lax.fori_loop(0, n_copy, chunk, 0)
    for c in range(n_copy):
        for copy in copies(c):
            copy.wait()
    for c in planes:
        c.wait()


def solution(mesh):
    n_cols, n_rows = mesh.shape["col"], mesh.shape["row"]

    def local_step(vel_u, vel_v, value_a11, salinity, sea_level, trans_u, trans_v, bathymetry, kmt_levels, tide_force):
        n_lev, ny, nx = vel_u.shape
        whole, wide = ny + 2 * H, nx + LANES
        n_chunk, bank = n_lev // CH, (n_lev + 1) // 2
        hbm_spec = pl.BlockSpec(memory_space=pltpu.HBM)
        vmem_spec = pl.BlockSpec(memory_space=pltpu.VMEM)
        cube = (n_lev, ny, nx)
        deep = (n_lev + 2, ny, nx)
        n_row = n_lev + -n_lev % SUB
        column, pair_c, rows1, rows2 = (ny, LANES), (2, ny, LANES), (n_row, nx), (2, n_row, nx)
        banks, two, small, both = (2, 2, ny, LANES), (2, ny, nx), (SUB, LANES), (UN, 2, ny, nx)

        edges = (UN, 2, ny, LANES)

        def sds(*shape):
            return jax.ShapeDtypeStruct(shape, F32)

        def bufs(*shapes):
            return [pltpu.VMEM(shape, F32) for shape in shapes]

        def sems(*shape):
            return pltpu.SemaphoreType.DMA(shape)

        passed = [(3, ny, nx), two, (3, ny, nx), rows1, banks, rows2, rows2]
        *cubes, bar, corr, face, vcs, halo, trow_n, trow_s = pl.pallas_call(
            functools.partial(main_kernel, n_rows, n_cols),
            out_shape=bufs(*[deep] * 4, *passed),
            in_specs=[hbm_spec] * 9 + [pl.BlockSpec(memory_space=pltpu.SMEM)],
            out_specs=[vmem_spec] * (4 + len(passed)),
            scratch_shapes=[
                pltpu.VMEM((ny, nx), jnp.int32),
                *bufs((7, whole, wide), (12, whole, wide), (2, ny + SUB, wide)),
                *bufs(*[(7, 3 * SUB, LANES)] * 2, *[(7, 2 * SUB, LANES)] * 2, *[(7, SUB, LANES)] * 4),
                *bufs(cube, cube, *[deep] * 3, cube, *[(ny, nx)] * 4, two, two, two, two, both, both, (UN, ny, nx), (UN, ny, nx), both, edges, (4, n_row, nx), (n_row, LANES)),
                *bufs(banks, banks, pair_c, pair_c, column, pair_c, pair_c, column, small, small, banks, small),
                *bufs(rows2, rows2, rows1, rows2, rows2, rows1),
                *bufs(pair_c, pair_c, rows2, rows2, pair_c, pair_c, rows2, rows2, column, rows1, column, rows1),
                sems(5), sems(4, n_chunk), sems(38), sems(38),
            ],
            compiler_params=pltpu.CompilerParams(collective_id=0, has_side_effects=True, vmem_limit_bytes=44 * 2**20),
        )(kmt_levels, bathymetry, sea_level, trans_u, trans_v, vel_u, vel_v, value_a11, salinity, tide_force.T)

        return pl.pallas_call(
            functools.partial(last_kernel, bank=bank),
            out_shape=[sds(ny, nx)] * 3 + [sds(*cube)] * 4,
            in_specs=[vmem_spec] * (4 + len(passed)),
            out_specs=[hbm_spec] * 7,
            scratch_shapes=[*bufs(*[cube] * 4, both, both, edges), sems(3), sems(4, n_lev // KB)],
            compiler_params=pltpu.CompilerParams(vmem_limit_bytes=18 * 2**20),
        )(*cubes, bar, corr, face, vcs, halo, trow_n, trow_s)

    spec_cube = P(None, "row", "col")
    spec_plane = P("row", "col")
    return jax.shard_map(local_step, mesh=mesh, in_specs=(spec_cube,) * 4 + (spec_plane,) * 5 + (P(None, None),),
                         out_specs=(spec_plane,) * 3 + (spec_cube,) * 4, check_vma=False)
```

```python
import functools

import jax
import jax.numpy as jnp
from jax import lax
from jax.experimental import pallas as pl
from jax.experimental.pallas import tpu as pltpu
from jax.sharding import PartitionSpec as P

TIME_STEP = 4.0
ALPHA_T = 0.02
BETA_S = 0.015
VISC_KV = 0.001
DIFF_KT = 0.0005
MESH = pl.DeviceIdType.MESH
H = 32
CH = 15
UN = 5
UE = 15
KB = 5
SUB, LANES = 8, 128
LAST = LANES - 1
F32 = jnp.float32
HEAD = 0.25 * TIME_STEP
KMT, DEPTH, ETA, TU, TV, FX, FY = range(7)
KU, KV, DZU, DZV, GU, GV, BU, BV, WD, GW, BW, UW = range(12)
FIRST = slice(0, 1)


def iota(shape, axis):
    return lax.broadcasted_iota(jnp.int32, shape, axis)


def reduced(x):
    return pl.reciprocal(x, approx=False)


def scaled(x):
    return x if HEAD == 1.0 else HEAD * x


def lane_of(x):
    return iota(x.shape, 1)


def slot_of(k, bank):
    b = int(k >= bank) if isinstance(k, int) else (k >= bank).astype(jnp.int32)
    return b, 2 * (k - b * bank)


def real(k):
    return float(k) if isinstance(k, int) else k.astype(F32)


def turn(x, n):
    return pltpu.roll(x, n % LANES if isinstance(n, int) else n, 1)


def shift_east(x, halo):
    left, right = turn(x[:, :LANES], -1), turn(x[:, LANES:], -1)
    edge = lane_of(left) == LAST
    return jnp.concatenate([jnp.where(edge, right, left), jnp.where(edge, halo, right)], axis=1)


def shift_west(x, halo):
    left, right = turn(x[:, :LANES], 1), turn(x[:, LANES:], 1)
    edge = lane_of(left) == 0
    return jnp.concatenate([jnp.where(edge, halo, left), jnp.where(edge, left, right)], axis=1)


def tiles_of(x):
    return [x[SUB * t:SUB * t + SUB] for t in range(x.shape[0] // SUB)]


def shift_north(x, halo):
    rolled = [pltpu.roll(t, SUB - 1, 0) for t in tiles_of(x)]
    edge = iota(rolled[0].shape, 0) == SUB - 1
    rolled.append(jnp.broadcast_to(halo, rolled[0].shape))
    return jnp.concatenate([jnp.where(edge, b, a) for a, b in zip(rolled[:-1], rolled[1:])], axis=0)


def shift_south(x, halo):
    rolled = [pltpu.roll(t, 1, 0) for t in tiles_of(x)]
    edge = iota(rolled[0].shape, 0) == 0
    rolled.insert(0, jnp.broadcast_to(halo, rolled[0].shape))
    return jnp.concatenate([jnp.where(edge, a, b) for a, b in zip(rolled[:-1], rolled[1:])], axis=0)


def merged(west, east):
    even = lane_of(west) % 2 == 0
    back = turn(east, -1)
    return jnp.where(even, west, back), turn(jnp.where(even, back, west), -1)


def main_kernel(n_rows, n_cols,
                kmt_in, bat_in, eta_in, tu_in, tv_in, u_in, v_in, t_in, s_in, tide,
                pu, pv, tb, sb, bar_out, corr_out, face_out, vcs_out,
                halo_out, trow_n_out, trow_s_out,
                kmt_v, ext, xp, acc, pk_w, pk_e, r_e, r_w, r_ne, r_nw, r_se, r_sw,
                ub, vb, gc, gu, gv, pp, wet_v, dz_v, cc_v, cum_v, faces, coefs, push_v, sum_v, s_now, s_low, s_head, s_corner, s_side, s_edge, row_h, corner_r,
                bank_uv, bank_ts, sc_w, sc_e, sp_w, rc_e, rc_w, rp_e, rc_nw, rc_se, hc, corner_p,
                sr_n, sr_s, sp_s, rr_n, rr_s, rp_n,
                tc_w, tc_e, tr_n, tr_s, qc_e, qc_w, qr_n, qr_s, su_e, sv_n, ru_w, rv_s,
                plane_sem, in_sem, send_sem, recv_sem):
    n_sub = tide.shape[1]
    n_lev = u_in.shape[0]
    n_chunk = n_lev // CH
    bank, n_row = (n_lev + 1) // 2, sp_s.shape[0]
    ny, nx = kmt_in.shape
    dt_sub = TIME_STEP / n_sub
    col, row = lax.axis_index("col"), lax.axis_index("row")
    east, west = lax.rem(col + 1, n_cols), lax.rem(col + n_cols - 1, n_cols)
    north, south = lax.rem(row + 1, n_rows), lax.rem(row + n_rows - 1, n_rows)
    where_to = {"n": (col, north), "s": (col, south), "e": (east, row), "w": (west, row),
                "ne": (east, north), "nw": (west, north), "se": (east, south), "sw": (west, south)}
    own = (pl.ds(H, ny), pl.ds(0, nx))
    mid, cols = slice(H, H + ny), slice(0, nx)
    at_n, at_s = slice(H + ny, H + ny + 1), slice(H - 1, H)
    whole, wide = ny + 2 * H, nx + LANES
    at_w, at_e = slice(wide - 1, wide), slice(nx, nx + 1)
    first_row, last_row = FIRST, slice(ny - 1, ny)

    planes = [pltpu.make_async_copy(kmt_in, kmt_v, plane_sem.at[KMT])]
    for i, ref in ((DEPTH, bat_in), (ETA, eta_in), (TU, tu_in), (TV, tv_in)):
        planes.append(pltpu.make_async_copy(ref, ext.at[(i, *own)], plane_sem.at[i]))
    def load(a, c):
        src, dst, off = ((u_in, ub, 0), (v_in, vb, 0), (t_in, tb, 1), (s_in, sb, 1))[a]
        return pltpu.make_async_copy(src.at[pl.ds(c * CH, CH)], dst.at[pl.ds(c * CH + off, CH)], in_sem.at[a, c])

    for c in range(n_chunk):
        load(0, c).start()
        load(1, c).start()
    for c in planes:
        c.start()

    barrier = pltpu.get_barrier_semaphore()
    for c_id, r_id in where_to.values():
        pl.semaphore_signal(barrier, inc=1, device_id={"col": c_id, "row": r_id}, device_id_type=MESH)

    used = []

    def remote(src, dst, to):
        c_id, r_id = where_to[to]
        i = len(used)
        used.append(i)
        copy = pltpu.make_async_remote_copy(src_ref=src, dst_ref=dst, send_sem=send_sem.at[i], recv_sem=recv_sem.at[i],
                                            device_id={"col": c_id, "row": r_id}, device_id_type=MESH)
        return copy, to[0]

    below_wall, above_wall = row < n_rows - 1, row > 0

    def sends(copies, act):
        for copy, to in copies:
            if to in "ns":
                pl.when(below_wall if to == "n" else above_wall)(functools.partial(act, copy))
            else:
                act(copy)

    def started(copies):
        sends(copies, lambda c: c.start())
        return copies

    def sent(copies):
        sends(copies, lambda c: c.wait_send())

    def received(copies):
        for copy, to in copies:
            if to in "ns":
                pl.when(above_wall if to == "n" else below_wall)(copy.wait_recv)
            else:
                copy.wait_recv()

    def wide_copies(p0, n):
        ps = pl.ds(p0, n)
        low, mids, high = pl.ds(0, 2 * SUB), pl.ds(0, SUB), pl.ds(2 * SUB, SUB)
        return started([
            remote(ext.at[ps, pl.ds(H, H), pl.ds(0, nx)], ext.at[ps, pl.ds(H + ny, H), pl.ds(0, nx)], "s"),
            remote(ext.at[ps, pl.ds(ny, H), pl.ds(0, nx)], ext.at[ps, pl.ds(0, H), pl.ds(0, nx)], "n"),
            remote(pk_w.at[ps, low], r_e.at[ps], "w"),
            remote(pk_e.at[ps, low], r_w.at[ps], "e"),
            remote(pk_w.at[ps, mids], r_ne.at[ps], "sw"),
            remote(pk_e.at[ps, mids], r_nw.at[ps], "se"),
            remote(pk_w.at[ps, high], r_se.at[ps], "nw"),
            remote(pk_e.at[ps, high], r_sw.at[ps], "ne"),
        ])

    group = iota((SUB, LANES), 1) // H
    n_groups = LANES // H

    def pack(p):
        x = ext[(p, *own)]
        for ref, tile, g0 in ((pk_w, x[:, :LANES], 0), (pk_e, x[:, nx - LANES:], n_groups - 1)):
            for at, first, count in ((0, 0, 4), (1, 4, 2), (2, 2, 4)):
                total = jnp.zeros((SUB, LANES), F32)
                for q in range(count):
                    rows = tile[SUB * (first + q):SUB * (first + q) + SUB]
                    rows = turn(rows, H * (q - g0)) if q != g0 else rows
                    total = jnp.where(group == q, rows, total)
                ref[p, SUB * at:SUB * at + SUB, :] = total

    def unpack(p):
        edge = H // SUB
        for t in range(whole // SUB):
            if t < edge:
                e_tile, w_tile, q = r_se[p], r_sw[p], t
            elif t < (H + ny) // SUB:
                rows = slice(SUB * ((t - edge) // n_groups), SUB * ((t - edge) // n_groups) + SUB)
                e_tile, w_tile, q = r_e[p, rows], r_w[p, rows], (t - edge) % n_groups
            else:
                e_tile, w_tile, q = r_ne[p], r_nw[p], t - (H + ny) // SUB
            e_tile = turn(e_tile, -H * q) if q else e_tile
            w_tile = turn(w_tile, H * (n_groups - 1 - q)) if q != n_groups - 1 else w_tile
            side = jnp.where(group == 0, e_tile, jnp.where(group == n_groups - 1, w_tile, 0.0))
            ext[p, SUB * t:SUB * t + SUB, nx:] = side

    zero = jnp.zeros((ny, nx), F32)
    for ref in (bank_uv, bank_ts, sp_w, su_e):
        ref[...] = jnp.zeros(ref.shape, F32)
    lane = iota((ny, LANES), 1)
    even = lane % 2 == 0

    def both_edges(x):
        return jnp.where(lane < LANES // 2, x[:, :LANES], x[:, nx - LANES:])

    def gather(x, y, k, banks, rows_s, rows_n):
        b, m = slot_of(k, bank)
        here = ((lane + 1 - m) & LAST) < 2
        pltpu.store(banks.at[0, b], turn(both_edges(x), m), mask=here)
        pltpu.store(banks.at[1, b], turn(both_edges(y), m), mask=here)
        here = pl.ds(k, 1)
        rows_s[0, here] = x[first_row]
        rows_s[1, here] = y[first_row]
        rows_n[0, here] = x[last_row]
        rows_n[1, here] = y[last_row]

    def in_chunks(arrays, levels, step, follow=()):
        def chunk(c, carry):
            for a in arrays:
                load(a, c).wait()
            if follow:
                for a in follow:
                    load(a, c).start()

            def group_of(i, carry):
                levels(c * CH + i * step)
                return carry

            return lax.fori_loop(0, CH // step, group_of, carry)

        lax.fori_loop(0, n_chunk, chunk, 0)

    def edge_levels(k0):
        for d in range(UE):
            gather(ub[k0 + d], vb[k0 + d], k0 + d, bank_uv, sr_s, sr_n)

    in_chunks((0, 1), edge_levels, UE, (2, 3))

    def split_banks(banks):
        a, b = banks[0], turn(banks[1], 1)
        return jnp.where(even, a, b), turn(jnp.where(even, b, a), 1)

    for i in range(2):
        sc_w[i], sc_e[i] = split_banks(bank_uv.at[i])
    for c in planes:
        c.wait()
    kmt = kmt_v[...].astype(F32)
    ext[(KMT, *own)] = kmt
    for p in range(FX):
        pack(p)
    pl.semaphore_wait(barrier, len(where_to))
    first = wide_copies(KMT, 2)
    second = started([
        remote(sc_w, rc_e, "w"),
        remote(sc_e, rc_w, "e"),
        remote(sr_n, rr_s, "n"),
        remote(sr_s, rr_n, "s"),
        remote(sc_e.at[0, pl.ds(0, SUB)], rc_nw, "se"),
        remote(sc_w.at[1, pl.ds(ny - SUB, SUB)], rc_se, "nw"),
    ])

    dz = ext[(DEPTH, *own)] / jnp.maximum(kmt, 1.0)
    safe = jnp.where(kmt > 0, dz, 1.0)
    wet_v[...] = kmt
    dz_v[...] = TIME_STEP * dz
    cc_v[...] = (TIME_STEP * DIFF_KT) / (safe * safe)
    cum_v[...] = zero
    for ref in (tb, sb, pu, pv):
        ref[0] = zero
        ref[n_lev + 1] = zero
    for ref in (gc, gu, gv):
        ref[0] = zero + 1.0

    def pressure_levels(k0):
        cum = cum_v[...]
        for d in range(UE):
            k = k0 + d
            dens = BETA_S * (sb[k + 1] - 1.0) - ALPHA_T * (tb[k + 1] - 1.0)
            dens = jnp.where(k.astype(F32) < wet_v[...], dens, 0.0)
            cum = cum + dens
            pres = dz_v[...] * (cum - 0.5 * dens)
            pp[k] = pres
            b, m = slot_of(k, bank)
            pltpu.store(sp_w, turn(pres[:, :LANES], m + b), mask=lane == m + b)
            sp_s[pl.ds(k, 1)] = pres[first_row]
        cum_v[...] = cum

    in_chunks((2, 3), pressure_levels, UE)
    last_edges = started([remote(sp_w, rp_e, "w"), remote(sp_s, rp_n, "s")])

    def down_levels(i, carry):
        k0 = i * UN
        g, t_up, s_up = gc[k0], tb[k0], sb[k0]
        wet = k0.astype(F32) < wet_v[...]
        for d in range(UN):
            k = k0 + d
            below = (k + 1).astype(F32) < wet_v[...]
            coef = cc_v[...]
            up = jnp.where(below, coef, 0.0)
            inv = reduced(1.0 + up + coef * (1.0 - g))
            g = up * inv
            t_up = jnp.where(wet, (tb[k + 1] + coef * t_up) * inv, 0.0)
            s_up = jnp.where(wet, (sb[k + 1] + coef * s_up) * inv, 0.0)
            gc[k + 1] = g
            tb[k + 1] = t_up
            sb[k + 1] = s_up
            wet = below
        return carry

    lax.fori_loop(0, n_lev // UN, down_levels, 0)

    sent(first)
    received(first)
    for p in (KMT, DEPTH):
        unpack(p)
    line = iota((whole, wide), 0)
    seen = ((line >= H) | (row > 0)) & ((line < H + ny) | (row < n_rows - 1))
    kx = jnp.where(seen, ext[KMT], 0.0)
    ext[KMT] = kx
    dzx = jnp.where(seen, ext[DEPTH], 0.0) / jnp.maximum(kx, 1.0)
    ku = jnp.minimum(kx, pltpu.roll(kx, wide - 1, 1))
    kv = jnp.minimum(kx, pltpu.roll(kx, whole - 1, 0))
    dzu = 0.5 * (dzx + pltpu.roll(dzx, wide - 1, 1))
    dzv = 0.5 * (dzx + pltpu.roll(dzx, whole - 1, 0))
    xp[KU] = ku
    xp[KV] = kv
    xp[DZU] = dzu
    xp[DZV] = dzv
    xp[GU] = jnp.where(ku > 0, dt_sub * (ku * dzu), 0.0)
    xp[GV] = jnp.where(kv > 0, dt_sub * (kv * dzv), 0.0)
    xp[WD] = jnp.where(kx > 0, dt_sub, 0.0)
    xp[GW] = pltpu.roll(xp[GU], 1, 1)
    face_out[2] = wet_v[...]
    for i in range(2):
        count = xp[(KU + i, *own)]
        safe = jnp.where(count > 0, xp[(DZU + i, *own)], 1.0)
        faces[i] = count
        face_out[i] = count
        coefs[i] = (TIME_STEP * VISC_KV) / (safe * safe)
        push_v[i] = zero
        sum_v[i] = zero

    received(second)
    pair = lane // 2
    lev = jnp.where(pair < bank, pair + bank * (lane % 2), n_lev).astype(F32)

    def column(ref, count):
        return jnp.where(lev < count, ref, 0.0)

    u_w = column(rc_w[0], xp[KU, mid, at_w])
    v_w = column(rc_w[1], xp[KV, mid, at_w])
    u_e = column(rc_e[0], xp[KU, mid, at_e])
    v_e = column(rc_e[1], xp[KV, mid, at_e])
    u_last = column(sc_e[0], xp[KU, mid, nx - 1:nx])
    v_zero = column(sc_w[1], xp[KV, mid, FIRST])
    corner_u = jnp.where(lev[FIRST] < xp[KU, at_n, at_w], rc_nw[FIRST, :], 0.0)
    q_e = scaled((u_last + u_e) * (u_last + u_e))
    c_w = scaled((u_w + shift_north(u_w, corner_u)) * (v_w + v_zero))
    hc[1, 0], hc[1, 1] = merged(c_w, v_e)
    corner_p[...] = jnp.where(lev[:SUB] < xp[KV, H - SUB:H, at_e], rc_se[...], 0.0)

    def corner_levels(i, carry):
        for d in range(UE):
            b, m = slot_of(i * UE + d, bank)
            corner_r[pl.ds(i * UE + d, 1)] = turn(corner_p[...], LAST - m - b)[SUB - 1:]
        return carry

    lax.fori_loop(0, n_lev // UE, corner_levels, 0)
    row_lev = iota((n_row, nx), 0).astype(F32)

    def row_of(x, f, at):
        return jnp.where(row_lev < xp[KU + f, at, cols], x, 0.0)

    v_s = row_of(rr_s[1], 1, at_s)
    v_last = row_of(sr_n[1], 1, slice(H + ny - 1, H + ny))
    v_n = row_of(rr_n[1], 1, at_n)
    row_h[0] = row_of(rr_n[0], 0, at_n)
    row_h[1] = scaled((row_of(rr_s[0], 0, at_s) + row_of(sr_s[0], 0, slice(H, H + 1))) * (v_s + shift_east(v_s, corner_r[...])))
    row_h[2] = v_s
    row_h[3] = scaled((v_last + v_n) * (v_last + v_n))
    received(last_edges)
    state = wide_copies(ETA, 3)
    hc[0, 0], hc[0, 1] = merged(u_w, q_e + rp_e[...])
    row_h[3] += jnp.where(below_wall, rp_n[...], 0.0)

    def forces(k, slot):
        kf = real(k)
        k = k if isinstance(k, int) else jnp.minimum(k, n_lev - 1)
        masked = []
        for f, ref in ((0, ub), (1, vb)):
            wet = kf < faces[f]
            masked.append(jnp.where(wet, ref[k], 0.0))
            s_now[slot, f] = masked[f]
            s_low[slot, f] = jnp.where(wet, coefs[f], 0.0)
        u, v = masked
        p = pp[k]
        b, m = slot_of(k, bank)
        u_n, corner_s, v_s, edge_v = [row_h[i, pl.ds(k, 1)] for i in range(4)]
        for i in range(2):
            s_edge[slot, i] = turn(hc[i, b], LANES - m)
        cen_u = shift_west(u, s_edge[slot, 0]) + u
        head = scaled(cen_u * cen_u) + p
        s_head[slot] = head
        corner = scaled((u + shift_north(u, u_n)) * (v + shift_east(v, s_edge[slot, 1])))
        s_corner[slot] = corner
        s_side[slot, 0] = (corner - shift_south(corner, corner_s)) - head
        cen_v = shift_south(v, v_s) + v
        head_v = scaled(cen_v * cen_v) + p
        s_side[slot, 1] = (shift_north(head_v, edge_v) - head_v) + corner

    def solve_down(k, slot, below):
        kf = k.astype(F32)
        head, corner = s_head[slot], s_corner[slot]
        grad_u = shift_east(head, s_edge[slot, 0]) + s_side[slot, 0]
        grad_v = s_side[slot, 1] - shift_west(corner, s_edge[slot, 1])
        for f, grad, part, gain in ((0, grad_u, pu, gu), (1, grad_v, pv, gv)):
            low, up = s_low[slot, f], s_low[below, f]
            inv = reduced(1.0 + up + low * (1.0 - gain[k]))
            gain[k + 1] = up * inv
            pull = jnp.where(kf < faces[f], grad, 0.0)
            push_v[f] += pull
            part[k + 1] = ((s_now[slot, f] - pull) + low * part[k]) * inv

    def momentum_levels(i, carry):
        k = UN * i
        for d in range(UN):
            forces(k + d + 1, (d + 1) % UN)
            solve_down(k + d, d, (d + 1) % UN)
        return carry

    forces(0, 0)
    lax.fori_loop(0, n_lev // UN, momentum_levels, 0)

    for f in range(2):
        ext[(FX + f, *own)] = xp[(DZU + f, *own)] * push_v[f] * (-1.0 / TIME_STEP)
        pack(FX + f)
    third = wide_copies(FX, 2)

    def upward(levels):
        def group_of(i, carry):
            levels(n_lev - 1 - i * UE)
            return carry

        lax.fori_loop(0, n_lev // UE, group_of, 0)

    def mix_levels(k0):
        t, s = tb[k0 + 2], sb[k0 + 2]
        for d in range(UE):
            k = k0 - d
            g = gc[k + 1]
            t = tb[k + 1] + g * t
            s = sb[k + 1] + g * s
            tb[k + 1] = t
            sb[k + 1] = s
            gather(t, s, k, bank_ts, tr_s, tr_n)

    upward(mix_levels)
    for i in range(2):
        tc_w[i], tc_e[i] = split_banks(bank_ts.at[i])
    tracer = started([
        remote(tc_w, qc_e, "w"),
        remote(tc_e, qc_w, "e"),
        remote(tr_n, qr_s, "n"),
        remote(tr_s, qr_n, "s"),
    ])

    def rise_levels(k0):
        u, v = pu[k0 + 2], pv[k0 + 2]
        sum_u, sum_w = sum_v[0], sum_v[1]
        for d in range(UE):
            k = k0 - d
            u = pu[k + 1] + gu[k + 1] * u
            v = pv[k + 1] + gv[k + 1] * v
            pu[k + 1] = u
            pv[k + 1] = v
            sum_u += u
            sum_w += v
            b, m = slot_of(k, bank)
            pltpu.store(su_e, turn(u[:, nx - LANES:], m + b + 1), mask=lane == m + b)
            sv_n[pl.ds(k, 1)] = v[last_row]
        sum_v[0], sum_v[1] = sum_u, sum_w

    upward(rise_levels)
    fourth = started([remote(su_e, ru_w, "e"), remote(sv_n, rv_s, "n")])

    sent(state)
    received(state)
    for p in (ETA, TU, TV):
        unpack(p)
        ext[p] = jnp.where((xp[WD] if p == ETA else xp[KU + p - TU]) > 0, ext[p], 0.0)
    xp[UW] = pltpu.roll(ext[TU], 1, 1)
    received(third)
    for f in range(2):
        unpack(FX + f)
        xp[BU + f] = jnp.where(xp[KU + f] > 0, dt_sub * ext[FX + f], 0.0)
    xp[BW] = pltpu.roll(xp[BU], 1, 1)
    acc[...] = jnp.zeros(acc.shape, F32)
    norm = 6.0 / (n_sub * (n_sub + 1) * (n_sub + 2))
    line8 = iota((SUB, wide), 0)
    t0 = H // SUB - 1

    def substep(n, lo, hi):
        tide_u, tide_v = tide[0, n], tide[1, n]
        weight = norm * ((n + 1) * (n_sub - n)).astype(F32)

        def finish(t, eta, rolled, rolled_next, u, u_w, v):
            rows = slice(SUB * t, SUB * t + SUB)
            eta_n = jnp.where(line8 == SUB - 1, rolled_next, rolled)
            eta_e = pltpu.roll(eta, wide - 1, 1)
            eta_w = pltpu.roll(eta, 1, 1)
            xp[UW, rows] = u_w + (xp[GW, rows] * (tide_u + (eta_w - eta)) + xp[BW, rows])
            u_new = u + (xp[GU, rows] * (tide_u + (eta - eta_e)) + xp[BU, rows])
            v_new = v + (xp[GV, rows] * (tide_v + (eta - eta_n)) + xp[BV, rows])
            ext[TU, rows] = u_new
            ext[TV, rows] = v_new
            if t0 <= t < (H + ny) // SUB:
                at = slice(SUB * (t - t0), SUB * (t - t0) + SUB)
                acc[0, at] += weight * u_new
                acc[1, at, :nx] += weight * v_new[:, :nx]

        last = None
        v_below = jnp.zeros((SUB, wide), F32)
        for t in range(lo, hi):
            rows = slice(SUB * t, SUB * t + SUB)
            u, u_w, v = ext[TU, rows], xp[UW, rows], ext[TV, rows]
            v_roll = pltpu.roll(v, 1, 0)
            v_s = jnp.where(line8 == 0, v_below, v_roll)
            v_below = v_roll
            eta = ext[ETA, rows] - xp[WD, rows] * ((u - u_w) + (v - v_s))
            ext[ETA, rows] = eta
            rolled = pltpu.roll(eta, SUB - 1, 0)
            if last is not None:
                eta_b, rolled_b, *face_b = last
                finish(t - 1, eta_b, rolled_b, rolled, *face_b)
            last = (eta, rolled, u, u_w, v)
        finish(hi - 1, eta, rolled, rolled, u, u_w, v)

    edge_tiles = H // SUB
    for e in range(edge_tiles, 0, -1):
        begin = max(0, n_sub + 1 - SUB * e) if e < edge_tiles else 0
        end = n_sub + 1 - SUB * (e - 1) if e > 1 else n_sub
        span = (edge_tiles - e, whole // SUB - edge_tiles + e)

        def two(i, carry, begin=begin, span=span):
            substep(begin + 2 * i, *span)
            substep(begin + 2 * i + 1, *span)
            return carry

        lax.fori_loop(0, (end - begin) // 2, two, 0)
        if (end - begin) % 2:
            substep(jnp.int32(end - 1), *span)

    for i in range(3):
        bar_out[i] = ext[(ETA + i, *own)]

    def safe_depth(f, rows, lanes):
        depth = xp[KU + f, rows, lanes] * xp[DZU + f, rows, lanes]
        return jnp.where(depth > 0, depth, 1.0)

    inner = slice(SUB, SUB + ny)
    for f in range(2):
        corr_out[f] = (acc[f, inner, cols] - xp[DZU + f, mid, cols] * sum_v[f]) / safe_depth(f, mid, cols)
    received(fourth)
    star = ru_w[...]
    fix = (acc[0, inner, at_w] - xp[DZU, mid, at_w] * jnp.sum(star, axis=1, keepdims=True)) / safe_depth(0, mid, at_w)
    u_c = column(star + fix, xp[KU, mid, at_w])
    star = row_of(rv_s[...], 1, at_s)
    total = jnp.sum(star, axis=0, keepdims=True)
    fix = (acc[1, SUB - 1:SUB, cols] - xp[DZV, at_s, cols] * total) / safe_depth(1, at_s, cols)
    vcs_out[...] = row_of(star + fix, 1, at_s)
    received(tracer)
    for i in range(2):
        halo_out[i, 0], halo_out[i, 1] = merged((0.5 * TIME_STEP) * u_c * (qc_w[i] + tc_w[i]), qc_e[i])
    trow_n_out[...] = jnp.where(below_wall, qr_n[...], 0.0)
    trow_s_out[...] = jnp.where(above_wall, qr_s[...], 0.0)
    sent(second + last_edges + third + tracer + fourth)


def last_kernel(us, vs, tm, sm, bar, corr, faces, vcs, halo, trow_n, trow_s,
                eta_out, tu_out, tv_out, u_out, v_out, t_out, s_out,
                new_u, new_v, new_t, new_s, flux, rest, turned, bar_sem, out_sem, *, bank):
    n_lev = u_out.shape[0]
    planes = [pltpu.make_async_copy(bar.at[i], ref, bar_sem.at[i]) for i, ref in enumerate((eta_out, tu_out, tv_out))]
    for c in planes:
        c.start()

    def fluxes(k, slot):
        kf = real(k)
        u = jnp.where(kf < faces[0], us[k + 1] + corr[0], 0.0)
        v = jnp.where(kf < faces[1], vs[k + 1] + corr[1], 0.0)
        new_u[k] = u
        new_v[k] = v
        u = (0.5 * TIME_STEP) * u
        v = (0.5 * TIME_STEP) * v
        here = pl.ds(k, 1)
        v_s = (0.5 * TIME_STEP) * vcs[here]
        b, m = slot_of(k, bank)
        for a, src in ((0, tm), (1, sm)):
            x = src[k + 1]
            turned[slot, a] = turn(halo[a, b], LANES - m)
            flux_x = u * (x + shift_east(x, turned[slot, a]))
            flux_y = v * (x + shift_north(x, trow_n[a, here]))
            edge_y = v_s * (trow_s[a, here] + x[FIRST])
            flux[slot, a] = flux_x
            rest[slot, a] = (x - flux_x) - (flux_y - shift_south(flux_y, edge_y))

    def finish(k, slot):
        wet = k.astype(F32) < faces[2]
        for a, dst in ((0, new_t), (1, new_s)):
            moved = shift_west(flux[slot, a], turned[slot, a])
            dst[k] = jnp.where(wet, rest[slot, a] + moved, 0.0)

    def copies(c):
        return [pltpu.make_async_copy(src.at[pl.ds(c * KB, KB)], dst.at[pl.ds(c * KB, KB)], out_sem.at[i, c])
                for i, (src, dst) in enumerate(((new_u, u_out), (new_v, v_out), (new_t, t_out), (new_s, s_out)))]

    def chunk(c, carry):
        def done(d):
            finish(c * UE + d, d)
            if d % KB == KB - 1:
                for copy in copies(c * (UE // KB) + d // KB):
                    copy.start()

        for d in range(1, UE):
            fluxes(c * UE + d, d)
            done(d - 1)
        fluxes(jnp.minimum(c * UE + UE, n_lev - 1), 0)
        done(UE - 1)
        return carry

    n_copy = n_lev // KB
    fluxes(0, 0)
    lax.fori_loop(0, n_lev // UE, chunk, 0)
    for c in range(n_copy):
        for copy in copies(c):
            copy.wait()
    for c in planes:
        c.wait()


def solution(mesh):
    n_cols, n_rows = mesh.shape["col"], mesh.shape["row"]

    def local_step(vel_u, vel_v, value_a11, salinity, sea_level, trans_u, trans_v, bathymetry, kmt_levels, tide_force):
        n_lev, ny, nx = vel_u.shape
        whole, wide = ny + 2 * H, nx + LANES
        n_chunk, bank = n_lev // CH, (n_lev + 1) // 2
        hbm_spec = pl.BlockSpec(memory_space=pltpu.HBM)
        vmem_spec = pl.BlockSpec(memory_space=pltpu.VMEM)
        cube = (n_lev, ny, nx)
        deep = (n_lev + 2, ny, nx)
        n_row = n_lev + -n_lev % SUB
        column, pair_c, rows1, rows2 = (ny, LANES), (2, ny, LANES), (n_row, nx), (2, n_row, nx)
        banks, two, small, both = (2, 2, ny, LANES), (2, ny, nx), (SUB, LANES), (UN, 2, ny, nx)

        edges = (UN, 2, ny, LANES)

        def sds(*shape):
            return jax.ShapeDtypeStruct(shape, F32)

        def bufs(*shapes):
            return [pltpu.VMEM(shape, F32) for shape in shapes]

        def sems(*shape):
            return pltpu.SemaphoreType.DMA(shape)

        passed = [(3, ny, nx), two, (3, ny, nx), rows1, banks, rows2, rows2]
        *cubes, bar, corr, face, vcs, halo, trow_n, trow_s = pl.pallas_call(
            functools.partial(main_kernel, n_rows, n_cols),
            out_shape=bufs(*[deep] * 4, *passed),
            in_specs=[hbm_spec] * 9 + [pl.BlockSpec(memory_space=pltpu.SMEM)],
            out_specs=[vmem_spec] * (4 + len(passed)),
            scratch_shapes=[
                pltpu.VMEM((ny, nx), jnp.int32),
                *bufs((7, whole, wide), (12, whole, wide), (2, ny + SUB, wide)),
                *bufs(*[(7, 3 * SUB, LANES)] * 2, *[(7, 2 * SUB, LANES)] * 2, *[(7, SUB, LANES)] * 4),
                *bufs(cube, cube, *[deep] * 3, cube, *[(ny, nx)] * 4, two, two, two, two, both, both, (UN, ny, nx), (UN, ny, nx), both, edges, (4, n_row, nx), (n_row, LANES)),
                *bufs(banks, banks, pair_c, pair_c, column, pair_c, pair_c, column, small, small, banks, small),
                *bufs(rows2, rows2, rows1, rows2, rows2, rows1),
                *bufs(pair_c, pair_c, rows2, rows2, pair_c, pair_c, rows2, rows2, column, rows1, column, rows1),
                sems(5), sems(4, n_chunk), sems(38), sems(38),
            ],
            compiler_params=pltpu.CompilerParams(collective_id=0, has_side_effects=True, vmem_limit_bytes=44 * 2**20),
        )(kmt_levels, bathymetry, sea_level, trans_u, trans_v, vel_u, vel_v, value_a11, salinity, tide_force.T)

        return pl.pallas_call(
            functools.partial(last_kernel, bank=bank),
            out_shape=[sds(ny, nx)] * 3 + [sds(*cube)] * 4,
            in_specs=[vmem_spec] * (4 + len(passed)),
            out_specs=[hbm_spec] * 7,
            scratch_shapes=[*bufs(*[cube] * 4, (UE, 2, ny, nx), (UE, 2, ny, nx), (UE, 2, ny, LANES)), sems(3), sems(4, n_lev // KB)],
            compiler_params=pltpu.CompilerParams(vmem_limit_bytes=24 * 2**20),
        )(*cubes, bar, corr, face, vcs, halo, trow_n, trow_s)

    spec_cube = P(None, "row", "col")
    spec_plane = P("row", "col")
    return jax.shard_map(local_step, mesh=mesh, in_specs=(spec_cube,) * 4 + (spec_plane,) * 5 + (P(None, None),),
                         out_specs=(spec_plane,) * 3 + (spec_cube,) * 4, check_vma=False)
```

```python
import functools

import jax
import jax.numpy as jnp
from jax import lax
from jax.experimental import pallas as pl
from jax.experimental.pallas import tpu as pltpu
from jax.sharding import PartitionSpec as P

TIME_STEP = 4.0
ALPHA_T = 0.02
BETA_S = 0.015
VISC_KV = 0.001
DIFF_KT = 0.0005
MESH = pl.DeviceIdType.MESH
H = 32
CH = 15
UN = 5
UE = 15
KB = 5
SUB, LANES = 8, 128
LAST = LANES - 1
F32 = jnp.float32
HEAD = 0.25 * TIME_STEP
KMT, DEPTH, ETA, TU, TV, FX, FY = range(7)
KU, KV, DZU, DZV, GU, GV, BU, BV, WD, GW, BW, UW = range(12)
FIRST = slice(0, 1)


def iota(shape, axis):
    return lax.broadcasted_iota(jnp.int32, shape, axis)


def reduced(x):
    return pl.reciprocal(x, approx=False)


def scaled(x):
    return x if HEAD == 1.0 else HEAD * x


def lane_of(x):
    return iota(x.shape, 1)


def slot_of(k, bank):
    b = int(k >= bank) if isinstance(k, int) else (k >= bank).astype(jnp.int32)
    return b, 2 * (k - b * bank)


def real(k):
    return float(k) if isinstance(k, int) else k.astype(F32)


def turn(x, n):
    return pltpu.roll(x, n % LANES if isinstance(n, int) else n, 1)


def shift_east(x, halo):
    left, right = turn(x[:, :LANES], -1), turn(x[:, LANES:], -1)
    edge = lane_of(left) == LAST
    return jnp.concatenate([jnp.where(edge, right, left), jnp.where(edge, halo, right)], axis=1)


def shift_west(x, halo):
    left, right = turn(x[:, :LANES], 1), turn(x[:, LANES:], 1)
    edge = lane_of(left) == 0
    return jnp.concatenate([jnp.where(edge, halo, left), jnp.where(edge, left, right)], axis=1)


def tiles_of(x):
    return [x[SUB * t:SUB * t + SUB] for t in range(x.shape[0] // SUB)]


def shift_north(x, halo):
    rolled = [pltpu.roll(t, SUB - 1, 0) for t in tiles_of(x)]
    edge = iota(rolled[0].shape, 0) == SUB - 1
    rolled.append(jnp.broadcast_to(halo, rolled[0].shape))
    return jnp.concatenate([jnp.where(edge, b, a) for a, b in zip(rolled[:-1], rolled[1:])], axis=0)


def shift_south(x, halo):
    rolled = [pltpu.roll(t, 1, 0) for t in tiles_of(x)]
    edge = iota(rolled[0].shape, 0) == 0
    rolled.insert(0, jnp.broadcast_to(halo, rolled[0].shape))
    return jnp.concatenate([jnp.where(edge, a, b) for a, b in zip(rolled[:-1], rolled[1:])], axis=0)


def merged(west, east):
    even = lane_of(west) % 2 == 0
    back = turn(east, -1)
    return jnp.where(even, west, back), turn(jnp.where(even, back, west), -1)


def main_kernel(n_rows, n_cols,
                kmt_in, bat_in, eta_in, tu_in, tv_in, u_in, v_in, t_in, s_in, tide_in,
                pu, pv, tb, sb, bar_out, corr_out, face_out, vcs_out,
                halo_out, trow_n_out, trow_s_out,
                tide, kmt_v, ext, xp, acc, pk_w, pk_e, r_e, r_w, r_ne, r_nw, r_se, r_sw,
                ub, vb, gc, gu, gv, pp, wet_v, dz_v, cc_v, cum_v, faces, coefs, push_v, sum_v, s_now, s_low, s_head, s_corner, s_side, s_edge, row_h, corner_r,
                bank_uv, bank_ts, sc_w, sc_e, sp_w, rc_e, rc_w, rp_e, rc_nw, rc_se, hc, corner_p,
                sr_n, sr_s, sp_s, rr_n, rr_s, rp_n,
                tc_w, tc_e, tr_n, tr_s, qc_e, qc_w, qr_n, qr_s, su_e, sv_n, ru_w, rv_s,
                plane_sem, in_sem, send_sem, recv_sem):
    n_sub = tide.shape[1]
    n_lev = u_in.shape[0]
    n_chunk = n_lev // CH
    bank, n_row = (n_lev + 1) // 2, sp_s.shape[0]
    ny, nx = kmt_in.shape
    dt_sub = TIME_STEP / n_sub
    col, row = lax.axis_index("col"), lax.axis_index("row")
    east, west = lax.rem(col + 1, n_cols), lax.rem(col + n_cols - 1, n_cols)
    north, south = lax.rem(row + 1, n_rows), lax.rem(row + n_rows - 1, n_rows)
    where_to = {"n": (col, north), "s": (col, south), "e": (east, row), "w": (west, row),
                "ne": (east, north), "nw": (west, north), "se": (east, south), "sw": (west, south)}
    own = (pl.ds(H, ny), pl.ds(0, nx))
    mid, cols = slice(H, H + ny), slice(0, nx)
    at_n, at_s = slice(H + ny, H + ny + 1), slice(H - 1, H)
    whole, wide = ny + 2 * H, nx + LANES
    at_w, at_e = slice(wide - 1, wide), slice(nx, nx + 1)
    first_row, last_row = FIRST, slice(ny - 1, ny)

    planes = [pltpu.make_async_copy(kmt_in, kmt_v, plane_sem.at[KMT])]
    for i, ref in ((DEPTH, bat_in), (ETA, eta_in), (TU, tu_in), (TV, tv_in)):
        planes.append(pltpu.make_async_copy(ref, ext.at[(i, *own)], plane_sem.at[i]))
    planes.append(pltpu.make_async_copy(tide_in, tide, plane_sem.at[FX]))
    def load(a, c):
        src, dst, off = ((u_in, ub, 0), (v_in, vb, 0), (t_in, tb, 1), (s_in, sb, 1))[a]
        return pltpu.make_async_copy(src.at[pl.ds(c * CH, CH)], dst.at[pl.ds(c * CH + off, CH)], in_sem.at[a, c])

    for c in range(n_chunk):
        load(0, c).start()
        load(1, c).start()
    for c in planes:
        c.start()

    barrier = pltpu.get_barrier_semaphore()
    for c_id, r_id in where_to.values():
        pl.semaphore_signal(barrier, inc=1, device_id={"col": c_id, "row": r_id}, device_id_type=MESH)

    used = []

    def remote(src, dst, to):
        c_id, r_id = where_to[to]
        i = len(used)
        used.append(i)
        copy = pltpu.make_async_remote_copy(src_ref=src, dst_ref=dst, send_sem=send_sem.at[i], recv_sem=recv_sem.at[i],
                                            device_id={"col": c_id, "row": r_id}, device_id_type=MESH)
        return copy, to[0]

    below_wall, above_wall = row < n_rows - 1, row > 0

    def sends(copies, act):
        for copy, to in copies:
            if to in "ns":
                pl.when(below_wall if to == "n" else above_wall)(functools.partial(act, copy))
            else:
                act(copy)

    def started(copies):
        sends(copies, lambda c: c.start())
        return copies

    def sent(copies):
        sends(copies, lambda c: c.wait_send())

    def received(copies):
        for copy, to in copies:
            if to in "ns":
                pl.when(above_wall if to == "n" else below_wall)(copy.wait_recv)
            else:
                copy.wait_recv()

    def wide_copies(p0, n):
        ps = pl.ds(p0, n)
        low, mids, high = pl.ds(0, 2 * SUB), pl.ds(0, SUB), pl.ds(2 * SUB, SUB)
        return started([
            remote(ext.at[ps, pl.ds(H, H), pl.ds(0, nx)], ext.at[ps, pl.ds(H + ny, H), pl.ds(0, nx)], "s"),
            remote(ext.at[ps, pl.ds(ny, H), pl.ds(0, nx)], ext.at[ps, pl.ds(0, H), pl.ds(0, nx)], "n"),
            remote(pk_w.at[ps, low], r_e.at[ps], "w"),
            remote(pk_e.at[ps, low], r_w.at[ps], "e"),
            remote(pk_w.at[ps, mids], r_ne.at[ps], "sw"),
            remote(pk_e.at[ps, mids], r_nw.at[ps], "se"),
            remote(pk_w.at[ps, high], r_se.at[ps], "nw"),
            remote(pk_e.at[ps, high], r_sw.at[ps], "ne"),
        ])

    group = iota((SUB, LANES), 1) // H
    n_groups = LANES // H

    def pack(p):
        x = ext[(p, *own)]
        for ref, tile, g0 in ((pk_w, x[:, :LANES], 0), (pk_e, x[:, nx - LANES:], n_groups - 1)):
            for at, first, count in ((0, 0, 4), (1, 4, 2), (2, 2, 4)):
                total = jnp.zeros((SUB, LANES), F32)
                for q in range(count):
                    rows = tile[SUB * (first + q):SUB * (first + q) + SUB]
                    rows = turn(rows, H * (q - g0)) if q != g0 else rows
                    total = jnp.where(group == q, rows, total)
                ref[p, SUB * at:SUB * at + SUB, :] = total

    def unpack(p):
        edge = H // SUB
        for t in range(whole // SUB):
            if t < edge:
                e_tile, w_tile, q = r_se[p], r_sw[p], t
            elif t < (H + ny) // SUB:
                rows = slice(SUB * ((t - edge) // n_groups), SUB * ((t - edge) // n_groups) + SUB)
                e_tile, w_tile, q = r_e[p, rows], r_w[p, rows], (t - edge) % n_groups
            else:
                e_tile, w_tile, q = r_ne[p], r_nw[p], t - (H + ny) // SUB
            e_tile = turn(e_tile, -H * q) if q else e_tile
            w_tile = turn(w_tile, H * (n_groups - 1 - q)) if q != n_groups - 1 else w_tile
            side = jnp.where(group == 0, e_tile, jnp.where(group == n_groups - 1, w_tile, 0.0))
            ext[p, SUB * t:SUB * t + SUB, nx:] = side

    zero = jnp.zeros((ny, nx), F32)
    for ref in (bank_uv, bank_ts, sp_w, su_e):
        ref[...] = jnp.zeros(ref.shape, F32)
    lane = iota((ny, LANES), 1)
    even = lane % 2 == 0

    def both_edges(x):
        return jnp.where(lane < LANES // 2, x[:, :LANES], x[:, nx - LANES:])

    def gather(x, y, k, banks, rows_s, rows_n):
        b, m = slot_of(k, bank)
        here = ((lane + 1 - m) & LAST) < 2
        pltpu.store(banks.at[0, b], turn(both_edges(x), m), mask=here)
        pltpu.store(banks.at[1, b], turn(both_edges(y), m), mask=here)
        here = pl.ds(k, 1)
        rows_s[0, here] = x[first_row]
        rows_s[1, here] = y[first_row]
        rows_n[0, here] = x[last_row]
        rows_n[1, here] = y[last_row]

    def in_chunks(arrays, levels, step, follow=()):
        def chunk(c, carry):
            for a in arrays:
                load(a, c).wait()
            if follow:
                for a in follow:
                    load(a, c).start()

            def group_of(i, carry):
                levels(c * CH + i * step)
                return carry

            return lax.fori_loop(0, CH // step, group_of, carry)

        lax.fori_loop(0, n_chunk, chunk, 0)

    def edge_levels(k0):
        for d in range(UE):
            gather(ub[k0 + d], vb[k0 + d], k0 + d, bank_uv, sr_s, sr_n)

    in_chunks((0, 1), edge_levels, UE, (2, 3))

    def split_banks(banks):
        a, b = banks[0], turn(banks[1], 1)
        return jnp.where(even, a, b), turn(jnp.where(even, b, a), 1)

    for i in range(2):
        sc_w[i], sc_e[i] = split_banks(bank_uv.at[i])
    for c in planes:
        c.wait()
    kmt = kmt_v[...].astype(F32)
    ext[(KMT, *own)] = kmt
    for p in (KMT, DEPTH):
        pack(p)
    pl.semaphore_wait(barrier, len(where_to))
    first = wide_copies(KMT, 2)
    second = started([
        remote(sc_w, rc_e, "w"),
        remote(sc_e, rc_w, "e"),
        remote(sr_n, rr_s, "n"),
        remote(sr_s, rr_n, "s"),
        remote(sc_e.at[0, pl.ds(0, SUB)], rc_nw, "se"),
        remote(sc_w.at[1, pl.ds(ny - SUB, SUB)], rc_se, "nw"),
    ])

    dz = ext[(DEPTH, *own)] / jnp.maximum(kmt, 1.0)
    safe = jnp.where(kmt > 0, dz, 1.0)
    wet_v[...] = kmt
    dz_v[...] = TIME_STEP * dz
    cc_v[...] = (TIME_STEP * DIFF_KT) / (safe * safe)
    cum_v[...] = zero
    for ref in (tb, sb, pu, pv):
        ref[0] = zero
        ref[n_lev + 1] = zero
    for ref in (gc, gu, gv):
        ref[0] = zero + 1.0

    def pressure_levels(k0):
        cum = cum_v[...]
        for d in range(UE):
            k = k0 + d
            dens = BETA_S * (sb[k + 1] - 1.0) - ALPHA_T * (tb[k + 1] - 1.0)
            dens = jnp.where(k.astype(F32) < wet_v[...], dens, 0.0)
            cum = cum + dens
            pres = dz_v[...] * (cum - 0.5 * dens)
            pp[k] = pres
            b, m = slot_of(k, bank)
            pltpu.store(sp_w, turn(pres[:, :LANES], m + b), mask=lane == m + b)
            sp_s[pl.ds(k, 1)] = pres[first_row]
        cum_v[...] = cum

    in_chunks((2, 3), pressure_levels, UE)
    last_edges = started([remote(sp_w, rp_e, "w"), remote(sp_s, rp_n, "s")])

    def down_levels(i, carry):
        k0 = i * UN
        g, t_up, s_up = gc[k0], tb[k0], sb[k0]
        wet = k0.astype(F32) < wet_v[...]
        for d in range(UN):
            k = k0 + d
            below = (k + 1).astype(F32) < wet_v[...]
            coef = cc_v[...]
            up = jnp.where(below, coef, 0.0)
            inv = reduced(1.0 + up + coef * (1.0 - g))
            g = up * inv
            t_up = jnp.where(wet, (tb[k + 1] + coef * t_up) * inv, 0.0)
            s_up = jnp.where(wet, (sb[k + 1] + coef * s_up) * inv, 0.0)
            gc[k + 1] = g
            tb[k + 1] = t_up
            sb[k + 1] = s_up
            wet = below
        return carry

    lax.fori_loop(0, n_lev // UN, down_levels, 0)

    sent(first)
    received(first)
    for p in (KMT, DEPTH):
        unpack(p)
    line = iota((whole, wide), 0)
    seen = ((line >= H) | (row > 0)) & ((line < H + ny) | (row < n_rows - 1))
    kx = jnp.where(seen, ext[KMT], 0.0)
    ext[KMT] = kx
    dzx = jnp.where(seen, ext[DEPTH], 0.0) / jnp.maximum(kx, 1.0)
    ku = jnp.minimum(kx, pltpu.roll(kx, wide - 1, 1))
    kv = jnp.minimum(kx, pltpu.roll(kx, whole - 1, 0))
    dzu = 0.5 * (dzx + pltpu.roll(dzx, wide - 1, 1))
    dzv = 0.5 * (dzx + pltpu.roll(dzx, whole - 1, 0))
    xp[KU] = ku
    xp[KV] = kv
    xp[DZU] = dzu
    xp[DZV] = dzv
    xp[GU] = jnp.where(ku > 0, dt_sub * (ku * dzu), 0.0)
    xp[GV] = jnp.where(kv > 0, dt_sub * (kv * dzv), 0.0)
    xp[WD] = jnp.where(kx > 0, dt_sub, 0.0)
    xp[GW] = pltpu.roll(xp[GU], 1, 1)
    face_out[2] = wet_v[...]
    for i in range(2):
        count = xp[(KU + i, *own)]
        safe = jnp.where(count > 0, xp[(DZU + i, *own)], 1.0)
        faces[i] = count
        face_out[i] = count
        coefs[i] = (TIME_STEP * VISC_KV) / (safe * safe)
        push_v[i] = zero
        sum_v[i] = zero

    received(second)
    pair = lane // 2
    lev = jnp.where(pair < bank, pair + bank * (lane % 2), n_lev).astype(F32)

    def column(ref, count):
        return jnp.where(lev < count, ref, 0.0)

    u_w = column(rc_w[0], xp[KU, mid, at_w])
    v_w = column(rc_w[1], xp[KV, mid, at_w])
    u_e = column(rc_e[0], xp[KU, mid, at_e])
    v_e = column(rc_e[1], xp[KV, mid, at_e])
    u_last = column(sc_e[0], xp[KU, mid, nx - 1:nx])
    v_zero = column(sc_w[1], xp[KV, mid, FIRST])
    corner_u = jnp.where(lev[FIRST] < xp[KU, at_n, at_w], rc_nw[FIRST, :], 0.0)
    q_e = scaled((u_last + u_e) * (u_last + u_e))
    c_w = scaled((u_w + shift_north(u_w, corner_u)) * (v_w + v_zero))
    hc[1, 0], hc[1, 1] = merged(c_w, v_e)
    corner = jnp.where(lev[FIRST] < xp[KV, H - 1:H, at_e], rc_se[SUB - 1:], 0.0)
    corner_p[...] = jnp.transpose(jnp.broadcast_to(corner, (LANES, LANES)))
    corner_r[0:bank] = corner_p[pl.ds(0, bank, stride=2)]
    corner_r[bank:n_lev] = corner_p[pl.ds(1, n_lev - bank, stride=2)]
    row_lev = iota((n_row, nx), 0).astype(F32)

    def row_of(x, f, at):
        return jnp.where(row_lev < xp[KU + f, at, cols], x, 0.0)

    v_s = row_of(rr_s[1], 1, at_s)
    v_last = row_of(sr_n[1], 1, slice(H + ny - 1, H + ny))
    v_n = row_of(rr_n[1], 1, at_n)
    row_h[0] = row_of(rr_n[0], 0, at_n)
    row_h[1] = scaled((row_of(rr_s[0], 0, at_s) + row_of(sr_s[0], 0, slice(H, H + 1))) * (v_s + shift_east(v_s, corner_r[...])))
    row_h[2] = v_s
    row_h[3] = scaled((v_last + v_n) * (v_last + v_n))
    received(last_edges)
    for p in (ETA, TU, TV):
        pack(p)
    state = wide_copies(ETA, 3)
    hc[0, 0], hc[0, 1] = merged(u_w, q_e + rp_e[...])
    row_h[3] += jnp.where(below_wall, rp_n[...], 0.0)

    def forces(k, slot):
        kf = real(k)
        k = k if isinstance(k, int) else jnp.minimum(k, n_lev - 1)
        masked = []
        for f, ref in ((0, ub), (1, vb)):
            wet = kf < faces[f]
            masked.append(jnp.where(wet, ref[k], 0.0))
            s_now[slot, f] = masked[f]
            s_low[slot, f] = jnp.where(wet, coefs[f], 0.0)
        u, v = masked
        p = pp[k]
        b, m = slot_of(k, bank)
        u_n, corner_s, v_s, edge_v = [row_h[i, pl.ds(k, 1)] for i in range(4)]
        for i in range(2):
            s_edge[slot, i] = turn(hc[i, b], LANES - m)
        cen_u = shift_west(u, s_edge[slot, 0]) + u
        head = scaled(cen_u * cen_u) + p
        s_head[slot] = head
        corner = scaled((u + shift_north(u, u_n)) * (v + shift_east(v, s_edge[slot, 1])))
        s_corner[slot] = corner
        s_side[slot, 0] = (corner - shift_south(corner, corner_s)) - head
        cen_v = shift_south(v, v_s) + v
        head_v = scaled(cen_v * cen_v) + p
        s_side[slot, 1] = (shift_north(head_v, edge_v) - head_v) + corner

    def solve_down(k, slot, below):
        kf = k.astype(F32)
        head, corner = s_head[slot], s_corner[slot]
        grad_u = shift_east(head, s_edge[slot, 0]) + s_side[slot, 0]
        grad_v = s_side[slot, 1] - shift_west(corner, s_edge[slot, 1])
        for f, grad, part, gain in ((0, grad_u, pu, gu), (1, grad_v, pv, gv)):
            low, up = s_low[slot, f], s_low[below, f]
            inv = reduced(1.0 + up + low * (1.0 - gain[k]))
            gain[k + 1] = up * inv
            pull = jnp.where(kf < faces[f], grad, 0.0)
            push_v[f] += pull
            part[k + 1] = ((s_now[slot, f] - pull) + low * part[k]) * inv

    def momentum_levels(i, carry):
        k = UN * i
        for d in range(UN):
            forces(k + d + 1, (d + 1) % UN)
            solve_down(k + d, d, (d + 1) % UN)
        return carry

    forces(0, 0)
    lax.fori_loop(0, n_lev // UN, momentum_levels, 0)

    for f in range(2):
        ext[(FX + f, *own)] = xp[(DZU + f, *own)] * push_v[f] * (-1.0 / TIME_STEP)
        pack(FX + f)
    third = wide_copies(FX, 2)

    def upward(levels):
        def group_of(i, carry):
            levels(n_lev - 1 - i * UE)
            return carry

        lax.fori_loop(0, n_lev // UE, group_of, 0)

    def mix_levels(k0):
        t, s = tb[k0 + 2], sb[k0 + 2]
        for d in range(UE):
            k = k0 - d
            g = gc[k + 1]
            t = tb[k + 1] + g * t
            s = sb[k + 1] + g * s
            tb[k + 1] = t
            sb[k + 1] = s
            gather(t, s, k, bank_ts, tr_s, tr_n)

    upward(mix_levels)
    for i in range(2):
        tc_w[i], tc_e[i] = split_banks(bank_ts.at[i])
    tracer = started([
        remote(tc_w, qc_e, "w"),
        remote(tc_e, qc_w, "e"),
        remote(tr_n, qr_s, "n"),
        remote(tr_s, qr_n, "s"),
    ])

    def rise_levels(k0):
        u, v = pu[k0 + 2], pv[k0 + 2]
        sum_u, sum_w = sum_v[0], sum_v[1]
        for d in range(UE):
            k = k0 - d
            u = pu[k + 1] + gu[k + 1] * u
            v = pv[k + 1] + gv[k + 1] * v
            pu[k + 1] = u
            pv[k + 1] = v
            sum_u += u
            sum_w += v
            b, m = slot_of(k, bank)
            pltpu.store(su_e, turn(u[:, nx - LANES:], m + b + 1), mask=lane == m + b)
            sv_n[pl.ds(k, 1)] = v[last_row]
        sum_v[0], sum_v[1] = sum_u, sum_w

    upward(rise_levels)
    fourth = started([remote(su_e, ru_w, "e"), remote(sv_n, rv_s, "n")])

    sent(state)
    received(state)
    for p in (ETA, TU, TV):
        unpack(p)
        ext[p] = jnp.where((xp[WD] if p == ETA else xp[KU + p - TU]) > 0, ext[p], 0.0)
    xp[UW] = pltpu.roll(ext[TU], 1, 1)
    received(third)
    for f in range(2):
        unpack(FX + f)
        xp[BU + f] = jnp.where(xp[KU + f] > 0, dt_sub * ext[FX + f], 0.0)
    xp[BW] = pltpu.roll(xp[BU], 1, 1)
    acc[...] = jnp.zeros(acc.shape, F32)
    norm = 6.0 / (n_sub * (n_sub + 1) * (n_sub + 2))
    line8 = iota((SUB, wide), 0)
    t0 = H // SUB - 1

    def substep(n, lo, hi):
        tide_u, tide_v = tide[0, n], tide[1, n]
        weight = norm * ((n + 1) * (n_sub - n)).astype(F32)

        def finish(t, eta, rolled, rolled_next, u, u_w, v):
            rows = slice(SUB * t, SUB * t + SUB)
            eta_n = jnp.where(line8 == SUB - 1, rolled_next, rolled)
            eta_e = pltpu.roll(eta, wide - 1, 1)
            eta_w = pltpu.roll(eta, 1, 1)
            xp[UW, rows] = u_w + (xp[GW, rows] * (tide_u + (eta_w - eta)) + xp[BW, rows])
            u_new = u + (xp[GU, rows] * (tide_u + (eta - eta_e)) + xp[BU, rows])
            v_new = v + (xp[GV, rows] * (tide_v + (eta - eta_n)) + xp[BV, rows])
            ext[TU, rows] = u_new
            ext[TV, rows] = v_new
            if t0 <= t < (H + ny) // SUB:
                at = slice(SUB * (t - t0), SUB * (t - t0) + SUB)
                acc[0, at] += weight * u_new
                acc[1, at, :nx] += weight * v_new[:, :nx]

        last = None
        v_below = jnp.zeros((SUB, wide), F32)
        for t in range(lo, hi):
            rows = slice(SUB * t, SUB * t + SUB)
            u, u_w, v = ext[TU, rows], xp[UW, rows], ext[TV, rows]
            v_roll = pltpu.roll(v, 1, 0)
            v_s = jnp.where(line8 == 0, v_below, v_roll)
            v_below = v_roll
            eta = ext[ETA, rows] - xp[WD, rows] * ((u - u_w) + (v - v_s))
            ext[ETA, rows] = eta
            rolled = pltpu.roll(eta, SUB - 1, 0)
            if last is not None:
                eta_b, rolled_b, *face_b = last
                finish(t - 1, eta_b, rolled_b, rolled, *face_b)
            last = (eta, rolled, u, u_w, v)
        finish(hi - 1, eta, rolled, rolled, u, u_w, v)

    edge_tiles = H // SUB
    for e in range(edge_tiles, 0, -1):
        begin = max(0, n_sub + 1 - SUB * e) if e < edge_tiles else 0
        end = n_sub + 1 - SUB * (e - 1) if e > 1 else n_sub
        span = (edge_tiles - e, whole // SUB - edge_tiles + e)

        def two(i, carry, begin=begin, span=span):
            substep(begin + 2 * i, *span)
            substep(begin + 2 * i + 1, *span)
            return carry

        lax.fori_loop(0, (end - begin) // 2, two, 0)
        if (end - begin) % 2:
            substep(jnp.int32(end - 1), *span)

    for i in range(3):
        bar_out[i] = ext[(ETA + i, *own)]

    def safe_depth(f, rows, lanes):
        depth = xp[KU + f, rows, lanes] * xp[DZU + f, rows, lanes]
        return jnp.where(depth > 0, depth, 1.0)

    inner = slice(SUB, SUB + ny)
    for f in range(2):
        corr_out[f] = (acc[f, inner, cols] - xp[DZU + f, mid, cols] * sum_v[f]) / safe_depth(f, mid, cols)
    received(fourth)
    star = ru_w[...]
    fix = (acc[0, inner, at_w] - xp[DZU, mid, at_w] * jnp.sum(star, axis=1, keepdims=True)) / safe_depth(0, mid, at_w)
    u_c = column(star + fix, xp[KU, mid, at_w])
    star = row_of(rv_s[...], 1, at_s)
    total = jnp.sum(star, axis=0, keepdims=True)
    fix = (acc[1, SUB - 1:SUB, cols] - xp[DZV, at_s, cols] * total) / safe_depth(1, at_s, cols)
    vcs_out[...] = row_of(star + fix, 1, at_s)
    received(tracer)
    for i in range(2):
        halo_out[i, 0], halo_out[i, 1] = merged((0.5 * TIME_STEP) * u_c * (qc_w[i] + tc_w[i]), qc_e[i])
    trow_n_out[...] = jnp.where(below_wall, qr_n[...], 0.0)
    trow_s_out[...] = jnp.where(above_wall, qr_s[...], 0.0)
    sent(second + last_edges + third + tracer + fourth)


def last_kernel(us, vs, tm, sm, bar, corr, faces, vcs, halo, trow_n, trow_s,
                eta_out, tu_out, tv_out, u_out, v_out, t_out, s_out,
                new_u, new_v, new_t, new_s, flux, rest, turned, bar_sem, out_sem, *, bank):
    n_lev = u_out.shape[0]
    planes = [pltpu.make_async_copy(bar.at[i], ref, bar_sem.at[i]) for i, ref in enumerate((eta_out, tu_out, tv_out))]
    for c in planes:
        c.start()

    def fluxes(k, slot):
        kf = real(k)
        u = jnp.where(kf < faces[0], us[k + 1] + corr[0], 0.0)
        v = jnp.where(kf < faces[1], vs[k + 1] + corr[1], 0.0)
        new_u[k] = u
        new_v[k] = v
        u = (0.5 * TIME_STEP) * u
        v = (0.5 * TIME_STEP) * v
        here = pl.ds(k, 1)
        v_s = (0.5 * TIME_STEP) * vcs[here]
        b, m = slot_of(k, bank)
        for a, src in ((0, tm), (1, sm)):
            x = src[k + 1]
            turned[slot, a] = turn(halo[a, b], LANES - m)
            flux_x = u * (x + shift_east(x, turned[slot, a]))
            flux_y = v * (x + shift_north(x, trow_n[a, here]))
            edge_y = v_s * (trow_s[a, here] + x[FIRST])
            flux[slot, a] = flux_x
            rest[slot, a] = (x - flux_x) - (flux_y - shift_south(flux_y, edge_y))

    def finish(k, slot):
        wet = k.astype(F32) < faces[2]
        for a, dst in ((0, new_t), (1, new_s)):
            moved = shift_west(flux[slot, a], turned[slot, a])
            dst[k] = jnp.where(wet, rest[slot, a] + moved, 0.0)

    results = (new_u, u_out), (new_v, v_out), (new_t, t_out), (new_s, s_out)

    def copies(c):
        return [pltpu.make_async_copy(src.at[pl.ds(c * KB, KB)], dst.at[pl.ds(c * KB, KB)], out_sem.at[i])
                for i, (src, dst) in enumerate(results)]

    def chunk(c, carry):
        def done(d):
            finish(c * UE + d, d)
            if d % KB == KB - 1:
                for copy in copies(c * (UE // KB) + d // KB):
                    copy.start()

        for d in range(1, UE):
            fluxes(c * UE + d, d)
            done(d - 1)
        fluxes(jnp.minimum(c * UE + UE, n_lev - 1), 0)
        done(UE - 1)
        return carry

    fluxes(0, 0)
    lax.fori_loop(0, n_lev // UE, chunk, 0)
    for i, (src, dst) in enumerate(results):
        pltpu.make_async_copy(src, dst, out_sem.at[i]).wait()
    for c in planes:
        c.wait()


def solution(mesh):
    n_cols, n_rows = mesh.shape["col"], mesh.shape["row"]

    def local_step(vel_u, vel_v, value_a11, salinity, sea_level, trans_u, trans_v, bathymetry, kmt_levels, tide_force):
        n_lev, ny, nx = vel_u.shape
        whole, wide = ny + 2 * H, nx + LANES
        n_chunk, bank = n_lev // CH, (n_lev + 1) // 2
        hbm_spec = pl.BlockSpec(memory_space=pltpu.HBM)
        vmem_spec = pl.BlockSpec(memory_space=pltpu.VMEM)
        cube = (n_lev, ny, nx)
        deep = (n_lev + 2, ny, nx)
        n_row = n_lev + -n_lev % SUB
        column, pair_c, rows1, rows2 = (ny, LANES), (2, ny, LANES), (n_row, nx), (2, n_row, nx)
        banks, two, small, both = (2, 2, ny, LANES), (2, ny, nx), (SUB, LANES), (UN, 2, ny, nx)

        edges = (UN, 2, ny, LANES)

        def sds(*shape):
            return jax.ShapeDtypeStruct(shape, F32)

        def bufs(*shapes):
            return [pltpu.VMEM(shape, F32) for shape in shapes]

        def sems(*shape):
            return pltpu.SemaphoreType.DMA(shape)

        passed = [(3, ny, nx), two, (3, ny, nx), rows1, banks, rows2, rows2]
        *cubes, bar, corr, face, vcs, halo, trow_n, trow_s = pl.pallas_call(
            functools.partial(main_kernel, n_rows, n_cols),
            out_shape=bufs(*[deep] * 4, *passed),
            in_specs=[hbm_spec] * 10,
            out_specs=[vmem_spec] * (4 + len(passed)),
            scratch_shapes=[
                pltpu.SMEM(tide_force.shape[::-1], F32),
                pltpu.VMEM((ny, nx), jnp.int32),
                *bufs((7, whole, wide), (12, whole, wide), (2, ny + SUB, wide)),
                *bufs(*[(7, 3 * SUB, LANES)] * 2, *[(7, 2 * SUB, LANES)] * 2, *[(7, SUB, LANES)] * 4),
                *bufs(cube, cube, *[deep] * 3, cube, *[(ny, nx)] * 4, two, two, two, two, both, both, (UN, ny, nx), (UN, ny, nx), both, edges, (4, n_row, nx), (n_row, LANES)),
                *bufs(banks, banks, pair_c, pair_c, column, pair_c, pair_c, column, small, small, banks, (LANES, LANES)),
                *bufs(rows2, rows2, rows1, rows2, rows2, rows1),
                *bufs(pair_c, pair_c, rows2, rows2, pair_c, pair_c, rows2, rows2, column, rows1, column, rows1),
                sems(6), sems(4, n_chunk), sems(38), sems(38),
            ],
            compiler_params=pltpu.CompilerParams(collective_id=0, has_side_effects=True, vmem_limit_bytes=44 * 2**20),
        )(kmt_levels, bathymetry, sea_level, trans_u, trans_v, vel_u, vel_v, value_a11, salinity, tide_force.T)

        return pl.pallas_call(
            functools.partial(last_kernel, bank=bank),
            out_shape=[sds(ny, nx)] * 3 + [sds(*cube)] * 4,
            in_specs=[vmem_spec] * (4 + len(passed)),
            out_specs=[hbm_spec] * 7,
            scratch_shapes=[*bufs(*[cube] * 4, (UE, 2, ny, nx), (UE, 2, ny, nx), (UE, 2, ny, LANES)), sems(3), sems(4)],
            compiler_params=pltpu.CompilerParams(vmem_limit_bytes=24 * 2**20),
        )(*cubes, bar, corr, face, vcs, halo, trow_n, trow_s)

    spec_cube = P(None, "row", "col")
    spec_plane = P("row", "col")
    return jax.shard_map(local_step, mesh=mesh, in_specs=(spec_cube,) * 4 + (spec_plane,) * 5 + (P(None, None),),
                         out_specs=(spec_plane,) * 3 + (spec_cube,) * 4, check_vma=False)
```

```python
import functools

import jax
import jax.numpy as jnp
from jax import lax
from jax.experimental import pallas as pl
from jax.experimental.pallas import tpu as pltpu
from jax.sharding import PartitionSpec as P

TIME_STEP = 4.0
ALPHA_T = 0.02
BETA_S = 0.015
VISC_KV = 0.001
DIFF_KT = 0.0005
MESH = pl.DeviceIdType.MESH
H = 32
CH = 15
UN = 15
UD = 5
UE = 15
KB = 5
SUB, LANES = 8, 128
LAST = LANES - 1
F32 = jnp.float32
HEAD = 0.25 * TIME_STEP
KMT, DEPTH, ETA, TU, TV, FX, FY = range(7)
KU, KV, DZU, DZV, GU, GV, BU, BV, WD, GW, BW, UW = range(12)
FIRST = slice(0, 1)


def iota(shape, axis):
    return lax.broadcasted_iota(jnp.int32, shape, axis)


def reduced(x):
    return pl.reciprocal(x, approx=False)


def scaled(x):
    return x if HEAD == 1.0 else HEAD * x


def lane_of(x):
    return iota(x.shape, 1)


def slot_of(k, bank):
    b = int(k >= bank) if isinstance(k, int) else (k >= bank).astype(jnp.int32)
    return b, 2 * (k - b * bank)


def real(k):
    return float(k) if isinstance(k, int) else k.astype(F32)


def turn(x, n):
    return pltpu.roll(x, n % LANES if isinstance(n, int) else n, 1)


def shift_east(x, halo):
    left, right = turn(x[:, :LANES], -1), turn(x[:, LANES:], -1)
    edge = lane_of(left) == LAST
    return jnp.concatenate([jnp.where(edge, right, left), jnp.where(edge, halo, right)], axis=1)


def shift_west(x, halo):
    left, right = turn(x[:, :LANES], 1), turn(x[:, LANES:], 1)
    edge = lane_of(left) == 0
    return jnp.concatenate([jnp.where(edge, halo, left), jnp.where(edge, left, right)], axis=1)


def tiles_of(x):
    return [x[SUB * t:SUB * t + SUB] for t in range(x.shape[0] // SUB)]


def shift_north(x, halo):
    rolled = [pltpu.roll(t, SUB - 1, 0) for t in tiles_of(x)]
    edge = iota(rolled[0].shape, 0) == SUB - 1
    rolled.append(jnp.broadcast_to(halo, rolled[0].shape))
    return jnp.concatenate([jnp.where(edge, b, a) for a, b in zip(rolled[:-1], rolled[1:])], axis=0)


def shift_south(x, halo):
    rolled = [pltpu.roll(t, 1, 0) for t in tiles_of(x)]
    edge = iota(rolled[0].shape, 0) == 0
    rolled.insert(0, jnp.broadcast_to(halo, rolled[0].shape))
    return jnp.concatenate([jnp.where(edge, a, b) for a, b in zip(rolled[:-1], rolled[1:])], axis=0)


def merged(west, east):
    even = lane_of(west) % 2 == 0
    back = turn(east, -1)
    return jnp.where(even, west, back), turn(jnp.where(even, back, west), -1)


def main_kernel(n_rows, n_cols,
                kmt_in, bat_in, eta_in, tu_in, tv_in, u_in, v_in, t_in, s_in, tide_in,
                pu, pv, tb, sb, bar_out, corr_out, face_out, vcs_out,
                halo_out, trow_n_out, trow_s_out,
                tide, kmt_v, ext, xp, acc, pk_w, pk_e, r_e, r_w, r_ne, r_nw, r_se, r_sw,
                ub, vb, gc, gu, gv, pp, wet_v, dz_v, cc_v, cum_v, faces, coefs, push_v, sum_v, s_now, s_low, s_head, s_corner, s_side, s_edge, row_h, corner_r,
                bank_uv, bank_ts, sc_w, sc_e, sp_w, rc_e, rc_w, rp_e, rc_nw, rc_se, hc, corner_p,
                sr_n, sr_s, sp_s, rr_n, rr_s, rp_n,
                tc_w, tc_e, tr_n, tr_s, qc_e, qc_w, qr_n, qr_s, su_e, sv_n, ru_w, rv_s,
                plane_sem, in_sem, send_sem, recv_sem):
    n_sub = tide.shape[1]
    n_lev = u_in.shape[0]
    n_chunk = n_lev // CH
    bank, n_row = (n_lev + 1) // 2, sp_s.shape[0]
    ny, nx = kmt_in.shape
    dt_sub = TIME_STEP / n_sub
    col, row = lax.axis_index("col"), lax.axis_index("row")
    east, west = lax.rem(col + 1, n_cols), lax.rem(col + n_cols - 1, n_cols)
    north, south = lax.rem(row + 1, n_rows), lax.rem(row + n_rows - 1, n_rows)
    where_to = {"n": (col, north), "s": (col, south), "e": (east, row), "w": (west, row),
                "ne": (east, north), "nw": (west, north), "se": (east, south), "sw": (west, south)}
    own = (pl.ds(H, ny), pl.ds(0, nx))
    mid, cols = slice(H, H + ny), slice(0, nx)
    at_n, at_s = slice(H + ny, H + ny + 1), slice(H - 1, H)
    whole, wide = ny + 2 * H, nx + LANES
    at_w, at_e = slice(wide - 1, wide), slice(nx, nx + 1)
    first_row, last_row = FIRST, slice(ny - 1, ny)

    planes = [pltpu.make_async_copy(kmt_in, kmt_v, plane_sem.at[KMT])]
    for i, ref in ((DEPTH, bat_in), (ETA, eta_in), (TU, tu_in), (TV, tv_in)):
        planes.append(pltpu.make_async_copy(ref, ext.at[(i, *own)], plane_sem.at[i]))
    planes.append(pltpu.make_async_copy(tide_in, tide, plane_sem.at[FX]))
    def load(a, c):
        src, dst, off = ((u_in, ub, 0), (v_in, vb, 0), (t_in, tb, 1), (s_in, sb, 1))[a]
        return pltpu.make_async_copy(src.at[pl.ds(c * CH, CH)], dst.at[pl.ds(c * CH + off, CH)], in_sem.at[a, c])

    for c in range(n_chunk):
        load(0, c).start()
        load(1, c).start()
    for c in planes:
        c.start()

    barrier = pltpu.get_barrier_semaphore()
    for c_id, r_id in where_to.values():
        pl.semaphore_signal(barrier, inc=1, device_id={"col": c_id, "row": r_id}, device_id_type=MESH)

    used = []

    def remote(src, dst, to):
        c_id, r_id = where_to[to]
        i = len(used)
        used.append(i)
        copy = pltpu.make_async_remote_copy(src_ref=src, dst_ref=dst, send_sem=send_sem.at[i], recv_sem=recv_sem.at[i],
                                            device_id={"col": c_id, "row": r_id}, device_id_type=MESH)
        return copy, to[0]

    below_wall, above_wall = row < n_rows - 1, row > 0

    def sends(copies, act):
        for copy, to in copies:
            if to in "ns":
                pl.when(below_wall if to == "n" else above_wall)(functools.partial(act, copy))
            else:
                act(copy)

    def started(copies):
        sends(copies, lambda c: c.start())
        return copies

    def sent(copies):
        sends(copies, lambda c: c.wait_send())

    def received(copies):
        for copy, to in copies:
            if to in "ns":
                pl.when(above_wall if to == "n" else below_wall)(copy.wait_recv)
            else:
                copy.wait_recv()

    def wide_copies(p0, n):
        ps = pl.ds(p0, n)
        low, mids, high = pl.ds(0, 2 * SUB), pl.ds(0, SUB), pl.ds(2 * SUB, SUB)
        return started([
            remote(ext.at[ps, pl.ds(H, H), pl.ds(0, nx)], ext.at[ps, pl.ds(H + ny, H), pl.ds(0, nx)], "s"),
            remote(ext.at[ps, pl.ds(ny, H), pl.ds(0, nx)], ext.at[ps, pl.ds(0, H), pl.ds(0, nx)], "n"),
            remote(pk_w.at[ps, low], r_e.at[ps], "w"),
            remote(pk_e.at[ps, low], r_w.at[ps], "e"),
            remote(pk_w.at[ps, mids], r_ne.at[ps], "sw"),
            remote(pk_e.at[ps, mids], r_nw.at[ps], "se"),
            remote(pk_w.at[ps, high], r_se.at[ps], "nw"),
            remote(pk_e.at[ps, high], r_sw.at[ps], "ne"),
        ])

    group = iota((SUB, LANES), 1) // H
    n_groups = LANES // H

    def pack(p):
        x = ext[(p, *own)]
        for ref, tile, g0 in ((pk_w, x[:, :LANES], 0), (pk_e, x[:, nx - LANES:], n_groups - 1)):
            for at, first, count in ((0, 0, 4), (1, 4, 2), (2, 2, 4)):
                total = jnp.zeros((SUB, LANES), F32)
                for q in range(count):
                    rows = tile[SUB * (first + q):SUB * (first + q) + SUB]
                    rows = turn(rows, H * (q - g0)) if q != g0 else rows
                    total = jnp.where(group == q, rows, total)
                ref[p, SUB * at:SUB * at + SUB, :] = total

    def unpack(p):
        edge = H // SUB
        for t in range(whole // SUB):
            if t < edge:
                e_tile, w_tile, q = r_se[p], r_sw[p], t
            elif t < (H + ny) // SUB:
                rows = slice(SUB * ((t - edge) // n_groups), SUB * ((t - edge) // n_groups) + SUB)
                e_tile, w_tile, q = r_e[p, rows], r_w[p, rows], (t - edge) % n_groups
            else:
                e_tile, w_tile, q = r_ne[p], r_nw[p], t - (H + ny) // SUB
            e_tile = turn(e_tile, -H * q) if q else e_tile
            w_tile = turn(w_tile, H * (n_groups - 1 - q)) if q != n_groups - 1 else w_tile
            side = jnp.where(group == 0, e_tile, jnp.where(group == n_groups - 1, w_tile, 0.0))
            ext[p, SUB * t:SUB * t + SUB, nx:] = side

    zero = jnp.zeros((ny, nx), F32)
    for ref in (bank_uv, bank_ts, sp_w, su_e):
        ref[...] = jnp.zeros(ref.shape, F32)
    lane = iota((ny, LANES), 1)
    even = lane % 2 == 0

    def both_edges(x):
        return jnp.where(lane < LANES // 2, x[:, :LANES], x[:, nx - LANES:])

    def gather(x, y, k, banks, rows_s, rows_n):
        b, m = slot_of(k, bank)
        here = ((lane + 1 - m) & LAST) < 2
        pltpu.store(banks.at[0, b], turn(both_edges(x), m), mask=here)
        pltpu.store(banks.at[1, b], turn(both_edges(y), m), mask=here)
        here = pl.ds(k, 1)
        rows_s[0, here] = x[first_row]
        rows_s[1, here] = y[first_row]
        rows_n[0, here] = x[last_row]
        rows_n[1, here] = y[last_row]

    def in_chunks(arrays, levels, step, follow=()):
        def chunk(c, carry):
            for a in arrays:
                load(a, c).wait()
            if follow:
                for a in follow:
                    load(a, c).start()

            def group_of(i, carry):
                levels(c * CH + i * step)
                return carry

            return lax.fori_loop(0, CH // step, group_of, carry)

        lax.fori_loop(0, n_chunk, chunk, 0)

    def edge_levels(k0):
        for d in range(UE):
            gather(ub[k0 + d], vb[k0 + d], k0 + d, bank_uv, sr_s, sr_n)

    in_chunks((0, 1), edge_levels, UE, (2, 3))

    def split_banks(banks):
        a, b = banks[0], turn(banks[1], 1)
        return jnp.where(even, a, b), turn(jnp.where(even, b, a), 1)

    for i in range(2):
        sc_w[i], sc_e[i] = split_banks(bank_uv.at[i])
    for c in planes:
        c.wait()
    kmt = kmt_v[...].astype(F32)
    ext[(KMT, *own)] = kmt
    for p in (KMT, DEPTH):
        pack(p)
    pl.semaphore_wait(barrier, len(where_to))
    first = wide_copies(KMT, 2)
    second = started([
        remote(sc_w, rc_e, "w"),
        remote(sc_e, rc_w, "e"),
        remote(sr_n, rr_s, "n"),
        remote(sr_s, rr_n, "s"),
        remote(sc_e.at[0, pl.ds(0, SUB)], rc_nw, "se"),
        remote(sc_w.at[1, pl.ds(ny - SUB, SUB)], rc_se, "nw"),
    ])

    dz = ext[(DEPTH, *own)] / jnp.maximum(kmt, 1.0)
    safe = jnp.where(kmt > 0, dz, 1.0)
    wet_v[...] = kmt
    dz_v[...] = TIME_STEP * dz
    cc_v[...] = (TIME_STEP * DIFF_KT) / (safe * safe)
    cum_v[...] = zero
    for ref in (tb, sb, pu, pv):
        ref[0] = zero
        ref[n_lev + 1] = zero
    for ref in (gc, gu, gv):
        ref[0] = zero + 1.0

    def pressure_levels(k0):
        cum = cum_v[...]
        for d in range(UE):
            k = k0 + d
            dens = BETA_S * (sb[k + 1] - 1.0) - ALPHA_T * (tb[k + 1] - 1.0)
            dens = jnp.where(k.astype(F32) < wet_v[...], dens, 0.0)
            cum = cum + dens
            pres = dz_v[...] * (cum - 0.5 * dens)
            pp[k] = pres
            b, m = slot_of(k, bank)
            pltpu.store(sp_w, turn(pres[:, :LANES], m + b), mask=lane == m + b)
            sp_s[pl.ds(k, 1)] = pres[first_row]
        cum_v[...] = cum

    in_chunks((2, 3), pressure_levels, UE)
    last_edges = started([remote(sp_w, rp_e, "w"), remote(sp_s, rp_n, "s")])

    def down_levels(i, carry):
        k0 = i * UD
        g, t_up, s_up = gc[k0], tb[k0], sb[k0]
        wet = k0.astype(F32) < wet_v[...]
        for d in range(UD):
            k = k0 + d
            below = (k + 1).astype(F32) < wet_v[...]
            coef = cc_v[...]
            up = jnp.where(below, coef, 0.0)
            inv = reduced(1.0 + up + coef * (1.0 - g))
            g = up * inv
            t_up = jnp.where(wet, (tb[k + 1] + coef * t_up) * inv, 0.0)
            s_up = jnp.where(wet, (sb[k + 1] + coef * s_up) * inv, 0.0)
            gc[k + 1] = g
            tb[k + 1] = t_up
            sb[k + 1] = s_up
            wet = below
        return carry

    lax.fori_loop(0, n_lev // UD, down_levels, 0)

    sent(first)
    received(first)
    for p in (KMT, DEPTH):
        unpack(p)
    line = iota((whole, wide), 0)
    seen = ((line >= H) | (row > 0)) & ((line < H + ny) | (row < n_rows - 1))
    kx = jnp.where(seen, ext[KMT], 0.0)
    ext[KMT] = kx
    dzx = jnp.where(seen, ext[DEPTH], 0.0) / jnp.maximum(kx, 1.0)
    ku = jnp.minimum(kx, pltpu.roll(kx, wide - 1, 1))
    kv = jnp.minimum(kx, pltpu.roll(kx, whole - 1, 0))
    dzu = 0.5 * (dzx + pltpu.roll(dzx, wide - 1, 1))
    dzv = 0.5 * (dzx + pltpu.roll(dzx, whole - 1, 0))
    xp[KU] = ku
    xp[KV] = kv
    xp[DZU] = dzu
    xp[DZV] = dzv
    xp[GU] = jnp.where(ku > 0, dt_sub * (ku * dzu), 0.0)
    xp[GV] = jnp.where(kv > 0, dt_sub * (kv * dzv), 0.0)
    xp[WD] = jnp.where(kx > 0, dt_sub, 0.0)
    xp[GW] = pltpu.roll(xp[GU], 1, 1)
    face_out[2] = wet_v[...]
    for i in range(2):
        count = xp[(KU + i, *own)]
        safe = jnp.where(count > 0, xp[(DZU + i, *own)], 1.0)
        faces[i] = count
        face_out[i] = count
        coefs[i] = (TIME_STEP * VISC_KV) / (safe * safe)
        push_v[i] = zero
        sum_v[i] = zero

    received(second)
    pair = lane // 2
    lev = jnp.where(pair < bank, pair + bank * (lane % 2), n_lev).astype(F32)

    def column(ref, count):
        return jnp.where(lev < count, ref, 0.0)

    u_w = column(rc_w[0], xp[KU, mid, at_w])
    v_w = column(rc_w[1], xp[KV, mid, at_w])
    u_e = column(rc_e[0], xp[KU, mid, at_e])
    v_e = column(rc_e[1], xp[KV, mid, at_e])
    u_last = column(sc_e[0], xp[KU, mid, nx - 1:nx])
    v_zero = column(sc_w[1], xp[KV, mid, FIRST])
    corner_u = jnp.where(lev[FIRST] < xp[KU, at_n, at_w], rc_nw[FIRST, :], 0.0)
    q_e = scaled((u_last + u_e) * (u_last + u_e))
    c_w = scaled((u_w + shift_north(u_w, corner_u)) * (v_w + v_zero))
    hc[1, 0], hc[1, 1] = merged(c_w, v_e)
    corner = jnp.where(lev[FIRST] < xp[KV, H - 1:H, at_e], rc_se[SUB - 1:], 0.0)
    corner_p[...] = jnp.transpose(jnp.broadcast_to(corner, (LANES, LANES)))
    corner_r[0:bank] = corner_p[pl.ds(0, bank, stride=2)]
    corner_r[bank:n_lev] = corner_p[pl.ds(1, n_lev - bank, stride=2)]
    row_lev = iota((n_row, nx), 0).astype(F32)

    def row_of(x, f, at):
        return jnp.where(row_lev < xp[KU + f, at, cols], x, 0.0)

    v_s = row_of(rr_s[1], 1, at_s)
    v_last = row_of(sr_n[1], 1, slice(H + ny - 1, H + ny))
    v_n = row_of(rr_n[1], 1, at_n)
    row_h[0] = row_of(rr_n[0], 0, at_n)
    row_h[1] = scaled((row_of(rr_s[0], 0, at_s) + row_of(sr_s[0], 0, slice(H, H + 1))) * (v_s + shift_east(v_s, corner_r[...])))
    row_h[2] = v_s
    row_h[3] = scaled((v_last + v_n) * (v_last + v_n))
    received(last_edges)
    for p in (ETA, TU, TV):
        pack(p)
    state = wide_copies(ETA, 3)
    hc[0, 0], hc[0, 1] = merged(u_w, q_e + rp_e[...])
    row_h[3] += jnp.where(below_wall, rp_n[...], 0.0)

    def forces(k, slot):
        kf = real(k)
        k = k if isinstance(k, int) else jnp.minimum(k, n_lev - 1)
        masked = []
        for f, ref in ((0, ub), (1, vb)):
            wet = kf < faces[f]
            masked.append(jnp.where(wet, ref[k], 0.0))
            s_now[slot, f] = masked[f]
            s_low[slot, f] = jnp.where(wet, coefs[f], 0.0)
        u, v = masked
        p = pp[k]
        b, m = slot_of(k, bank)
        u_n, corner_s, v_s, edge_v = [row_h[i, pl.ds(k, 1)] for i in range(4)]
        for i in range(2):
            s_edge[slot, i] = turn(hc[i, b], LANES - m)
        cen_u = shift_west(u, s_edge[slot, 0]) + u
        head = scaled(cen_u * cen_u) + p
        s_head[slot] = head
        corner = scaled((u + shift_north(u, u_n)) * (v + shift_east(v, s_edge[slot, 1])))
        s_corner[slot] = corner
        s_side[slot, 0] = (corner - shift_south(corner, corner_s)) - head
        cen_v = shift_south(v, v_s) + v
        head_v = scaled(cen_v * cen_v) + p
        s_side[slot, 1] = (shift_north(head_v, edge_v) - head_v) + corner

    def solve_down(k, slot, below):
        kf = k.astype(F32)
        head, corner = s_head[slot], s_corner[slot]
        grad_u = shift_east(head, s_edge[slot, 0]) + s_side[slot, 0]
        grad_v = s_side[slot, 1] - shift_west(corner, s_edge[slot, 1])
        for f, grad, part, gain in ((0, grad_u, pu, gu), (1, grad_v, pv, gv)):
            low, up = s_low[slot, f], s_low[below, f]
            inv = reduced(1.0 + up + low * (1.0 - gain[k]))
            gain[k + 1] = up * inv
            pull = jnp.where(kf < faces[f], grad, 0.0)
            push_v[f] += pull
            part[k + 1] = ((s_now[slot, f] - pull) + low * part[k]) * inv

    def momentum_levels(i, carry):
        k = UN * i
        for d in range(UN):
            forces(k + d + 1, (d + 1) % UN)
            solve_down(k + d, d, (d + 1) % UN)
        return carry

    forces(0, 0)
    lax.fori_loop(0, n_lev // UN, momentum_levels, 0)

    for f in range(2):
        ext[(FX + f, *own)] = xp[(DZU + f, *own)] * push_v[f] * (-1.0 / TIME_STEP)
        pack(FX + f)
    third = wide_copies(FX, 2)

    def upward(levels):
        def group_of(i, carry):
            levels(n_lev - 1 - i * UE)
            return carry

        lax.fori_loop(0, n_lev // UE, group_of, 0)

    def mix_levels(k0):
        t, s = tb[k0 + 2], sb[k0 + 2]
        for d in range(UE):
            k = k0 - d
            g = gc[k + 1]
            t = tb[k + 1] + g * t
            s = sb[k + 1] + g * s
            tb[k + 1] = t
            sb[k + 1] = s
            gather(t, s, k, bank_ts, tr_s, tr_n)

    upward(mix_levels)
    for i in range(2):
        tc_w[i], tc_e[i] = split_banks(bank_ts.at[i])
    tracer = started([
        remote(tc_w, qc_e, "w"),
        remote(tc_e, qc_w, "e"),
        remote(tr_n, qr_s, "n"),
        remote(tr_s, qr_n, "s"),
    ])

    def rise_levels(k0):
        u, v = pu[k0 + 2], pv[k0 + 2]
        sum_u, sum_w = sum_v[0], sum_v[1]
        for d in range(UE):
            k = k0 - d
            u = pu[k + 1] + gu[k + 1] * u
            v = pv[k + 1] + gv[k + 1] * v
            pu[k + 1] = u
            pv[k + 1] = v
            sum_u += u
            sum_w += v
            b, m = slot_of(k, bank)
            pltpu.store(su_e, turn(u[:, nx - LANES:], m + b + 1), mask=lane == m + b)
            sv_n[pl.ds(k, 1)] = v[last_row]
        sum_v[0], sum_v[1] = sum_u, sum_w

    upward(rise_levels)
    fourth = started([remote(su_e, ru_w, "e"), remote(sv_n, rv_s, "n")])

    sent(state)
    received(state)
    for p in (ETA, TU, TV):
        unpack(p)
        ext[p] = jnp.where((xp[WD] if p == ETA else xp[KU + p - TU]) > 0, ext[p], 0.0)
    xp[UW] = pltpu.roll(ext[TU], 1, 1)
    received(third)
    for f in range(2):
        unpack(FX + f)
        xp[BU + f] = jnp.where(xp[KU + f] > 0, dt_sub * ext[FX + f], 0.0)
    xp[BW] = pltpu.roll(xp[BU], 1, 1)
    acc[...] = jnp.zeros(acc.shape, F32)
    norm = 6.0 / (n_sub * (n_sub + 1) * (n_sub + 2))
    line8 = iota((SUB, wide), 0)
    t0 = H // SUB - 1

    def substep(n, lo, hi):
        tide_u, tide_v = tide[0, n], tide[1, n]
        weight = norm * ((n + 1) * (n_sub - n)).astype(F32)

        def finish(t, eta, rolled, rolled_next, u, u_w, v):
            rows = slice(SUB * t, SUB * t + SUB)
            eta_n = jnp.where(line8 == SUB - 1, rolled_next, rolled)
            eta_e = pltpu.roll(eta, wide - 1, 1)
            eta_w = pltpu.roll(eta, 1, 1)
            xp[UW, rows] = u_w + (xp[GW, rows] * (tide_u + (eta_w - eta)) + xp[BW, rows])
            u_new = u + (xp[GU, rows] * (tide_u + (eta - eta_e)) + xp[BU, rows])
            v_new = v + (xp[GV, rows] * (tide_v + (eta - eta_n)) + xp[BV, rows])
            ext[TU, rows] = u_new
            ext[TV, rows] = v_new
            if t0 <= t < (H + ny) // SUB:
                at = slice(SUB * (t - t0), SUB * (t - t0) + SUB)
                acc[0, at] += weight * u_new
                acc[1, at, :nx] += weight * v_new[:, :nx]

        last = None
        v_below = jnp.zeros((SUB, wide), F32)
        for t in range(lo, hi):
            rows = slice(SUB * t, SUB * t + SUB)
            u, u_w, v = ext[TU, rows], xp[UW, rows], ext[TV, rows]
            v_roll = pltpu.roll(v, 1, 0)
            v_s = jnp.where(line8 == 0, v_below, v_roll)
            v_below = v_roll
            eta = ext[ETA, rows] - xp[WD, rows] * ((u - u_w) + (v - v_s))
            ext[ETA, rows] = eta
            rolled = pltpu.roll(eta, SUB - 1, 0)
            if last is not None:
                eta_b, rolled_b, *face_b = last
                finish(t - 1, eta_b, rolled_b, rolled, *face_b)
            last = (eta, rolled, u, u_w, v)
        finish(hi - 1, eta, rolled, rolled, u, u_w, v)

    edge_tiles = H // SUB
    for e in range(edge_tiles, 0, -1):
        begin = max(0, n_sub + 1 - SUB * e) if e < edge_tiles else 0
        end = n_sub + 1 - SUB * (e - 1) if e > 1 else n_sub
        span = (edge_tiles - e, whole // SUB - edge_tiles + e)

        def two(i, carry, begin=begin, span=span):
            substep(begin + 2 * i, *span)
            substep(begin + 2 * i + 1, *span)
            return carry

        lax.fori_loop(0, (end - begin) // 2, two, 0)
        if (end - begin) % 2:
            substep(jnp.int32(end - 1), *span)

    for i in range(3):
        bar_out[i] = ext[(ETA + i, *own)]

    def safe_depth(f, rows, lanes):
        depth = xp[KU + f, rows, lanes] * xp[DZU + f, rows, lanes]
        return jnp.where(depth > 0, depth, 1.0)

    inner = slice(SUB, SUB + ny)
    for f in range(2):
        corr_out[f] = (acc[f, inner, cols] - xp[DZU + f, mid, cols] * sum_v[f]) / safe_depth(f, mid, cols)
    received(fourth)
    star = ru_w[...]
    fix = (acc[0, inner, at_w] - xp[DZU, mid, at_w] * jnp.sum(star, axis=1, keepdims=True)) / safe_depth(0, mid, at_w)
    u_c = column(star + fix, xp[KU, mid, at_w])
    star = row_of(rv_s[...], 1, at_s)
    total = jnp.sum(star, axis=0, keepdims=True)
    fix = (acc[1, SUB - 1:SUB, cols] - xp[DZV, at_s, cols] * total) / safe_depth(1, at_s, cols)
    vcs_out[...] = row_of(star + fix, 1, at_s)
    received(tracer)
    for i in range(2):
        halo_out[i, 0], halo_out[i, 1] = merged((0.5 * TIME_STEP) * u_c * (qc_w[i] + tc_w[i]), qc_e[i])
    trow_n_out[...] = jnp.where(below_wall, qr_n[...], 0.0)
    trow_s_out[...] = jnp.where(above_wall, qr_s[...], 0.0)
    sent(second + last_edges + third + tracer + fourth)


def last_kernel(us, vs, tm, sm, bar, corr, faces, vcs, halo, trow_n, trow_s,
                eta_out, tu_out, tv_out, u_out, v_out, t_out, s_out,
                new_u, new_v, new_t, new_s, flux, rest, turned, bar_sem, out_sem, *, bank):
    n_lev = u_out.shape[0]
    planes = [pltpu.make_async_copy(bar.at[i], ref, bar_sem.at[i]) for i, ref in enumerate((eta_out, tu_out, tv_out))]
    for c in planes:
        c.start()

    def fluxes(k, slot):
        kf = real(k)
        u = jnp.where(kf < faces[0], us[k + 1] + corr[0], 0.0)
        v = jnp.where(kf < faces[1], vs[k + 1] + corr[1], 0.0)
        new_u[k] = u
        new_v[k] = v
        u = (0.5 * TIME_STEP) * u
        v = (0.5 * TIME_STEP) * v
        here = pl.ds(k, 1)
        v_s = (0.5 * TIME_STEP) * vcs[here]
        b, m = slot_of(k, bank)
        for a, src in ((0, tm), (1, sm)):
            x = src[k + 1]
            turned[slot, a] = turn(halo[a, b], LANES - m)
            flux_x = u * (x + shift_east(x, turned[slot, a]))
            flux_y = v * (x + shift_north(x, trow_n[a, here]))
            edge_y = v_s * (trow_s[a, here] + x[FIRST])
            flux[slot, a] = flux_x
            rest[slot, a] = (x - flux_x) - (flux_y - shift_south(flux_y, edge_y))

    def finish(k, slot):
        wet = k.astype(F32) < faces[2]
        for a, dst in ((0, new_t), (1, new_s)):
            moved = shift_west(flux[slot, a], turned[slot, a])
            dst[k] = jnp.where(wet, rest[slot, a] + moved, 0.0)

    results = (new_u, u_out), (new_v, v_out), (new_t, t_out), (new_s, s_out)

    def copies(c):
        return [pltpu.make_async_copy(src.at[pl.ds(c * KB, KB)], dst.at[pl.ds(c * KB, KB)], out_sem.at[i])
                for i, (src, dst) in enumerate(results)]

    def chunk(c, carry):
        def done(d):
            finish(c * UE + d, d)
            if d % KB == KB - 1:
                for copy in copies(c * (UE // KB) + d // KB):
                    copy.start()

        for d in range(1, UE):
            fluxes(c * UE + d, d)
            done(d - 1)
        fluxes(jnp.minimum(c * UE + UE, n_lev - 1), 0)
        done(UE - 1)
        return carry

    fluxes(0, 0)
    lax.fori_loop(0, n_lev // UE, chunk, 0)
    for i, (src, dst) in enumerate(results):
        pltpu.make_async_copy(src, dst, out_sem.at[i]).wait()
    for c in planes:
        c.wait()


def solution(mesh):
    n_cols, n_rows = mesh.shape["col"], mesh.shape["row"]

    def local_step(vel_u, vel_v, value_a11, salinity, sea_level, trans_u, trans_v, bathymetry, kmt_levels, tide_force):
        n_lev, ny, nx = vel_u.shape
        whole, wide = ny + 2 * H, nx + LANES
        n_chunk, bank = n_lev // CH, (n_lev + 1) // 2
        hbm_spec = pl.BlockSpec(memory_space=pltpu.HBM)
        vmem_spec = pl.BlockSpec(memory_space=pltpu.VMEM)
        cube = (n_lev, ny, nx)
        deep = (n_lev + 2, ny, nx)
        n_row = n_lev + -n_lev % SUB
        column, pair_c, rows1, rows2 = (ny, LANES), (2, ny, LANES), (n_row, nx), (2, n_row, nx)
        banks, two, small, both = (2, 2, ny, LANES), (2, ny, nx), (SUB, LANES), (UN, 2, ny, nx)

        edges = (UN, 2, ny, LANES)

        def sds(*shape):
            return jax.ShapeDtypeStruct(shape, F32)

        def bufs(*shapes):
            return [pltpu.VMEM(shape, F32) for shape in shapes]

        def sems(*shape):
            return pltpu.SemaphoreType.DMA(shape)

        passed = [(3, ny, nx), two, (3, ny, nx), rows1, banks, rows2, rows2]
        *cubes, bar, corr, face, vcs, halo, trow_n, trow_s = pl.pallas_call(
            functools.partial(main_kernel, n_rows, n_cols),
            out_shape=bufs(*[deep] * 4, *passed),
            in_specs=[hbm_spec] * 10,
            out_specs=[vmem_spec] * (4 + len(passed)),
            scratch_shapes=[
                pltpu.SMEM(tide_force.shape[::-1], F32),
                pltpu.VMEM((ny, nx), jnp.int32),
                *bufs((7, whole, wide), (12, whole, wide), (2, ny + SUB, wide)),
                *bufs(*[(7, 3 * SUB, LANES)] * 2, *[(7, 2 * SUB, LANES)] * 2, *[(7, SUB, LANES)] * 4),
                *bufs(cube, cube, *[deep] * 3, cube, *[(ny, nx)] * 4, two, two, two, two, both, both, (UN, ny, nx), (UN, ny, nx), both, edges, (4, n_row, nx), (n_row, LANES)),
                *bufs(banks, banks, pair_c, pair_c, column, pair_c, pair_c, column, small, small, banks, (LANES, LANES)),
                *bufs(rows2, rows2, rows1, rows2, rows2, rows1),
                *bufs(pair_c, pair_c, rows2, rows2, pair_c, pair_c, rows2, rows2, column, rows1, column, rows1),
                sems(6), sems(4, n_chunk), sems(38), sems(38),
            ],
            compiler_params=pltpu.CompilerParams(collective_id=0, has_side_effects=True, vmem_limit_bytes=46 * 2**20),
        )(kmt_levels, bathymetry, sea_level, trans_u, trans_v, vel_u, vel_v, value_a11, salinity, tide_force.T)

        return pl.pallas_call(
            functools.partial(last_kernel, bank=bank),
            out_shape=[sds(ny, nx)] * 3 + [sds(*cube)] * 4,
            in_specs=[vmem_spec] * (4 + len(passed)),
            out_specs=[hbm_spec] * 7,
            scratch_shapes=[*bufs(*[cube] * 4, (UE, 2, ny, nx), (UE, 2, ny, nx), (UE, 2, ny, LANES)), sems(3), sems(4)],
            compiler_params=pltpu.CompilerParams(vmem_limit_bytes=24 * 2**20),
        )(*cubes, bar, corr, face, vcs, halo, trow_n, trow_s)

    spec_cube = P(None, "row", "col")
    spec_plane = P("row", "col")
    return jax.shard_map(local_step, mesh=mesh, in_specs=(spec_cube,) * 4 + (spec_plane,) * 5 + (P(None, None),),
                         out_specs=(spec_plane,) * 3 + (spec_cube,) * 4, check_vma=False)
```
